32 devices in a mesh: dp: 2 (over x), tp: 4 (over z), cp: 4 (over y, core).
Axes of the slice: x: 2, y: 2, z: 4, core: 2. Of those that a mesh axis runs over, the one named last changes fastest.
Arguments:
- x_in: bfloat16 [2, 4096, 2048], P('dp', 'cp'), parts along dimension 0
- w_q: bfloat16 [2048, 16, 128], P(None, 'tp')
- w_k: bfloat16 [2048, 16, 128], P(None, 'tp')
- w_v: bfloat16 [2048, 16, 128], P(None, 'tp')
- w_o: bfloat16 [16, 128, 2048], P('tp')
- q_norm_w: float32 [16, 128], P('tp')
- k_norm_w: float32 [16, 128], P('tp')
- post_norm_w: float32 [2048], replicated
- grad_y: bfloat16 [2, 4096, 2048], P('dp', 'cp'), parts along dimension 0
Outputs:
- output 1: bfloat16 [2, 4096, 2048], P('dp', 'cp'), parts along dimension 0
- output 2: bfloat16 [2, 4096, 2048], P('dp', 'cp'), parts along dimension 0
- output 3: float32 [4096, 16, 128], P('dp', 'tp'), parts along dimension 0
- output 4: float32 [4096, 16, 128], P('dp', 'tp'), parts along dimension 0
- output 5: float32 [4096, 16, 128], P('dp', 'tp'), parts along dimension 0
- output 6: float32 [32, 128, 2048], P(('dp', 'tp')), parts along dimension 0
- output 7: float32 [32, 128], P(('dp', 'tp')), parts along dimension 0
- output 8: float32 [32, 128], P(('dp', 'tp')), parts along dimension 0
- output 9: float32 [4096], P('dp'), parts along dimension 0
There are 2 independent parts. The reference program is written for one: setup_inputs(seed, part) draws one part's arguments, and reference() takes and returns one part's arrays. A program takes and returns all parts, laid end to end along the dimension named above; an argument that names none is the same for every part.
All inputs are finite; a program needn't handle non-finite values.
Results may differ from the reference program's by a relative error of at most 0.0159639.
Values are sent between devices in bfloat16 or wider.
A program may use at most 1 GiB of HBM per device.

```python
import jax
import jax.numpy as jnp
from jax import lax

BATCH_SIZE = 1
SEQ_LEN = 4096
D_MODEL = 2048
NUM_HEADS = 16
KV_HEADS = 16
HEAD_DIM = 128
QUERY_ROWS = 256
ROPE_THETA = 500000.0
NORM_EPS = 1e-6


def setup_inputs(seed: int = 0, part: int = 0) -> dict:
    base_key = jax.random.key(seed)
    act_keys = jax.random.split(jax.random.fold_in(base_key, part), 2)
    wt_keys = jax.random.split(jax.random.fold_in(base_key, 1000003), 9)
    act_shape = (BATCH_SIZE, SEQ_LEN, D_MODEL)
    x_in = jax.random.normal(act_keys[0], act_shape, jnp.float32).astype(jnp.bfloat16)
    grad_y = jax.random.normal(act_keys[1], act_shape, jnp.float32).astype(jnp.bfloat16)
    in_scale = D_MODEL ** -0.5
    out_scale = (NUM_HEADS * HEAD_DIM) ** -0.5
    w_q = (jax.random.normal(wt_keys[0], (D_MODEL, NUM_HEADS, HEAD_DIM), jnp.float32) * in_scale).astype(jnp.bfloat16)
    w_k = (jax.random.normal(wt_keys[1], (D_MODEL, KV_HEADS, HEAD_DIM), jnp.float32) * in_scale).astype(jnp.bfloat16)
    w_v = (jax.random.normal(wt_keys[2], (D_MODEL, KV_HEADS, HEAD_DIM), jnp.float32) * in_scale).astype(jnp.bfloat16)
    w_o = (jax.random.normal(wt_keys[3], (NUM_HEADS, HEAD_DIM, D_MODEL), jnp.float32) * out_scale).astype(jnp.bfloat16)
    q_head_gain = jax.random.uniform(wt_keys[4], (NUM_HEADS, 1), jnp.float32, 0.6, 1.4)
    q_norm_w = q_head_gain * (1.0 + 0.1 * jax.random.normal(wt_keys[5], (NUM_HEADS, HEAD_DIM), jnp.float32))
    k_head_gain = jax.random.uniform(wt_keys[6], (KV_HEADS, 1), jnp.float32, 0.6, 1.4)
    k_norm_w = k_head_gain * (1.0 + 0.1 * jax.random.normal(wt_keys[7], (KV_HEADS, HEAD_DIM), jnp.float32))
    post_norm_w = 1.0 + 0.3 * jax.random.normal(wt_keys[8], (D_MODEL,), jnp.float32)
    return {"x_in": x_in, "w_q": w_q, "w_k": w_k, "w_v": w_v, "w_o": w_o, "q_norm_w": q_norm_w, "k_norm_w": k_norm_w, "post_norm_w": post_norm_w, "grad_y": grad_y}


def rope_tables():
    half_dim = HEAD_DIM // 2
    inv_freq = ROPE_THETA ** (-2.0 * jnp.arange(half_dim, dtype=jnp.float32) / HEAD_DIM)
    angles = jnp.arange(SEQ_LEN, dtype=jnp.float32)[:, None] * inv_freq[None, :]
    return jnp.cos(angles), jnp.sin(angles)


def apply_rope(values, cos_tab, sin_tab):
    half_dim = values.shape[-1] // 2
    low_half = values[..., :half_dim]
    high_half = values[..., half_dim:]
    cos_rows = cos_tab[:, None, :]
    sin_rows = sin_tab[:, None, :]
    return jnp.concatenate([low_half * cos_rows - high_half * sin_rows, high_half * cos_rows + low_half * sin_rows], axis=-1)


def whole_norm(lin_out, weight):
    inv_rms = lax.rsqrt(jnp.mean(lin_out * lin_out, axis=(-2, -1), keepdims=True) + NORM_EPS)
    return lin_out * inv_rms * weight


def causal_attention(q_rot, k_rot, v_val):
    group_size = NUM_HEADS // KV_HEADS
    n_blocks = SEQ_LEN // QUERY_ROWS
    q_heads = jnp.moveaxis(q_rot.reshape(BATCH_SIZE, SEQ_LEN, KV_HEADS, group_size, HEAD_DIM), 2, 0)
    k_heads = jnp.moveaxis(k_rot, 2, 0)
    v_heads = jnp.moveaxis(v_val, 2, 0)
    key_pos = jnp.arange(SEQ_LEN)
    score_scale = HEAD_DIM ** -0.5

    def one_head(head_args):
        q_head, k_head, v_head = head_args
        q_blocks = jnp.moveaxis(q_head.reshape(BATCH_SIZE, n_blocks, QUERY_ROWS, group_size, HEAD_DIM), 1, 0)

        def one_block(block_args):
            q_block, block_idx = block_args
            scores = jnp.einsum("bqgd,bkd->bgqk", q_block, k_head) * score_scale
            query_pos = block_idx * QUERY_ROWS + jnp.arange(QUERY_ROWS)
            allowed = query_pos[:, None] >= key_pos[None, :]
            scores = jnp.where(allowed, scores, -jnp.inf)
            probs_blk = jax.nn.softmax(scores, axis=-1)
            return jnp.einsum("bgqk,bkd->bqgd", probs_blk, v_head)

        out_blocks = lax.map(jax.checkpoint(one_block), (q_blocks, jnp.arange(n_blocks)))
        return jnp.moveaxis(out_blocks, 0, 1).reshape(BATCH_SIZE, SEQ_LEN, group_size, HEAD_DIM)

    out_heads = lax.map(one_head, (q_heads, k_heads, v_heads))
    return jnp.moveaxis(out_heads, 0, 2).reshape(BATCH_SIZE, SEQ_LEN, NUM_HEADS, HEAD_DIM)


def forward(x_f, w_q, w_k, w_v, w_o, q_norm_w, k_norm_w, post_norm_w):
    cos_tab, sin_tab = rope_tables()
    q_lin = jnp.einsum("btd,dhe->bthe", x_f, w_q)
    k_lin = jnp.einsum("btd,dhe->bthe", x_f, w_k)
    v_lin = jnp.einsum("btd,dhe->bthe", x_f, w_v)
    q_rot = apply_rope(whole_norm(q_lin, q_norm_w), cos_tab, sin_tab).astype(jnp.bfloat16).astype(jnp.float32)
    k_rot = apply_rope(whole_norm(k_lin, k_norm_w), cos_tab, sin_tab).astype(jnp.bfloat16).astype(jnp.float32)
    v_val = v_lin.astype(jnp.bfloat16).astype(jnp.float32)
    attn_out = causal_attention(q_rot, k_rot, v_val).astype(jnp.bfloat16).astype(jnp.float32)
    proj = jnp.einsum("bthe,hed->btd", attn_out, w_o)
    post_hat = proj * lax.rsqrt(jnp.mean(proj * proj, axis=-1, keepdims=True) + NORM_EPS)
    return x_f + post_hat * post_norm_w


def reference(x_in, w_q, w_k, w_v, w_o, q_norm_w, k_norm_w, post_norm_w, grad_y):
    y_full, pullback = jax.vjp(forward, x_in.astype(jnp.float32), w_q.astype(jnp.float32), w_k.astype(jnp.float32), w_v.astype(jnp.float32), w_o.astype(jnp.float32), q_norm_w, k_norm_w, post_norm_w)
    all_grads = pullback(grad_y.astype(jnp.float32))
    return (y_full.astype(jnp.bfloat16), all_grads[0].astype(jnp.bfloat16), all_grads[1], all_grads[2], all_grads[3], all_grads[4], all_grads[5], all_grads[6], all_grads[7])
```

```python
import functools

import jax
import jax.numpy as jnp
from jax import lax
from jax.experimental import pallas as pl
from jax.experimental.pallas import tpu as pltpu
from jax.sharding import PartitionSpec as P

ROPE_THETA = 500000.0
NORM_EPS = 1e-6
MASK_VALUE = -1e30
LOG2E = 1.4426950408889634
MESH = pl.DeviceIdType.MESH
VMEM_SPEC = pl.BlockSpec(memory_space=pltpu.VMEM)
VMEM_LIMIT = 60 * 1024 * 1024
NT = (((1,), (1,)), ((), ()))
TN = (((0,), (0,)), ((), ()))


def dot_nt(a, b):
    return lax.dot_general(a, b, NT, preferred_element_type=jnp.float32)


def dot_tn(a, b):
    return lax.dot_general(a, b, TN, preferred_element_type=jnp.float32)


def dot_nn(a, b):
    return jnp.dot(a, b, preferred_element_type=jnp.float32)


def rope_tables(start_pos, seq_rows, head_dim):
    half_dim = head_dim // 2
    inv_freq = ROPE_THETA ** (-2.0 * jnp.arange(half_dim, dtype=jnp.float32) / head_dim)
    positions = (start_pos + jnp.arange(seq_rows)).astype(jnp.float32)
    angles = positions[:, None] * inv_freq[None, :]
    return jnp.cos(angles), jnp.sin(angles)


def rope(values, cos_tab, sin_tab, sign):
    half_dim = values.shape[-1] // 2
    low_half = values[..., :half_dim]
    high_half = values[..., half_dim:]
    sin_tab = sign * sin_tab
    return jnp.concatenate([low_half * cos_tab - high_half * sin_tab, high_half * cos_tab + low_half * sin_tab], axis=-1)


def entry_barrier(axis, size):
    me = lax.axis_index(axis)
    barrier = pltpu.get_barrier_semaphore()
    for shift in range(1, size):
        pl.semaphore_signal(barrier, inc=1, device_id={axis: lax.rem(me + shift, size)}, device_id_type=MESH)
    pl.semaphore_wait(barrier, size - 1)


def exchange_kernel(axis, size, count, *refs):
    ins = refs[:count]
    outs = refs[count:2 * count]
    send_sem, recv_sem = refs[2 * count:]
    me = lax.axis_index(axis)
    entry_barrier(axis, size)
    copies = []
    for idx in range(count):
        for shift in (2, 1, 3) if size == 4 else range(1, size):
            dst = lax.rem(me + shift, size)
            copy = pltpu.make_async_remote_copy(
                src_ref=ins[idx].at[dst], dst_ref=outs[idx].at[me],
                send_sem=send_sem.at[idx, shift - 1], recv_sem=recv_sem.at[idx, shift - 1],
                device_id={axis: dst}, device_id_type=MESH)
            copy.start()
            copies.append(copy)
    for idx in range(count):
        outs[idx][me] = ins[idx][me]
    for copy in copies:
        copy.wait()


def exchange(axis, size, collective_id, *arrays):
    count = len(arrays)
    return pl.pallas_call(
        functools.partial(exchange_kernel, axis, size, count),
        out_shape=tuple(jax.ShapeDtypeStruct(a.shape, a.dtype) for a in arrays),
        in_specs=[VMEM_SPEC] * count,
        out_specs=tuple([VMEM_SPEC] * count),
        scratch_shapes=[pltpu.SemaphoreType.DMA((count, size - 1)), pltpu.SemaphoreType.DMA((count, size - 1))],
        compiler_params=pltpu.CompilerParams(collective_id=collective_id, has_side_effects=True, vmem_limit_bytes=VMEM_LIMIT),
        name="exchange_" + str(collective_id),
    )(*arrays)


def sum_kernel(axis, size, in_ref, out_ref, slots, send_sem, recv_sem):
    me = lax.axis_index(axis)
    entry_barrier(axis, size)
    copies = []
    for shift in range(1, size):
        copy = pltpu.make_async_remote_copy(
            src_ref=in_ref, dst_ref=slots.at[me],
            send_sem=send_sem.at[shift - 1], recv_sem=recv_sem.at[shift - 1],
            device_id={axis: lax.rem(me + shift, size)}, device_id_type=MESH)
        copy.start()
        copies.append(copy)
    slots[me] = in_ref[...]
    for copy in copies:
        copy.wait()
    total = slots[0]
    for idx in range(1, size):
        total = total + slots[idx]
    out_ref[...] = total


def small_sum(axis, size, collective_id, array):
    return pl.pallas_call(
        functools.partial(sum_kernel, axis, size),
        out_shape=jax.ShapeDtypeStruct(array.shape, array.dtype),
        in_specs=[VMEM_SPEC],
        out_specs=VMEM_SPEC,
        scratch_shapes=[pltpu.VMEM((size,) + array.shape, array.dtype), pltpu.SemaphoreType.DMA((size - 1,)), pltpu.SemaphoreType.DMA((size - 1,))],
        compiler_params=pltpu.CompilerParams(collective_id=collective_id, has_side_effects=True),
        name="small_sum_" + str(collective_id),
    )(array)


def causal_mask(scores):
    key_pos = lax.broadcasted_iota(jnp.int32, scores.shape, 0)
    query_pos = lax.broadcasted_iota(jnp.int32, scores.shape, 1)
    return jnp.where(key_pos <= query_pos, scores, MASK_VALUE)


def attend_kernel(block, factor, q_ref, k_ref, v_ref, o_ref, lse_ref):
    blk = pl.program_id(0)
    q_blk = q_ref[...]

    def scores_of(idx):
        rows = pl.ds(pl.multiple_of(idx * block, block), block)
        return dot_nt(k_ref[rows, :], q_blk), v_ref[rows, :]

    scores, v_blk = scores_of(blk)
    scores = causal_mask(scores)
    top = jnp.max(scores, axis=0, keepdims=True)
    probs = jnp.exp2((scores - top) * factor)
    norm = jnp.sum(probs, axis=0, keepdims=True)
    acc = dot_tn(v_blk, probs.astype(jnp.bfloat16))

    def step(idx, state):
        top, norm, acc = state
        scores, v_blk = scores_of(idx)
        new_top = jnp.maximum(top, jnp.max(scores, axis=0, keepdims=True))
        probs = jnp.exp2((scores - new_top) * factor)
        rescale = jnp.exp2((top - new_top) * factor)
        norm = norm * rescale + jnp.sum(probs, axis=0, keepdims=True)
        acc = acc * rescale + dot_tn(v_blk, probs.astype(jnp.bfloat16))
        return new_top, norm, acc

    top, norm, acc = lax.fori_loop(0, blk, step, (top, norm, acc))
    o_ref[...] = (acc / norm).T.astype(jnp.bfloat16)
    lse_ref[...] = top * factor + jnp.log2(norm)


def attend(q, k, v):
    rows, head_dim = q.shape
    block = min(512, rows // 4)
    whole = pl.BlockSpec((rows, head_dim), lambda i: (0, 0))
    part = pl.BlockSpec((block, head_dim), lambda i: (i, 0))
    return pl.pallas_call(
        functools.partial(attend_kernel, block, head_dim ** -0.5 * LOG2E),
        grid=(rows // block,),
        out_shape=(jax.ShapeDtypeStruct(q.shape, jnp.bfloat16), jax.ShapeDtypeStruct((1, rows), jnp.float32)),
        in_specs=[part, whole, whole],
        out_specs=(part, pl.BlockSpec((1, block), lambda i: (0, i))),
        compiler_params=pltpu.CompilerParams(vmem_limit_bytes=VMEM_LIMIT),
        cost_estimate=pl.CostEstimate(flops=2 * rows * rows * head_dim, bytes_accessed=8 * rows * head_dim, transcendentals=rows * rows // 2),
        name="attend",
    )(q, k, v)


def attend_back_kernel(block, scale, q_ref, k_ref, v_ref, o_ref, do_ref, lse_ref, dq_ref, dk_ref, dv_ref, delta_ref, dk_acc, dv_acc):
    blk = pl.program_id(0)
    n_blk = pl.num_programs(0)
    factor = scale * LOG2E

    @pl.when(blk == 0)
    def _():
        def prepare(idx, carry):
            rows = pl.ds(pl.multiple_of(idx * block, block), block)
            prod = do_ref[rows, :].astype(jnp.float32) * o_ref[rows, :].astype(jnp.float32)
            delta_ref[:, rows] = jnp.sum(prod.T, axis=0, keepdims=True)
            dq_ref[rows, :] = jnp.zeros((block, dq_ref.shape[1]), jnp.float32)
            return carry
        lax.fori_loop(0, n_blk, prepare, 0)

    k_blk = k_ref[...]
    v_blk = v_ref[...]

    def one(idx, masked):
        rows = pl.ds(pl.multiple_of(idx * block, block), block)
        q_blk = q_ref[rows, :]
        do_blk = do_ref[rows, :]
        scores = dot_nt(k_blk, q_blk)
        if masked:
            scores = causal_mask(scores)
        probs = jnp.exp2(scores * factor - lse_ref[:, rows])
        grad_v = dot_nn(probs.astype(jnp.bfloat16), do_blk)
        grad_p = dot_nt(v_blk, do_blk)
        grad_s = (probs * ((grad_p - delta_ref[:, rows]) * scale)).astype(jnp.bfloat16)
        dq_ref[rows, :] += dot_tn(grad_s, k_blk)
        return dot_nn(grad_s, q_blk), grad_v

    dk_acc[...], dv_acc[...] = one(blk, True)

    def step(idx, carry):
        grad_k, grad_v = one(idx, False)
        dk_acc[...] += grad_k
        dv_acc[...] += grad_v
        return carry

    lax.fori_loop(blk + 1, n_blk, step, 0)
    dk_ref[...] = dk_acc[...]
    dv_ref[...] = dv_acc[...].astype(jnp.bfloat16)


def attend_back(q, k, v, o, do, lse):
    rows, head_dim = q.shape
    block = min(512, rows // 4)
    whole = pl.BlockSpec((rows, head_dim), lambda i: (0, 0))
    part = pl.BlockSpec((block, head_dim), lambda i: (i, 0))
    stat = pl.BlockSpec((1, rows), lambda i: (0, 0))
    return pl.pallas_call(
        functools.partial(attend_back_kernel, block, head_dim ** -0.5),
        grid=(rows // block,),
        out_shape=(jax.ShapeDtypeStruct(q.shape, jnp.float32), jax.ShapeDtypeStruct(q.shape, jnp.float32), jax.ShapeDtypeStruct(q.shape, jnp.bfloat16)),
        in_specs=[whole, part, part, whole, whole, stat],
        out_specs=(whole, part, part),
        scratch_shapes=[pltpu.VMEM((1, rows), jnp.float32), pltpu.VMEM((block, head_dim), jnp.float32), pltpu.VMEM((block, head_dim), jnp.float32)],
        compiler_params=pltpu.CompilerParams(vmem_limit_bytes=VMEM_LIMIT),
        cost_estimate=pl.CostEstimate(flops=5 * rows * rows * head_dim, bytes_accessed=20 * rows * head_dim, transcendentals=rows * rows // 2),
        name="attend_back",
    )(q, k, v, o, do, lse)


def post_kernel(tp_size, o_ref, wo_ref, wown_ref, x_ref, gy_ref, pw_ref, y_ref, gp_ref, do_ref, gpost_ref):
    proj = dot_nn(o_ref[0], wo_ref[0])
    for idx in range(1, tp_size):
        proj = proj + dot_nn(o_ref[idx], wo_ref[idx])
    gain = pw_ref[...]
    inv = lax.rsqrt(jnp.mean(proj * proj, axis=-1, keepdims=True) + NORM_EPS)
    hat = proj * inv
    y_ref[...] = (x_ref[...].astype(jnp.float32) + hat * gain).astype(jnp.bfloat16)
    grad = gy_ref[...].astype(jnp.float32)
    gpost = jnp.sum(grad * hat, axis=0, keepdims=True)
    grad_hat = grad * gain
    grad_proj = (inv * (grad_hat - hat * jnp.mean(grad_hat * hat, axis=-1, keepdims=True))).astype(jnp.bfloat16)
    gp_ref[...] = grad_proj
    grad_o = dot_nt(grad_proj, wown_ref[...]).astype(jnp.bfloat16)
    head_dim = do_ref.shape[2]
    for idx in range(do_ref.shape[0]):
        do_ref[idx] = grad_o[:, idx * head_dim:(idx + 1) * head_dim]

    @pl.when(pl.program_id(0) == 0)
    def _():
        gpost_ref[...] = jnp.zeros_like(gpost_ref)

    gpost_ref[...] += gpost


def post(o_all, wo_all, w_own, x, gy, gain, heads, head_dim):
    tp_size, rows, width = o_all.shape
    d_model = x.shape[1]
    block = min(256, rows)
    act = pl.BlockSpec((block, d_model), lambda i: (i, 0))
    return pl.pallas_call(
        functools.partial(post_kernel, tp_size),
        grid=(rows // block,),
        out_shape=(jax.ShapeDtypeStruct((rows, d_model), jnp.bfloat16), jax.ShapeDtypeStruct((rows, d_model), jnp.bfloat16),
                   jax.ShapeDtypeStruct((heads, rows, head_dim), jnp.bfloat16), jax.ShapeDtypeStruct((1, d_model), jnp.float32)),
        in_specs=[pl.BlockSpec((tp_size, block, width), lambda i: (0, i, 0)), pl.BlockSpec(wo_all.shape, lambda i: (0, 0, 0)),
                  pl.BlockSpec(w_own.shape, lambda i: (0, 0)), act, act, pl.BlockSpec((1, d_model), lambda i: (0, 0))],
        out_specs=(act, act, pl.BlockSpec((heads, block, head_dim), lambda i: (0, i, 0)), pl.BlockSpec((1, d_model), lambda i: (0, 0))),
        compiler_params=pltpu.CompilerParams(vmem_limit_bytes=VMEM_LIMIT),
        cost_estimate=pl.CostEstimate(flops=2 * rows * d_model * (d_model + width), bytes_accessed=4 * d_model * d_model, transcendentals=rows),
        name="post",
    )(o_all, wo_all, w_own, x, gy, gain)


def chain_kernel(size, n_chunk, lag, part_ref, gy_ref, out_ref, sums_a, sums_b, rs_send, rs_recv, ag_send, ag_recv):
    me = lax.axis_index("tp")
    entry_barrier("tp", size)
    half = part_ref.shape[0] // 2
    rows = half // n_chunk
    last = size - 1

    def parts(side, chunk):
        local = pl.ds(pl.multiple_of(chunk * rows, rows), rows)
        glob = pl.ds(pl.multiple_of(side * half + chunk * rows, rows), rows)
        sums = (sums_a, sums_b)[side]
        return local, glob, sums

    def toward(side):
        return jnp.maximum(me - 1, 0) if side == 0 else jnp.minimum(me + 1, last)

    def away(side):
        return jnp.minimum(me + 1, last) if side == 0 else jnp.maximum(me - 1, 0)

    def rs_copy(side, chunk, first):
        local, glob, sums = parts(side, chunk)
        return pltpu.make_async_remote_copy(
            src_ref=part_ref.at[glob] if first else sums.at[local], dst_ref=sums.at[local],
            send_sem=rs_send.at[side, chunk], recv_sem=rs_recv.at[side, chunk],
            device_id={"tp": toward(side)}, device_id_type=MESH)

    def ag_copy(side, chunk):
        local, glob, sums = parts(side, chunk)
        return pltpu.make_async_remote_copy(
            src_ref=out_ref.at[glob], dst_ref=out_ref.at[glob],
            send_sem=ag_send.at[side, chunk], recv_sem=ag_recv.at[side, chunk],
            device_id={"tp": away(side)}, device_id_type=MESH)

    def step(idx, carry):
        for side in (0, 1):
            pos = me if side == 0 else last - me
            local, glob, sums = parts(side, idx)

            @pl.when((idx < n_chunk) & (pos == last))
            def _(side=side):
                rs_copy(side, idx, True).start()

            @pl.when((idx < n_chunk) & (pos > 0) & (pos < last))
            def _(side=side, local=local, glob=glob, sums=sums):
                rs_copy(side, idx, False).wait_recv()
                sums[local] = sums[local] + part_ref[glob]
                rs_copy(side, idx, False).start()

            @pl.when((idx < n_chunk) & (pos == 0))
            def _(side=side, local=local, glob=glob, sums=sums):
                rs_copy(side, idx, False).wait_recv()
                out_ref[glob] = (gy_ref[glob].astype(jnp.float32) + (sums[local] + part_ref[glob])).astype(jnp.bfloat16)
                ag_copy(side, idx).start()

            @pl.when((idx >= lag) & (pos > 0))
            def _(side=side):
                ag_copy(side, idx - lag).wait_recv()

            @pl.when((idx >= lag) & (pos > 0) & (pos < last))
            def _(side=side):
                ag_copy(side, idx - lag).start()
        return carry

    lax.fori_loop(0, n_chunk + lag, step, 0)

    def drain(idx, carry):
        for side in (0, 1):
            pos = me if side == 0 else last - me

            @pl.when(pos > 0)
            def _(side=side):
                rs_copy(side, idx, False).wait_send()

            @pl.when(pos < last)
            def _(side=side):
                ag_copy(side, idx).wait_send()
        return carry

    lax.fori_loop(0, n_chunk, drain, 0)


def chain_sum(size, collective_id, part, gy):
    rows, d_model = part.shape
    n_chunk = 16 if rows >= 512 else 2
    sems = [pltpu.SemaphoreType.DMA((2, n_chunk))] * 4
    return pl.pallas_call(
        functools.partial(chain_kernel, size, n_chunk, min(6, n_chunk)),
        out_shape=jax.ShapeDtypeStruct((rows, d_model), jnp.bfloat16),
        in_specs=[VMEM_SPEC, VMEM_SPEC],
        out_specs=VMEM_SPEC,
        scratch_shapes=[pltpu.VMEM((rows // 2, d_model), jnp.float32), pltpu.VMEM((rows // 2, d_model), jnp.float32)] + sems,
        compiler_params=pltpu.CompilerParams(collective_id=collective_id, has_side_effects=True, vmem_limit_bytes=VMEM_LIMIT),
        cost_estimate=pl.CostEstimate(flops=10 ** 11, bytes_accessed=16 * rows * d_model, transcendentals=0),
        name="chain_sum",
    )(part, gy)


def solution(mesh):
    tp_size = mesh.shape["tp"]
    cp_size = mesh.shape["cp"]
    act_spec = P("dp", "cp", None)
    col_spec = P(None, "tp", None)
    part_col = P("dp", "tp", None)
    in_specs = (act_spec, col_spec, col_spec, col_spec, P("tp", None, None), P("tp", None), P("tp", None), P(None), act_spec)
    out_specs = (act_spec, act_spec, part_col, part_col, part_col, P(("dp", "tp"), None, None), P(("dp", "tp"), None), P(("dp", "tp"), None), P("dp"))
    swap_core = [(dev, dev ^ 1) for dev in range(cp_size)]

    def local_run(x_in, w_q, w_k, w_v, w_o, q_norm_w, k_norm_w, post_norm_w, grad_y):
        rows, d_model = x_in.shape[1:]
        heads, head_dim = w_q.shape[1:]
        width = heads * head_dim
        full_width = width * tp_size
        x = x_in[0]
        gy = grad_y[0]
        cp_index = lax.axis_index("cp")
        cos_tab, sin_tab = rope_tables(cp_index * rows, rows, head_dim)
        wq, wk, wv = (w.reshape(d_model, width) for w in (w_q, w_k, w_v))

        core = cp_index % 2
        own_half = lax.dynamic_slice_in_dim(w_o, core * (heads // 2), heads // 2, axis=0)
        mine = lax.all_gather(own_half, "tp")
        other = lax.ppermute(mine, "cp", swap_core)
        wo_all = jnp.where(core == 0, jnp.concatenate([mine, other], axis=1), jnp.concatenate([other, mine], axis=1))
        wo_all = wo_all.reshape(tp_size, width, d_model)

        def by_head(t):
            return t.reshape(rows, heads, head_dim).transpose(1, 0, 2)

        q_lin = jnp.dot(x, wq, preferred_element_type=jnp.float32)
        k_lin = jnp.dot(x, wk, preferred_element_type=jnp.float32)
        v_lin = jnp.dot(x, wv, preferred_element_type=jnp.float32)
        squares = jnp.stack([jnp.sum(q_lin * q_lin, axis=1), jnp.sum(k_lin * k_lin, axis=1)])
        squares = small_sum("tp", tp_size, 0, squares)
        invs = lax.rsqrt(squares / full_width + NORM_EPS)[:, :, None]
        q_hat = by_head(q_lin * invs[0])
        k_hat = by_head(k_lin * invs[1])
        q_gain = q_norm_w[:, None, :]
        k_gain = k_norm_w[:, None, :]
        q_rot = rope(q_hat * q_gain, cos_tab, sin_tab, 1.0).astype(jnp.bfloat16)
        k_rot = rope(k_hat * k_gain, cos_tab, sin_tab, 1.0).astype(jnp.bfloat16)
        v_val = by_head(v_lin.astype(jnp.bfloat16))

        seq_shape = (cp_size * rows, head_dim)
        block_shape = (cp_size, rows, head_dim)
        q_seq, k_seq, v_seq = (t.reshape(seq_shape) for t in exchange("cp", cp_size, 1, q_rot, k_rot, v_val))
        o_seq, lse = attend(q_seq, k_seq, v_seq)
        (o_heads,) = exchange("cp", cp_size, 2, o_seq.reshape(block_shape))
        o_mine = o_heads.transpose(1, 0, 2).reshape(rows, width)
        o_all = lax.all_gather(o_mine, "tp")
        y_out, grad_proj, grad_o, grad_post = post(o_all, wo_all, w_o.reshape(width, d_model), x, gy, post_norm_w[None, :], heads, head_dim)
        (do_seq,) = exchange("cp", cp_size, 3, grad_o)
        dwo_part = lax.dot_general(o_mine, grad_proj, TN, preferred_element_type=jnp.float32)
        grad_w_o = lax.psum(dwo_part, "cp")

        dq_seq, dk_seq, dv_seq = attend_back(q_seq, k_seq, v_seq, o_seq, do_seq.reshape(seq_shape), lse)
        dq, dk, dv = exchange("cp", cp_size, 4, dq_seq.reshape(block_shape), dk_seq.reshape(block_shape), dv_seq.reshape(block_shape))

        def scaled_back(grad_rot, hat, gain):
            grad = rope(grad_rot, cos_tab, sin_tab, -1.0)
            grad_gain = jnp.sum(grad * hat, axis=1)
            grad_hat = grad * gain
            return grad_hat, grad_gain, jnp.sum(grad_hat * hat, axis=(0, 2))

        gq_hat, grad_q_norm, q_dot = scaled_back(dq, q_hat, q_gain)
        gk_hat, grad_k_norm, k_dot = scaled_back(dk, k_hat, k_gain)
        dots = small_sum("tp", tp_size, 5, jnp.stack([q_dot, k_dot])) / full_width

        def flat(t):
            return t.transpose(1, 0, 2).reshape(rows, width)

        dq16 = flat((invs[0][None] * (gq_hat - q_hat * dots[0][None, :, None])).astype(jnp.bfloat16))
        dk16 = flat((invs[1][None] * (gk_hat - k_hat * dots[1][None, :, None])).astype(jnp.bfloat16))
        dv16 = flat(dv)
        dw = tuple(lax.dot_general(x, g, TN, preferred_element_type=jnp.float32) for g in (dq16, dk16, dv16))
        dw, dq16, dk16, dv16 = lax.optimization_barrier((dw, dq16, dk16, dv16))
        dx_part = sum(lax.dot_general(g, w, NT, preferred_element_type=jnp.float32) for g, w in ((dq16, wq), (dk16, wk), (dv16, wv)))
        grad_x = chain_sum(tp_size, 6, dx_part, gy)
        grad_w_o, *dw = lax.optimization_barrier((grad_w_o,) + tuple(dw))
        sums = lax.psum((tuple(dw), grad_q_norm, grad_k_norm, grad_post[0]), "cp")
        dw, grad_q_norm, grad_k_norm, grad_post = sums
        dw = tuple(g.reshape(d_model, heads, head_dim) for g in dw)
        return (y_out[None], grad_x[None]) + dw + (grad_w_o.reshape(heads, head_dim, d_model), grad_q_norm, grad_k_norm, grad_post)

    return jax.shard_map(local_run, mesh=mesh, in_specs=in_specs, out_specs=out_specs, check_vma=False)
```

```python
import functools

import jax
import jax.numpy as jnp
from jax import lax
from jax.experimental import pallas as pl
from jax.experimental.pallas import tpu as pltpu
from jax.sharding import PartitionSpec as P

ROPE_THETA = 500000.0
NORM_EPS = 1e-6
MASK_VALUE = -1e30
LOG2E = 1.4426950408889634
MESH = pl.DeviceIdType.MESH
VMEM_SPEC = pl.BlockSpec(memory_space=pltpu.VMEM)
VMEM_LIMIT = 60 * 1024 * 1024
NT = (((1,), (1,)), ((), ()))
TN = (((0,), (0,)), ((), ()))


def dot_nt(a, b):
    return lax.dot_general(a, b, NT, preferred_element_type=jnp.float32)


def dot_tn(a, b):
    return lax.dot_general(a, b, TN, preferred_element_type=jnp.float32)


def dot_nn(a, b):
    return jnp.dot(a, b, preferred_element_type=jnp.float32)


def rope_tables(start_pos, seq_rows, head_dim):
    half_dim = head_dim // 2
    inv_freq = ROPE_THETA ** (-2.0 * jnp.arange(half_dim, dtype=jnp.float32) / head_dim)
    positions = (start_pos + jnp.arange(seq_rows)).astype(jnp.float32)
    angles = positions[:, None] * inv_freq[None, :]
    return jnp.cos(angles), jnp.sin(angles)


def rope(values, cos_tab, sin_tab, sign):
    half_dim = values.shape[-1] // 2
    low_half = values[..., :half_dim]
    high_half = values[..., half_dim:]
    sin_tab = sign * sin_tab
    return jnp.concatenate([low_half * cos_tab - high_half * sin_tab, high_half * cos_tab + low_half * sin_tab], axis=-1)


def entry_barrier(axis, size):
    me = lax.axis_index(axis)
    barrier = pltpu.get_barrier_semaphore()
    for shift in range(1, size):
        pl.semaphore_signal(barrier, inc=1, device_id={axis: lax.rem(me + shift, size)}, device_id_type=MESH)
    pl.semaphore_wait(barrier, size - 1)


def exchange_kernel(axis, size, count, *refs):
    ins = refs[:count]
    outs = refs[count:2 * count]
    send_sem, recv_sem = refs[2 * count:]
    me = lax.axis_index(axis)
    entry_barrier(axis, size)
    copies = []
    for idx in range(count):
        for shift in (2, 1, 3) if size == 4 else range(1, size):
            dst = lax.rem(me + shift, size)
            copy = pltpu.make_async_remote_copy(
                src_ref=ins[idx].at[dst], dst_ref=outs[idx].at[me],
                send_sem=send_sem.at[idx, shift - 1], recv_sem=recv_sem.at[idx, shift - 1],
                device_id={axis: dst}, device_id_type=MESH)
            copy.start()
            copies.append(copy)
    for idx in range(count):
        outs[idx][me] = ins[idx][me]
    for copy in copies:
        copy.wait()


def exchange_product_kernel(axis, size, block, in_ref, a_ref, b_ref, out_ref, prod_ref, send_sem, recv_sem):
    me = lax.axis_index(axis)
    entry_barrier(axis, size)
    copies = []
    for shift in (2, 1, 3) if size == 4 else range(1, size):
        dst = lax.rem(me + shift, size)
        copy = pltpu.make_async_remote_copy(
            src_ref=in_ref.at[dst], dst_ref=out_ref.at[me], send_sem=send_sem.at[shift - 1], recv_sem=recv_sem.at[shift - 1],
            device_id={axis: dst}, device_id_type=MESH)
        copy.start()
        copies.append(copy)
    out_ref[me] = in_ref[me]

    def step(idx, carry):
        cols = pl.ds(pl.multiple_of(idx * block, block), block)
        prod_ref[:, cols] = dot_tn(a_ref[...], b_ref[:, cols])
        return carry

    lax.fori_loop(0, b_ref.shape[1] // block, step, 0)
    for copy in copies:
        copy.wait()


def exchange_product(axis, size, collective_id, array, a, b):
    return pl.pallas_call(
        functools.partial(exchange_product_kernel, axis, size, min(512, b.shape[1])),
        out_shape=(jax.ShapeDtypeStruct(array.shape, array.dtype), jax.ShapeDtypeStruct((a.shape[1], b.shape[1]), jnp.float32)),
        in_specs=[VMEM_SPEC] * 3,
        out_specs=(VMEM_SPEC, VMEM_SPEC),
        scratch_shapes=[pltpu.SemaphoreType.DMA((size - 1,)), pltpu.SemaphoreType.DMA((size - 1,))],
        compiler_params=pltpu.CompilerParams(collective_id=collective_id, has_side_effects=True, vmem_limit_bytes=VMEM_LIMIT),
        name="exchange_product",
    )(array, a, b)


def exchange(axis, size, collective_id, *arrays):
    count = len(arrays)
    return pl.pallas_call(
        functools.partial(exchange_kernel, axis, size, count),
        out_shape=tuple(jax.ShapeDtypeStruct(a.shape, a.dtype) for a in arrays),
        in_specs=[VMEM_SPEC] * count,
        out_specs=tuple([VMEM_SPEC] * count),
        scratch_shapes=[pltpu.SemaphoreType.DMA((count, size - 1)), pltpu.SemaphoreType.DMA((count, size - 1))],
        compiler_params=pltpu.CompilerParams(collective_id=collective_id, has_side_effects=True, vmem_limit_bytes=VMEM_LIMIT),
        name="exchange_" + str(collective_id),
    )(*arrays)


def sum_kernel(axis, size, in_ref, out_ref, slots, send_sem, recv_sem):
    me = lax.axis_index(axis)
    entry_barrier(axis, size)
    copies = []
    for shift in range(1, size):
        copy = pltpu.make_async_remote_copy(
            src_ref=in_ref, dst_ref=slots.at[me],
            send_sem=send_sem.at[shift - 1], recv_sem=recv_sem.at[shift - 1],
            device_id={axis: lax.rem(me + shift, size)}, device_id_type=MESH)
        copy.start()
        copies.append(copy)
    slots[me] = in_ref[...]
    for copy in copies:
        copy.wait()
    total = slots[0]
    for idx in range(1, size):
        total = total + slots[idx]
    out_ref[...] = total


def small_sum(axis, size, collective_id, array):
    return pl.pallas_call(
        functools.partial(sum_kernel, axis, size),
        out_shape=jax.ShapeDtypeStruct(array.shape, array.dtype),
        in_specs=[VMEM_SPEC],
        out_specs=VMEM_SPEC,
        scratch_shapes=[pltpu.VMEM((size,) + array.shape, array.dtype), pltpu.SemaphoreType.DMA((size - 1,)), pltpu.SemaphoreType.DMA((size - 1,))],
        compiler_params=pltpu.CompilerParams(collective_id=collective_id, has_side_effects=True),
        name="small_sum_" + str(collective_id),
    )(array)


def causal_mask(scores):
    key_pos = lax.broadcasted_iota(jnp.int32, scores.shape, 0)
    query_pos = lax.broadcasted_iota(jnp.int32, scores.shape, 1)
    return jnp.where(key_pos <= query_pos, scores, MASK_VALUE)


def attend_kernel(block, factor, q_ref, k_ref, v_ref, o_ref, lse_ref):
    blk = pl.program_id(0)
    q_blk = q_ref[...]

    def scores_of(idx):
        rows = pl.ds(pl.multiple_of(idx * block, block), block)
        return dot_nt(k_ref[rows, :], q_blk), v_ref[rows, :]

    scores, v_blk = scores_of(blk)
    scores = causal_mask(scores)
    top = jnp.max(scores, axis=0, keepdims=True)
    probs = jnp.exp2((scores - top) * factor)
    norm = jnp.sum(probs, axis=0, keepdims=True)
    acc = dot_tn(v_blk, probs.astype(jnp.bfloat16))

    def step(idx, state):
        top, norm, acc = state
        scores, v_blk = scores_of(idx)
        new_top = jnp.maximum(top, jnp.max(scores, axis=0, keepdims=True))
        probs = jnp.exp2((scores - new_top) * factor)
        rescale = jnp.exp2((top - new_top) * factor)
        norm = norm * rescale + jnp.sum(probs, axis=0, keepdims=True)
        acc = acc * rescale + dot_tn(v_blk, probs.astype(jnp.bfloat16))
        return new_top, norm, acc

    top, norm, acc = lax.fori_loop(0, blk, step, (top, norm, acc))
    o_ref[...] = (acc / norm).T.astype(jnp.bfloat16)
    lse_ref[...] = top * factor + jnp.log2(norm)


def attend(q, k, v):
    rows, head_dim = q.shape
    block = min(512, rows // 4)
    whole = pl.BlockSpec((rows, head_dim), lambda i: (0, 0))
    part = pl.BlockSpec((block, head_dim), lambda i: (i, 0))
    return pl.pallas_call(
        functools.partial(attend_kernel, block, head_dim ** -0.5 * LOG2E),
        grid=(rows // block,),
        out_shape=(jax.ShapeDtypeStruct(q.shape, jnp.bfloat16), jax.ShapeDtypeStruct((1, rows), jnp.float32)),
        in_specs=[part, whole, whole],
        out_specs=(part, pl.BlockSpec((1, block), lambda i: (0, i))),
        compiler_params=pltpu.CompilerParams(vmem_limit_bytes=VMEM_LIMIT),
        cost_estimate=pl.CostEstimate(flops=2 * rows * rows * head_dim, bytes_accessed=8 * rows * head_dim, transcendentals=rows * rows // 2),
        name="attend",
    )(q, k, v)


def attend_back_kernel(block, scale, q_ref, k_ref, v_ref, o_ref, do_ref, lse_ref, dq_ref, dk_ref, dv_ref, delta_ref, dk_acc, dv_acc):
    blk = pl.program_id(0)
    n_blk = pl.num_programs(0)
    factor = scale * LOG2E

    @pl.when(blk == 0)
    def _():
        def prepare(idx, carry):
            rows = pl.ds(pl.multiple_of(idx * block, block), block)
            prod = do_ref[rows, :].astype(jnp.float32) * o_ref[rows, :].astype(jnp.float32)
            delta_ref[:, rows] = jnp.sum(prod.T, axis=0, keepdims=True)
            dq_ref[rows, :] = jnp.zeros((block, dq_ref.shape[1]), jnp.float32)
            return carry
        lax.fori_loop(0, n_blk, prepare, 0)

    k_blk = k_ref[...]
    v_blk = v_ref[...]

    def one(idx, masked):
        rows = pl.ds(pl.multiple_of(idx * block, block), block)
        q_blk = q_ref[rows, :]
        do_blk = do_ref[rows, :]
        scores = dot_nt(k_blk, q_blk)
        if masked:
            scores = causal_mask(scores)
        probs = jnp.exp2(scores * factor - lse_ref[:, rows])
        grad_v = dot_nn(probs.astype(jnp.bfloat16), do_blk)
        grad_p = dot_nt(v_blk, do_blk)
        grad_s = (probs * ((grad_p - delta_ref[:, rows]) * scale)).astype(jnp.bfloat16)
        dq_ref[rows, :] += dot_tn(grad_s, k_blk)
        return dot_nn(grad_s, q_blk), grad_v

    dk_acc[...], dv_acc[...] = one(blk, True)

    def step(idx, carry):
        grad_k, grad_v = one(idx, False)
        dk_acc[...] += grad_k
        dv_acc[...] += grad_v
        return carry

    lax.fori_loop(blk + 1, n_blk, step, 0)
    dk_ref[...] = dk_acc[...]
    dv_ref[...] = dv_acc[...].astype(jnp.bfloat16)


def attend_back(q, k, v, o, do, lse):
    rows, head_dim = q.shape
    block = min(512, rows // 4)
    whole = pl.BlockSpec((rows, head_dim), lambda i: (0, 0))
    part = pl.BlockSpec((block, head_dim), lambda i: (i, 0))
    stat = pl.BlockSpec((1, rows), lambda i: (0, 0))
    return pl.pallas_call(
        functools.partial(attend_back_kernel, block, head_dim ** -0.5),
        grid=(rows // block,),
        out_shape=(jax.ShapeDtypeStruct(q.shape, jnp.float32), jax.ShapeDtypeStruct(q.shape, jnp.float32), jax.ShapeDtypeStruct(q.shape, jnp.bfloat16)),
        in_specs=[whole, part, part, whole, whole, stat],
        out_specs=(whole, part, part),
        scratch_shapes=[pltpu.VMEM((1, rows), jnp.float32), pltpu.VMEM((block, head_dim), jnp.float32), pltpu.VMEM((block, head_dim), jnp.float32)],
        compiler_params=pltpu.CompilerParams(vmem_limit_bytes=VMEM_LIMIT),
        cost_estimate=pl.CostEstimate(flops=5 * rows * rows * head_dim, bytes_accessed=20 * rows * head_dim, transcendentals=rows * rows // 2),
        name="attend_back",
    )(q, k, v, o, do, lse)


def post_kernel(tp_size, o_ref, wo_ref, wown_ref, x_ref, gy_ref, pw_ref, y_ref, gp_ref, do_ref, gpost_ref):
    proj = dot_nn(o_ref[0], wo_ref[0])
    for idx in range(1, tp_size):
        proj = proj + dot_nn(o_ref[idx], wo_ref[idx])
    gain = pw_ref[...]
    inv = lax.rsqrt(jnp.mean(proj * proj, axis=-1, keepdims=True) + NORM_EPS)
    hat = proj * inv
    y_ref[...] = (x_ref[...].astype(jnp.float32) + hat * gain).astype(jnp.bfloat16)
    grad = gy_ref[...].astype(jnp.float32)
    gpost = jnp.sum(grad * hat, axis=0, keepdims=True)
    grad_hat = grad * gain
    grad_proj = (inv * (grad_hat - hat * jnp.mean(grad_hat * hat, axis=-1, keepdims=True))).astype(jnp.bfloat16)
    gp_ref[...] = grad_proj
    grad_o = dot_nt(grad_proj, wown_ref[...]).astype(jnp.bfloat16)
    head_dim = do_ref.shape[2]
    for idx in range(do_ref.shape[0]):
        do_ref[idx] = grad_o[:, idx * head_dim:(idx + 1) * head_dim]

    @pl.when(pl.program_id(0) == 0)
    def _():
        gpost_ref[...] = jnp.zeros_like(gpost_ref)

    gpost_ref[...] += gpost


def post(o_all, wo_all, w_own, x, gy, gain, heads, head_dim):
    tp_size, rows, width = o_all.shape
    d_model = x.shape[1]
    block = min(256, rows)
    act = pl.BlockSpec((block, d_model), lambda i: (i, 0))
    return pl.pallas_call(
        functools.partial(post_kernel, tp_size),
        grid=(rows // block,),
        out_shape=(jax.ShapeDtypeStruct((rows, d_model), jnp.bfloat16), jax.ShapeDtypeStruct((rows, d_model), jnp.bfloat16),
                   jax.ShapeDtypeStruct((heads, rows, head_dim), jnp.bfloat16), jax.ShapeDtypeStruct((1, d_model), jnp.float32)),
        in_specs=[pl.BlockSpec((tp_size, block, width), lambda i: (0, i, 0)), pl.BlockSpec(wo_all.shape, lambda i: (0, 0, 0)),
                  pl.BlockSpec(w_own.shape, lambda i: (0, 0)), act, act, pl.BlockSpec((1, d_model), lambda i: (0, 0))],
        out_specs=(act, act, pl.BlockSpec((heads, block, head_dim), lambda i: (0, i, 0)), pl.BlockSpec((1, d_model), lambda i: (0, 0))),
        compiler_params=pltpu.CompilerParams(vmem_limit_bytes=VMEM_LIMIT),
        cost_estimate=pl.CostEstimate(flops=2 * rows * d_model * (d_model + width), bytes_accessed=4 * d_model * d_model, transcendentals=rows),
        name="post",
    )(o_all, wo_all, w_own, x, gy, gain)


def chain_kernel(size, n_chunk, lag, part_ref, gy_ref, out_ref, sums_a, sums_b, rs_send, rs_recv, ag_send, ag_recv):
    me = lax.axis_index("tp")
    entry_barrier("tp", size)
    half = part_ref.shape[0] // 2
    rows = half // n_chunk
    last = size - 1

    def parts(side, chunk):
        local = pl.ds(pl.multiple_of(chunk * rows, rows), rows)
        glob = pl.ds(pl.multiple_of(side * half + chunk * rows, rows), rows)
        sums = (sums_a, sums_b)[side]
        return local, glob, sums

    def toward(side):
        return jnp.maximum(me - 1, 0) if side == 0 else jnp.minimum(me + 1, last)

    def away(side):
        return jnp.minimum(me + 1, last) if side == 0 else jnp.maximum(me - 1, 0)

    def rs_copy(side, chunk, first):
        local, glob, sums = parts(side, chunk)
        return pltpu.make_async_remote_copy(
            src_ref=part_ref.at[glob] if first else sums.at[local], dst_ref=sums.at[local],
            send_sem=rs_send.at[side, chunk], recv_sem=rs_recv.at[side, chunk],
            device_id={"tp": toward(side)}, device_id_type=MESH)

    def ag_copy(side, chunk):
        local, glob, sums = parts(side, chunk)
        return pltpu.make_async_remote_copy(
            src_ref=out_ref.at[glob], dst_ref=out_ref.at[glob],
            send_sem=ag_send.at[side, chunk], recv_sem=ag_recv.at[side, chunk],
            device_id={"tp": away(side)}, device_id_type=MESH)

    def place(side):
        return me if side == 0 else last - me

    def push(idx, carry):
        for side in (0, 1):
            @pl.when(place(side) == last)
            def _(side=side):
                rs_copy(side, idx, True).start()
        return carry

    lax.fori_loop(0, n_chunk, push, 0)

    def pass_on(side, chunk):
        local, glob, sums = parts(side, chunk)
        rs_copy(side, chunk, False).wait_recv()
        sums[local] = sums[local] + part_ref[glob]
        rs_copy(side, chunk, False).start()

    def finish(side, chunk):
        local, glob, sums = parts(side, chunk)
        rs_copy(side, chunk, False).wait_recv()
        out_ref[glob] = (gy_ref[glob].astype(jnp.float32) + (sums[local] + part_ref[glob])).astype(jnp.bfloat16)
        ag_copy(side, chunk).start()

    def reduce_step(idx, carry):
        for far in range(last - 1, 0, -1):
            chunk = idx - (last - 1 - far) * lag
            for side in (0, 1):
                @pl.when((chunk >= 0) & (chunk < n_chunk) & (place(side) == far))
                def _(side=side, chunk=chunk):
                    pass_on(side, chunk)
        for side in (0, 1):
            @pl.when((idx < n_chunk) & (place(side) == 0))
            def _(side=side):
                finish(side, idx)
        return carry

    lax.fori_loop(0, n_chunk + (last - 2) * lag, reduce_step, 0)

    def return_step(idx, carry):
        for far in range(1, last + 1):
            chunk = idx - (far - 1) * lag
            for side in (0, 1):
                @pl.when((chunk >= 0) & (chunk < n_chunk) & (place(side) == far))
                def _(side=side, chunk=chunk, far=far):
                    ag_copy(side, chunk).wait_recv()
                    if far < last:
                        ag_copy(side, chunk).start()
        return carry

    lax.fori_loop(0, n_chunk + (last - 1) * lag, return_step, 0)

    def drain(idx, carry):
        for side in (0, 1):
            @pl.when(place(side) > 0)
            def _(side=side):
                rs_copy(side, idx, False).wait_send()

            @pl.when(place(side) < last)
            def _(side=side):
                ag_copy(side, idx).wait_send()
        return carry

    lax.fori_loop(0, n_chunk, drain, 0)


def chain_sum(size, collective_id, part, gy):
    rows, d_model = part.shape
    n_chunk = 32 if rows >= 512 else 4
    sems = [pltpu.SemaphoreType.DMA((2, n_chunk))] * 4
    return pl.pallas_call(
        functools.partial(chain_kernel, size, n_chunk, 2),
        out_shape=jax.ShapeDtypeStruct((rows, d_model), jnp.bfloat16),
        in_specs=[VMEM_SPEC, VMEM_SPEC],
        out_specs=VMEM_SPEC,
        scratch_shapes=[pltpu.VMEM((rows // 2, d_model), jnp.float32), pltpu.VMEM((rows // 2, d_model), jnp.float32)] + sems,
        compiler_params=pltpu.CompilerParams(collective_id=collective_id, has_side_effects=True, vmem_limit_bytes=VMEM_LIMIT),
        cost_estimate=pl.CostEstimate(flops=10 ** 11, bytes_accessed=16 * rows * d_model, transcendentals=0),
        name="chain_sum",
    )(part, gy)


def solution(mesh):
    tp_size = mesh.shape["tp"]
    cp_size = mesh.shape["cp"]
    act_spec = P("dp", "cp", None)
    col_spec = P(None, "tp", None)
    part_col = P("dp", "tp", None)
    in_specs = (act_spec, col_spec, col_spec, col_spec, P("tp", None, None), P("tp", None), P("tp", None), P(None), act_spec)
    out_specs = (act_spec, act_spec, part_col, part_col, part_col, P(("dp", "tp"), None, None), P(("dp", "tp"), None), P(("dp", "tp"), None), P("dp"))
    swap_core = [(dev, dev ^ 1) for dev in range(cp_size)]

    def local_run(x_in, w_q, w_k, w_v, w_o, q_norm_w, k_norm_w, post_norm_w, grad_y):
        rows, d_model = x_in.shape[1:]
        heads, head_dim = w_q.shape[1:]
        width = heads * head_dim
        full_width = width * tp_size
        x = x_in[0]
        gy = grad_y[0]
        cp_index = lax.axis_index("cp")
        cos_tab, sin_tab = rope_tables(cp_index * rows, rows, head_dim)
        wq, wk, wv = (w.reshape(d_model, width) for w in (w_q, w_k, w_v))

        core = cp_index % 2
        own_half = lax.dynamic_slice_in_dim(w_o, core * (heads // 2), heads // 2, axis=0)
        mine = lax.all_gather(own_half, "tp")
        other = lax.ppermute(mine, "cp", swap_core)
        wo_all = jnp.where(core == 0, jnp.concatenate([mine, other], axis=1), jnp.concatenate([other, mine], axis=1))
        wo_all = wo_all.reshape(tp_size, width, d_model)

        def by_head(t):
            return t.reshape(rows, heads, head_dim).transpose(1, 0, 2)

        q_lin = jnp.dot(x, wq, preferred_element_type=jnp.float32)
        k_lin = jnp.dot(x, wk, preferred_element_type=jnp.float32)
        v_lin = jnp.dot(x, wv, preferred_element_type=jnp.float32)
        squares = jnp.stack([jnp.sum(q_lin * q_lin, axis=1), jnp.sum(k_lin * k_lin, axis=1)])
        squares = small_sum("tp", tp_size, 0, squares)
        invs = lax.rsqrt(squares / full_width + NORM_EPS)[:, :, None]
        q_hat = by_head(q_lin * invs[0])
        k_hat = by_head(k_lin * invs[1])
        q_gain = q_norm_w[:, None, :]
        k_gain = k_norm_w[:, None, :]
        q_rot = rope(q_hat * q_gain, cos_tab, sin_tab, 1.0).astype(jnp.bfloat16)
        k_rot = rope(k_hat * k_gain, cos_tab, sin_tab, 1.0).astype(jnp.bfloat16)
        v_val = by_head(v_lin.astype(jnp.bfloat16))

        seq_shape = (cp_size * rows, head_dim)
        block_shape = (cp_size, rows, head_dim)
        q_seq, k_seq, v_seq = (t.reshape(seq_shape) for t in exchange("cp", cp_size, 1, q_rot, k_rot, v_val))
        o_seq, lse = attend(q_seq, k_seq, v_seq)
        (o_heads,) = exchange("cp", cp_size, 2, o_seq.reshape(block_shape))
        o_mine = o_heads.transpose(1, 0, 2).reshape(rows, width)
        o_all = lax.all_gather(o_mine, "tp")
        y_out, grad_proj, grad_o, grad_post = post(o_all, wo_all, w_o.reshape(width, d_model), x, gy, post_norm_w[None, :], heads, head_dim)
        do_seq, dwo_part = exchange_product("cp", cp_size, 3, grad_o, o_mine, grad_proj)
        grad_w_o = lax.psum(dwo_part, "cp")

        dq_seq, dk_seq, dv_seq = attend_back(q_seq, k_seq, v_seq, o_seq, do_seq.reshape(seq_shape), lse)
        dq, dk, dv = exchange("cp", cp_size, 4, dq_seq.reshape(block_shape), dk_seq.reshape(block_shape), dv_seq.reshape(block_shape))

        def scaled_back(grad_rot, hat, gain):
            grad = rope(grad_rot, cos_tab, sin_tab, -1.0)
            grad_gain = jnp.sum(grad * hat, axis=1)
            grad_hat = grad * gain
            return grad_hat, grad_gain, jnp.sum(grad_hat * hat, axis=(0, 2))

        gq_hat, grad_q_norm, q_dot = scaled_back(dq, q_hat, q_gain)
        gk_hat, grad_k_norm, k_dot = scaled_back(dk, k_hat, k_gain)
        dots = small_sum("tp", tp_size, 5, jnp.stack([q_dot, k_dot])) / full_width

        def flat(t):
            return t.transpose(1, 0, 2).reshape(rows, width)

        dq16 = flat((invs[0][None] * (gq_hat - q_hat * dots[0][None, :, None])).astype(jnp.bfloat16))
        dk16 = flat((invs[1][None] * (gk_hat - k_hat * dots[1][None, :, None])).astype(jnp.bfloat16))
        dv16 = flat(dv)
        dw = tuple(lax.dot_general(x, g, TN, preferred_element_type=jnp.float32) for g in (dq16, dk16, dv16))
        dw, dq16, dk16, dv16 = lax.optimization_barrier((dw, dq16, dk16, dv16))
        dx_part = sum(lax.dot_general(g, w, NT, preferred_element_type=jnp.float32) for g, w in ((dq16, wq), (dk16, wk), (dv16, wv)))
        grad_w_o, *dw = lax.optimization_barrier((grad_w_o,) + tuple(dw))
        dw = lax.psum(tuple(dw), "cp")
        small = jnp.concatenate([grad_q_norm.reshape(1, width), grad_k_norm.reshape(1, width), grad_post], axis=1)
        small = small_sum("cp", cp_size, 7, small)
        dx_part, small = lax.optimization_barrier((dx_part, small))
        grad_x = chain_sum(tp_size, 6, dx_part, gy)
        grad_q_norm = small[0, :width].reshape(heads, head_dim)
        grad_k_norm = small[0, width:2 * width].reshape(heads, head_dim)
        grad_post = small[0, 2 * width:]
        dw = tuple(g.reshape(d_model, heads, head_dim) for g in lax.optimization_barrier(dw))
        return (y_out[None], grad_x[None]) + dw + (grad_w_o.reshape(heads, head_dim, d_model), grad_q_norm, grad_k_norm, grad_post)

    return jax.shard_map(local_run, mesh=mesh, in_specs=in_specs, out_specs=out_specs, check_vma=False)
```

```python
import functools

import jax
import jax.numpy as jnp
from jax import lax
from jax.experimental import pallas as pl
from jax.experimental.pallas import tpu as pltpu
from jax.sharding import PartitionSpec as P

ROPE_THETA = 500000.0
NORM_EPS = 1e-6
MASK_VALUE = -1e30
LOG2E = 1.4426950408889634
MESH = pl.DeviceIdType.MESH
VMEM_SPEC = pl.BlockSpec(memory_space=pltpu.VMEM)
VMEM_LIMIT = 60 * 1024 * 1024
NT = (((1,), (1,)), ((), ()))
TN = (((0,), (0,)), ((), ()))


def dot_nt(a, b):
    return lax.dot_general(a, b, NT, preferred_element_type=jnp.float32)


def dot_tn(a, b):
    return lax.dot_general(a, b, TN, preferred_element_type=jnp.float32)


def dot_nn(a, b):
    return jnp.dot(a, b, preferred_element_type=jnp.float32)


def rope_tables(positions, head_dim):
    half_dim = head_dim // 2
    inv_freq = ROPE_THETA ** (-2.0 * jnp.arange(half_dim, dtype=jnp.float32) / head_dim)
    angles = positions[:, None] * inv_freq[None, :]
    return jnp.cos(angles), jnp.sin(angles)


def rope(values, cos_tab, sin_tab):
    half_dim = values.shape[-1] // 2
    low_half = values[..., :half_dim]
    high_half = values[..., half_dim:]
    return jnp.concatenate([low_half * cos_tab - high_half * sin_tab, high_half * cos_tab + low_half * sin_tab], axis=-1)


def entry_barrier(axis, size):
    me = lax.axis_index(axis)
    barrier = pltpu.get_barrier_semaphore()
    for shift in range(1, size):
        pl.semaphore_signal(barrier, inc=1, device_id={axis: lax.rem(me + shift, size)}, device_id_type=MESH)
    pl.semaphore_wait(barrier, size - 1)


def exchange_kernel(axis, size, count, *refs):
    ins = refs[:count]
    outs = refs[count:2 * count]
    send_sem, recv_sem = refs[2 * count:]
    me = lax.axis_index(axis)
    entry_barrier(axis, size)
    copies = []
    for idx in range(count):
        for shift in (2, 1, 3) if size == 4 else range(1, size):
            dst = lax.rem(me + shift, size)
            copy = pltpu.make_async_remote_copy(
                src_ref=ins[idx].at[dst], dst_ref=outs[idx].at[me],
                send_sem=send_sem.at[idx, shift - 1], recv_sem=recv_sem.at[idx, shift - 1],
                device_id={axis: dst}, device_id_type=MESH)
            copy.start()
            copies.append(copy)
    for idx in range(count):
        outs[idx][me] = ins[idx][me]
    for copy in copies:
        copy.wait()


def exchange_product_kernel(axis, size, block, in_ref, a_ref, b_ref, out_ref, prod_ref, send_sem, recv_sem):
    me = lax.axis_index(axis)
    entry_barrier(axis, size)
    copies = []
    for shift in (2, 1, 3) if size == 4 else range(1, size):
        dst = lax.rem(me + shift, size)
        copy = pltpu.make_async_remote_copy(
            src_ref=in_ref.at[dst], dst_ref=out_ref.at[me], send_sem=send_sem.at[shift - 1], recv_sem=recv_sem.at[shift - 1],
            device_id={axis: dst}, device_id_type=MESH)
        copy.start()
        copies.append(copy)
    out_ref[me] = in_ref[me]

    def step(idx, carry):
        cols = pl.ds(pl.multiple_of(idx * block, block), block)
        prod_ref[:, cols] = dot_tn(a_ref[...], b_ref[:, cols])
        return carry

    lax.fori_loop(0, b_ref.shape[1] // block, step, 0)
    for copy in copies:
        copy.wait()


def exchange_product(axis, size, collective_id, array, a, b):
    return pl.pallas_call(
        functools.partial(exchange_product_kernel, axis, size, min(512, b.shape[1])),
        out_shape=(jax.ShapeDtypeStruct(array.shape, array.dtype), jax.ShapeDtypeStruct((a.shape[1], b.shape[1]), jnp.float32)),
        in_specs=[VMEM_SPEC] * 3,
        out_specs=(VMEM_SPEC, VMEM_SPEC),
        scratch_shapes=[pltpu.SemaphoreType.DMA((size - 1,)), pltpu.SemaphoreType.DMA((size - 1,))],
        compiler_params=pltpu.CompilerParams(collective_id=collective_id, has_side_effects=True, vmem_limit_bytes=VMEM_LIMIT),
        name="exchange_product",
    )(array, a, b)


def exchange(axis, size, collective_id, *arrays):
    count = len(arrays)
    return pl.pallas_call(
        functools.partial(exchange_kernel, axis, size, count),
        out_shape=tuple(jax.ShapeDtypeStruct(a.shape, a.dtype) for a in arrays),
        in_specs=[VMEM_SPEC] * count,
        out_specs=tuple([VMEM_SPEC] * count),
        scratch_shapes=[pltpu.SemaphoreType.DMA((count, size - 1)), pltpu.SemaphoreType.DMA((count, size - 1))],
        compiler_params=pltpu.CompilerParams(collective_id=collective_id, has_side_effects=True, vmem_limit_bytes=VMEM_LIMIT),
        name="exchange_" + str(collective_id),
    )(*arrays)


def sum_kernel(axis, size, in_ref, out_ref, slots, send_sem, recv_sem):
    me = lax.axis_index(axis)
    entry_barrier(axis, size)
    copies = []
    for shift in range(1, size):
        copy = pltpu.make_async_remote_copy(
            src_ref=in_ref, dst_ref=slots.at[me],
            send_sem=send_sem.at[shift - 1], recv_sem=recv_sem.at[shift - 1],
            device_id={axis: lax.rem(me + shift, size)}, device_id_type=MESH)
        copy.start()
        copies.append(copy)
    slots[me] = in_ref[...]
    for copy in copies:
        copy.wait()
    total = slots[0]
    for idx in range(1, size):
        total = total + slots[idx]
    out_ref[...] = total


def small_sum(axis, size, collective_id, array):
    return pl.pallas_call(
        functools.partial(sum_kernel, axis, size),
        out_shape=jax.ShapeDtypeStruct(array.shape, array.dtype),
        in_specs=[VMEM_SPEC],
        out_specs=VMEM_SPEC,
        scratch_shapes=[pltpu.VMEM((size,) + array.shape, array.dtype), pltpu.SemaphoreType.DMA((size - 1,)), pltpu.SemaphoreType.DMA((size - 1,))],
        compiler_params=pltpu.CompilerParams(collective_id=collective_id, has_side_effects=True),
        name="small_sum_" + str(collective_id),
    )(array)


def causal_mask(scores):
    key_pos = lax.broadcasted_iota(jnp.int32, scores.shape, 0)
    query_pos = lax.broadcasted_iota(jnp.int32, scores.shape, 1)
    return jnp.where(key_pos <= query_pos, scores, MASK_VALUE)


def attend_kernel(block, factor, q_ref, k_ref, v_ref, o_ref, lse_ref):
    blk = pl.program_id(0)
    q_blk = q_ref[...]

    def scores_of(idx):
        rows = pl.ds(pl.multiple_of(idx * block, block), block)
        return dot_nt(k_ref[rows, :], q_blk), v_ref[rows, :]

    scores, v_blk = scores_of(blk)
    scores = causal_mask(scores)
    top = jnp.max(scores, axis=0, keepdims=True)
    probs = jnp.exp2((scores - top) * factor)
    norm = jnp.sum(probs, axis=0, keepdims=True)
    acc = dot_tn(v_blk, probs.astype(jnp.bfloat16))

    def step(idx, state):
        top, norm, acc = state
        scores, v_blk = scores_of(idx)
        new_top = jnp.maximum(top, jnp.max(scores, axis=0, keepdims=True))
        probs = jnp.exp2((scores - new_top) * factor)
        rescale = jnp.exp2((top - new_top) * factor)
        norm = norm * rescale + jnp.sum(probs, axis=0, keepdims=True)
        acc = acc * rescale + dot_tn(v_blk, probs.astype(jnp.bfloat16))
        return new_top, norm, acc

    top, norm, acc = lax.fori_loop(0, blk, step, (top, norm, acc))
    o_ref[...] = (acc / norm).T.astype(jnp.bfloat16)
    lse_ref[...] = top * factor + jnp.log2(norm)


def attend(q, k, v):
    rows, head_dim = q.shape
    block = min(512, rows // 4)
    whole = pl.BlockSpec((rows, head_dim), lambda i: (0, 0))
    part = pl.BlockSpec((block, head_dim), lambda i: (i, 0))
    return pl.pallas_call(
        functools.partial(attend_kernel, block, head_dim ** -0.5 * LOG2E),
        grid=(rows // block,),
        out_shape=(jax.ShapeDtypeStruct(q.shape, jnp.bfloat16), jax.ShapeDtypeStruct((1, rows), jnp.float32)),
        in_specs=[part, whole, whole],
        out_specs=(part, pl.BlockSpec((1, block), lambda i: (0, i))),
        compiler_params=pltpu.CompilerParams(vmem_limit_bytes=VMEM_LIMIT),
        cost_estimate=pl.CostEstimate(flops=2 * rows * rows * head_dim, bytes_accessed=8 * rows * head_dim, transcendentals=rows * rows // 2),
        name="attend",
    )(q, k, v)


def attend_back_kernel(block, scale, q_ref, k_ref, v_ref, o_ref, do_ref, lse_ref, dq_ref, dk_ref, dv_ref, delta_ref, dk_acc, dv_acc):
    blk = pl.program_id(0)
    n_blk = pl.num_programs(0)
    factor = scale * LOG2E

    @pl.when(blk == 0)
    def _():
        def prepare(idx, carry):
            rows = pl.ds(pl.multiple_of(idx * block, block), block)
            prod = do_ref[rows, :].astype(jnp.float32) * o_ref[rows, :].astype(jnp.float32)
            delta_ref[:, rows] = jnp.sum(prod.T, axis=0, keepdims=True)
            dq_ref[rows, :] = jnp.zeros((block, dq_ref.shape[1]), jnp.float32)
            return carry
        lax.fori_loop(0, n_blk, prepare, 0)

    k_blk = k_ref[...]
    v_blk = v_ref[...]

    def one(idx, masked):
        rows = pl.ds(pl.multiple_of(idx * block, block), block)
        q_blk = q_ref[rows, :]
        do_blk = do_ref[rows, :]
        scores = dot_nt(k_blk, q_blk)
        if masked:
            scores = causal_mask(scores)
        probs = jnp.exp2(scores * factor - lse_ref[:, rows])
        grad_v = dot_nn(probs.astype(jnp.bfloat16), do_blk)
        grad_p = dot_nt(v_blk, do_blk)
        grad_s = (probs * ((grad_p - delta_ref[:, rows]) * scale)).astype(jnp.bfloat16)
        dq_ref[rows, :] += dot_tn(grad_s, k_blk)
        return dot_nn(grad_s, q_blk), grad_v

    dk_acc[...], dv_acc[...] = one(blk, True)

    def step(idx, carry):
        grad_k, grad_v = one(idx, False)
        dk_acc[...] += grad_k
        dv_acc[...] += grad_v
        return carry

    lax.fori_loop(blk + 1, n_blk, step, 0)
    dk_ref[...] = dk_acc[...]
    dv_ref[...] = dv_acc[...].astype(jnp.bfloat16)


def attend_back(q, k, v, o, do, lse):
    rows, head_dim = q.shape
    block = min(512, rows // 4)
    whole = pl.BlockSpec((rows, head_dim), lambda i: (0, 0))
    part = pl.BlockSpec((block, head_dim), lambda i: (i, 0))
    stat = pl.BlockSpec((1, rows), lambda i: (0, 0))
    return pl.pallas_call(
        functools.partial(attend_back_kernel, block, head_dim ** -0.5),
        grid=(rows // block,),
        out_shape=(jax.ShapeDtypeStruct(q.shape, jnp.float32), jax.ShapeDtypeStruct(q.shape, jnp.float32), jax.ShapeDtypeStruct(q.shape, jnp.bfloat16)),
        in_specs=[whole, part, part, whole, whole, stat],
        out_specs=(whole, part, part),
        scratch_shapes=[pltpu.VMEM((1, rows), jnp.float32), pltpu.VMEM((block, head_dim), jnp.float32), pltpu.VMEM((block, head_dim), jnp.float32)],
        compiler_params=pltpu.CompilerParams(vmem_limit_bytes=VMEM_LIMIT),
        cost_estimate=pl.CostEstimate(flops=5 * rows * rows * head_dim, bytes_accessed=20 * rows * head_dim, transcendentals=rows * rows // 2),
        name="attend_back",
    )(q, k, v, o, do, lse)


def post_kernel(tp_size, o_ref, wo_ref, wown_ref, x_ref, gy_ref, pw_ref, y_ref, gp_ref, do_ref, gpost_ref):
    proj = dot_nn(o_ref[0], wo_ref[0])
    for idx in range(1, tp_size):
        proj = proj + dot_nn(o_ref[idx], wo_ref[idx])
    gain = pw_ref[...]
    inv = lax.rsqrt(jnp.mean(proj * proj, axis=-1, keepdims=True) + NORM_EPS)
    hat = proj * inv
    y_ref[...] = (x_ref[...].astype(jnp.float32) + hat * gain).astype(jnp.bfloat16)
    grad = gy_ref[...].astype(jnp.float32)
    gpost = jnp.sum(grad * hat, axis=0, keepdims=True)
    grad_hat = grad * gain
    grad_proj = (inv * (grad_hat - hat * jnp.mean(grad_hat * hat, axis=-1, keepdims=True))).astype(jnp.bfloat16)
    gp_ref[...] = grad_proj
    grad_o = dot_nt(grad_proj, wown_ref[...]).astype(jnp.bfloat16)
    head_dim = do_ref.shape[2]
    for idx in range(do_ref.shape[0]):
        do_ref[idx] = grad_o[:, idx * head_dim:(idx + 1) * head_dim]

    @pl.when(pl.program_id(0) == 0)
    def _():
        gpost_ref[...] = jnp.zeros_like(gpost_ref)

    gpost_ref[...] += gpost


def post(o_all, wo_all, w_own, x, gy, gain, heads, head_dim):
    tp_size, rows, width = o_all.shape
    d_model = x.shape[1]
    block = min(256, rows)
    act = pl.BlockSpec((block, d_model), lambda i: (i, 0))
    return pl.pallas_call(
        functools.partial(post_kernel, tp_size),
        grid=(rows // block,),
        out_shape=(jax.ShapeDtypeStruct((rows, d_model), jnp.bfloat16), jax.ShapeDtypeStruct((rows, d_model), jnp.bfloat16),
                   jax.ShapeDtypeStruct((heads, rows, head_dim), jnp.bfloat16), jax.ShapeDtypeStruct((1, d_model), jnp.float32)),
        in_specs=[pl.BlockSpec((tp_size, block, width), lambda i: (0, i, 0)), pl.BlockSpec(wo_all.shape, lambda i: (0, 0, 0)),
                  pl.BlockSpec(w_own.shape, lambda i: (0, 0)), act, act, pl.BlockSpec((1, d_model), lambda i: (0, 0))],
        out_specs=(act, act, pl.BlockSpec((heads, block, head_dim), lambda i: (0, i, 0)), pl.BlockSpec((1, d_model), lambda i: (0, 0))),
        compiler_params=pltpu.CompilerParams(vmem_limit_bytes=VMEM_LIMIT),
        cost_estimate=pl.CostEstimate(flops=2 * rows * d_model * (d_model + width), bytes_accessed=4 * d_model * d_model, transcendentals=rows),
        name="post",
    )(o_all, wo_all, w_own, x, gy, gain)


def chain_kernel(size, n_chunk, lag, tile, dq_ref, dk_ref, dv_ref, wq_ref, wk_ref, wv_ref, gy_ref, out_ref, part_ref, sums_a, sums_b, rs_send, rs_recv, ag_send, ag_recv):
    me = lax.axis_index("tp")
    entry_barrier("tp", size)
    half = part_ref.shape[0] // 2
    rows = half // n_chunk
    last = size - 1

    def parts(side, chunk):
        local = pl.ds(pl.multiple_of(chunk * rows, rows), rows)
        glob = pl.ds(pl.multiple_of(side * half + chunk * rows, rows), rows)
        sums = (sums_a, sums_b)[side]
        return local, glob, sums

    def toward(side):
        return jnp.maximum(me - 1, 0) if side == 0 else jnp.minimum(me + 1, last)

    def away(side):
        return jnp.minimum(me + 1, last) if side == 0 else jnp.maximum(me - 1, 0)

    def rs_copy(side, chunk, first):
        local, glob, sums = parts(side, chunk)
        return pltpu.make_async_remote_copy(
            src_ref=part_ref.at[glob] if first else sums.at[local], dst_ref=sums.at[local],
            send_sem=rs_send.at[side, chunk], recv_sem=rs_recv.at[side, chunk],
            device_id={"tp": toward(side)}, device_id_type=MESH)

    def ag_copy(side, chunk):
        local, glob, sums = parts(side, chunk)
        return pltpu.make_async_remote_copy(
            src_ref=out_ref.at[glob], dst_ref=out_ref.at[glob],
            send_sem=ag_send.at[side, chunk], recv_sem=ag_recv.at[side, chunk],
            device_id={"tp": away(side)}, device_id_type=MESH)

    def place(side):
        return me if side == 0 else last - me

    heads = dq_ref.shape[0]
    d_model = out_ref.shape[1]
    block = min(512, d_model)
    n_tile = 2 * half // tile
    per_tile = tile // rows

    def push(number):
        for side in (0, 1):
            @pl.when((lax.rem(number, 2) == side) & (place(side) == last))
            def _(side=side):
                def one(idx, carry):
                    rs_copy(side, (number // 2) * per_tile + idx, True).start()
                    return carry
                lax.fori_loop(0, per_tile, one, 0)

    def product(number, carry):
        tile_rows = pl.ds(pl.multiple_of(lax.rem(number, 2) * half + (number // 2) * tile, tile), tile)

        def columns(idx, carry):
            cols = pl.ds(pl.multiple_of(idx * block, block), block)
            total = None
            for grad_ref, w_ref in ((dq_ref, wq_ref), (dk_ref, wk_ref), (dv_ref, wv_ref)):
                grad = jnp.concatenate([grad_ref[idx_h, tile_rows, :] for idx_h in range(heads)], axis=1)
                term = dot_nn(grad, w_ref[:, cols])
                total = term if total is None else total + term
            part_ref[tile_rows, cols] = total
            return carry

        lax.fori_loop(0, d_model // block, columns, 0)

        @pl.when(number > 0)
        def _():
            push(number - 1)
        return carry

    lax.fori_loop(0, n_tile, product, 0)
    push(jnp.int32(n_tile - 1))

    def pass_on(side, chunk):
        local, glob, sums = parts(side, chunk)
        rs_copy(side, chunk, False).wait_recv()
        sums[local] = sums[local] + part_ref[glob]
        rs_copy(side, chunk, False).start()

    def finish(side, chunk):
        local, glob, sums = parts(side, chunk)
        rs_copy(side, chunk, False).wait_recv()
        out_ref[glob] = (gy_ref[glob].astype(jnp.float32) + (sums[local] + part_ref[glob])).astype(jnp.bfloat16)
        ag_copy(side, chunk).start()

    def reduce_step(idx, carry):
        for far in range(last - 1, 0, -1):
            chunk = idx - (last - 1 - far) * lag
            for side in (0, 1):
                @pl.when((chunk >= 0) & (chunk < n_chunk) & (place(side) == far))
                def _(side=side, chunk=chunk):
                    pass_on(side, chunk)
        for side in (0, 1):
            @pl.when((idx < n_chunk) & (place(side) == 0))
            def _(side=side):
                finish(side, idx)
        return carry

    lax.fori_loop(0, n_chunk + (last - 2) * lag, reduce_step, 0)

    def return_step(idx, carry):
        for far in range(1, last + 1):
            chunk = idx - (far - 1) * lag
            for side in (0, 1):
                @pl.when((chunk >= 0) & (chunk < n_chunk) & (place(side) == far))
                def _(side=side, chunk=chunk, far=far):
                    ag_copy(side, chunk).wait_recv()
                    if far < last:
                        ag_copy(side, chunk).start()
        return carry

    lax.fori_loop(0, n_chunk + (last - 1) * lag, return_step, 0)

    def drain(idx, carry):
        for side in (0, 1):
            @pl.when(place(side) > 0)
            def _(side=side):
                rs_copy(side, idx, False).wait_send()

            @pl.when(place(side) < last)
            def _(side=side):
                ag_copy(side, idx).wait_send()
        return carry

    lax.fori_loop(0, n_chunk, drain, 0)


def chain_sum(size, collective_id, grads, weights, gy):
    rows, d_model = gy.shape
    n_chunk = 32 if rows >= 512 else 4
    sems = [pltpu.SemaphoreType.DMA((2, n_chunk))] * 4
    return pl.pallas_call(
        functools.partial(chain_kernel, size, n_chunk, 2, min(256, rows // 4)),
        out_shape=jax.ShapeDtypeStruct((rows, d_model), jnp.bfloat16),
        in_specs=[VMEM_SPEC] * 7,
        out_specs=VMEM_SPEC,
        scratch_shapes=[pltpu.VMEM((rows, d_model), jnp.float32), pltpu.VMEM((rows // 2, d_model), jnp.float32), pltpu.VMEM((rows // 2, d_model), jnp.float32)] + sems,
        compiler_params=pltpu.CompilerParams(collective_id=collective_id, has_side_effects=True, vmem_limit_bytes=VMEM_LIMIT),
        cost_estimate=pl.CostEstimate(flops=10 ** 11, bytes_accessed=16 * rows * d_model, transcendentals=0),
        name="chain_sum",
    )(*grads, *weights, gy)


def flip(index, distance):
    if distance == 1:
        return index + 1 - 2 * lax.rem(index, 2)
    if distance == 2:
        return lax.rem(index + 2, 4)
    return 3 - index if distance == 3 else index


def weights_back_kernel(tp_size, full_width, sub, x0, x1, x2, x3, wqk_ref, dq_ref, dk_ref, dv_ref, cos_ref, sin_ref, qg_ref, kg_ref,
                        dwq_ref, dwk_ref, dwv_ref, exq_ref, exk_ref, exv_ref, gq_ref, gk_ref,
                        x_buf, lin_ref, q16_ref, k16_ref, own, slots_tp, mid, slots_cp, total, x_sem, tp_send, tp_recv, cp_send, cp_recv, ex_send, ex_recv):
    me = lax.axis_index("cp")
    my_tp = lax.axis_index("tp")
    rows, head_dim = dq_ref.shape[1:]
    loads = []
    for dist, x_ref in enumerate((x0, x1, x2, x3)):
        load = pltpu.make_async_copy(x_ref, x_buf.at[dist], x_sem.at[dist])
        load.start()
        loads.append(load)
    barrier = pltpu.get_barrier_semaphore()
    for dist in (1, 2, 3):
        pl.semaphore_signal(barrier, inc=1, device_id={"cp": flip(me, dist)}, device_id_type=MESH)
    for shift in range(1, tp_size):
        pl.semaphore_signal(barrier, inc=1, device_id={"tp": lax.rem(my_tp + shift, tp_size)}, device_id_type=MESH)
    pl.semaphore_wait(barrier, 3 + tp_size - 1)

    def ex_copy(idx, src, dst, dist):
        peer = flip(me, dist)
        return pltpu.make_async_remote_copy(
            src_ref=src.at[peer], dst_ref=dst.at[me], send_sem=ex_send.at[idx, dist - 1], recv_sem=ex_recv.at[idx, dist - 1],
            device_id={"cp": peer}, device_id_type=MESH)

    copies = [ex_copy(2, dv_ref, exv_ref, dist) for dist in (2, 3, 1)]
    for copy in copies:
        copy.start()

    def grad_of(ref, blk, part, table):
        g = ref[blk, part, :]
        half_dim = head_dim // 2
        turned = jnp.concatenate([g[:, half_dim:], g[:, :half_dim]], axis=1)
        return g * cos_ref[table, :] - turned * sin_ref[table, :]

    sides = ((dq_ref, qg_ref, 0), (dk_ref, kg_ref, 1))
    for dist in range(4):
        blk = flip(me, dist)
        loads[dist].wait()

        def first(idx, carry, dist=dist, blk=blk):
            part = pl.ds(pl.multiple_of(idx * sub, sub), sub)
            table = pl.ds(pl.multiple_of(blk * rows + idx * sub, sub), sub)
            lin = dot_nn(x_buf[dist, part, :], wqk_ref[...])
            lin_ref[dist, part, :] = lin
            for ref, gain_ref, number in sides:
                mine = lin[:, number * head_dim:(number + 1) * head_dim]
                grad = grad_of(ref, blk, part, table) * gain_ref[...]
                own[2 * number:2 * number + 1, table] = jnp.sum((mine * mine).T, axis=0, keepdims=True)
                own[2 * number + 1:2 * number + 2, table] = jnp.sum((grad * mine).T, axis=0, keepdims=True)
            return carry

        lax.fori_loop(0, rows // sub, first, 0)

    moves = []
    for shift in range(1, tp_size):
        move = pltpu.make_async_remote_copy(
            src_ref=own, dst_ref=slots_tp.at[my_tp], send_sem=tp_send.at[shift - 1], recv_sem=tp_recv.at[shift - 1],
            device_id={"tp": lax.rem(my_tp + shift, tp_size)}, device_id_type=MESH)
        move.start()
        moves.append(move)
    slots_tp[my_tp] = own[...]
    for move in moves:
        move.wait()
    acc = slots_tp[0]
    for idx in range(1, tp_size):
        acc = acc + slots_tp[idx]
    mid[...] = acc
    moves = []
    for dist in (2, 3, 1):
        move = pltpu.make_async_remote_copy(
            src_ref=mid, dst_ref=slots_cp.at[me], send_sem=cp_send.at[dist - 1], recv_sem=cp_recv.at[dist - 1],
            device_id={"cp": flip(me, dist)}, device_id_type=MESH)
        move.start()
        moves.append(move)
    slots_cp[me] = mid[...]
    for move in moves:
        move.wait()
    total[...] = slots_cp[0] + slots_cp[1] + slots_cp[2] + slots_cp[3]

    gq_ref[...] = jnp.zeros_like(gq_ref)
    gk_ref[...] = jnp.zeros_like(gk_ref)
    outs = ((q16_ref, exq_ref, gq_ref), (k16_ref, exk_ref, gk_ref))
    for dist in (2, 3, 1, 0):
        blk = flip(me, dist)

        def second(idx, carry, dist=dist, blk=blk):
            part = pl.ds(pl.multiple_of(idx * sub, sub), sub)
            table = pl.ds(pl.multiple_of(blk * rows + idx * sub, sub), sub)
            lin = lin_ref[dist, part, :]
            for (ref, gain_ref, number), (d16_ref, _, gain_out) in zip(sides, outs):
                mine = lin[:, number * head_dim:(number + 1) * head_dim]
                inv = lax.rsqrt(total[2 * number:2 * number + 1, table] / full_width + NORM_EPS)
                dot = inv * total[2 * number + 1:2 * number + 2, table] / full_width
                inv = jnp.broadcast_to(inv, (head_dim, sub)).T
                dot = jnp.broadcast_to(dot, (head_dim, sub)).T
                raw = grad_of(ref, blk, part, table)
                hat = mine * inv
                d16_ref[blk, part, :] = (inv * (raw * gain_ref[...] - hat * dot)).astype(jnp.bfloat16)
                gain_out[...] += jnp.sum(raw * hat, axis=0, keepdims=True)
            return carry

        lax.fori_loop(0, rows // sub, second, 0)
        if dist:
            for idx, (d16_ref, ex_ref, _) in enumerate(outs):
                copy = ex_copy(idx, d16_ref, ex_ref, dist)
                copy.start()
                copies.append(copy)
    for src, dst in ((q16_ref, exq_ref), (k16_ref, exk_ref), (dv_ref, exv_ref)):
        dst[me] = src[me]

    block = min(512, x_buf.shape[2])

    def weight_step(idx, carry):
        cols = pl.ds(pl.multiple_of(idx * block, block), block)
        acc = None
        for dist in range(4):
            blk = flip(me, dist)
            grads = jnp.concatenate([q16_ref[blk], k16_ref[blk], dv_ref[blk]], axis=1)
            term = dot_tn(grads, x_buf[dist, :, cols])
            acc = term if acc is None else acc + term
        acc = acc.T
        for number, out in enumerate((dwq_ref, dwk_ref, dwv_ref)):
            out[cols, :] = acc[:, number * head_dim:(number + 1) * head_dim]
        return carry

    lax.fori_loop(0, x_buf.shape[2] // block, weight_step, 0)
    for copy in copies:
        copy.wait()


def weights_back(tp_size, collective_id, full_width, xs, wqk, dq, dk, dv, cos_tab, sin_tab, q_gain, k_gain):
    _, rows, head_dim = dq.shape
    d_model = xs[0].shape[1]
    any_spec = pl.BlockSpec(memory_space=pl.ANY)
    dma = pltpu.SemaphoreType.DMA
    stat = pltpu.VMEM((4, 4 * rows), jnp.float32)
    dw = jax.ShapeDtypeStruct((d_model, head_dim), jnp.float32)
    ex = jax.ShapeDtypeStruct(dq.shape, jnp.bfloat16)
    gain = jax.ShapeDtypeStruct((1, head_dim), jnp.float32)
    return pl.pallas_call(
        functools.partial(weights_back_kernel, tp_size, full_width, min(256, rows)),
        out_shape=(dw, dw, dw, ex, ex, ex, gain, gain),
        in_specs=[any_spec] * 4 + [VMEM_SPEC] * 8,
        out_specs=tuple([VMEM_SPEC] * 8),
        scratch_shapes=[pltpu.VMEM((4, rows, d_model), jnp.bfloat16), pltpu.VMEM((4, rows, 2 * head_dim), jnp.float32),
                        pltpu.VMEM(dq.shape, jnp.bfloat16), pltpu.VMEM(dq.shape, jnp.bfloat16),
                        stat, pltpu.VMEM((tp_size, 4, 4 * rows), jnp.float32), stat, pltpu.VMEM((4, 4, 4 * rows), jnp.float32), stat,
                        dma((4,)), dma((tp_size - 1,)), dma((tp_size - 1,)), dma((3,)), dma((3,)), dma((3, 3)), dma((3, 3))],
        compiler_params=pltpu.CompilerParams(collective_id=collective_id, has_side_effects=True, vmem_limit_bytes=VMEM_LIMIT),
        name="weights_back",
    )(*xs, wqk, dq, dk, dv, cos_tab, sin_tab, q_gain, k_gain)


def solution(mesh):
    tp_size = mesh.shape["tp"]
    cp_size = mesh.shape["cp"]
    act_spec = P("dp", "cp", None)
    col_spec = P(None, "tp", None)
    part_col = P("dp", "tp", None)
    in_specs = (act_spec, col_spec, col_spec, col_spec, P("tp", None, None), P("tp", None), P("tp", None), P(None), act_spec)
    out_specs = (act_spec, act_spec, part_col, part_col, part_col, P(("dp", "tp"), None, None), P(("dp", "tp"), None), P(("dp", "tp"), None), P("dp"))
    swap_core = [(dev, dev ^ 1) for dev in range(cp_size)]

    def local_run(x_in, w_q, w_k, w_v, w_o, q_norm_w, k_norm_w, post_norm_w, grad_y):
        rows, d_model = x_in.shape[1:]
        heads, head_dim = w_q.shape[1:]
        width = heads * head_dim
        full_width = width * tp_size
        x = x_in[0]
        gy = grad_y[0]
        cp_index = lax.axis_index("cp")
        cos_tab, sin_tab = rope_tables((cp_index * rows + jnp.arange(rows)).astype(jnp.float32), head_dim)
        wq, wk, wv = (w.reshape(d_model, width) for w in (w_q, w_k, w_v))

        core = cp_index % 2
        own_half = lax.dynamic_slice_in_dim(w_o, core * (heads // 2), heads // 2, axis=0)
        mine = lax.all_gather(own_half, "tp")
        other = lax.ppermute(mine, "cp", swap_core)
        wo_all = jnp.where(core == 0, jnp.concatenate([mine, other], axis=1), jnp.concatenate([other, mine], axis=1))
        wo_all = wo_all.reshape(tp_size, width, d_model)

        def by_head(t):
            return t.reshape(rows, heads, head_dim).transpose(1, 0, 2)

        q_lin = jnp.dot(x, wq, preferred_element_type=jnp.float32)
        k_lin = jnp.dot(x, wk, preferred_element_type=jnp.float32)
        v_lin = jnp.dot(x, wv, preferred_element_type=jnp.float32)
        squares = jnp.stack([jnp.sum(q_lin * q_lin, axis=1), jnp.sum(k_lin * k_lin, axis=1)])
        squares = small_sum("tp", tp_size, 0, squares)
        invs = lax.rsqrt(squares / full_width + NORM_EPS)[:, :, None]
        q_hat = by_head(q_lin * invs[0])
        k_hat = by_head(k_lin * invs[1])
        q_gain = q_norm_w[:, None, :]
        k_gain = k_norm_w[:, None, :]
        q_rot = rope(q_hat * q_gain, cos_tab, sin_tab).astype(jnp.bfloat16)
        k_rot = rope(k_hat * k_gain, cos_tab, sin_tab).astype(jnp.bfloat16)
        v_val = by_head(v_lin.astype(jnp.bfloat16))

        seq_shape = (cp_size * rows, head_dim)
        block_shape = (cp_size, rows, head_dim)
        q_seq, k_seq, v_seq = (t.reshape(seq_shape) for t in exchange("cp", cp_size, 1, q_rot, k_rot, v_val))
        o_seq, lse = attend(q_seq, k_seq, v_seq)
        (o_heads,) = exchange("cp", cp_size, 2, o_seq.reshape(block_shape))
        positions = jnp.arange(cp_size * rows, dtype=jnp.float32)
        o_heads, x_send, positions, w_q2, w_k2, w_v2 = lax.optimization_barrier((o_heads, x, positions, w_q, w_k, w_v))
        x_far = lax.ppermute(x_send, "cp", [(dev, dev ^ 2) for dev in range(cp_size)])
        x_near = lax.ppermute(x_send, "cp", swap_core)
        x_cross = lax.ppermute(x_far, "cp", swap_core)
        seq_cos, seq_sin = rope_tables(positions, head_dim)
        seq_cos = jnp.concatenate([seq_cos, seq_cos], axis=1)
        seq_sin = jnp.concatenate([-seq_sin, seq_sin], axis=1)
        turned = tuple(w.reshape(d_model, width).T for w in (w_q2, w_k2, w_v2))
        wqk_head = jnp.concatenate([lax.dynamic_slice_in_dim(w, cp_index, 1, axis=1)[:, 0, :] for w in (w_q2, w_k2)], axis=1)
        gains_head = tuple(lax.dynamic_slice_in_dim(w, cp_index, 1, axis=0) for w in (q_norm_w, k_norm_w))
        o_mine = o_heads.transpose(1, 0, 2).reshape(rows, width)
        o_all = lax.all_gather(o_mine, "tp")
        y_out, grad_proj, grad_o, grad_post = post(o_all, wo_all, w_o.reshape(width, d_model), x, gy, post_norm_w[None, :], heads, head_dim)
        do_seq, dwo_part = exchange_product("cp", cp_size, 3, grad_o, o_mine, grad_proj)
        grad_w_o = lax.psum(dwo_part, "cp")

        dq_seq, dk_seq, dv_seq = attend_back(q_seq, k_seq, v_seq, o_seq, do_seq.reshape(seq_shape), lse)
        *dw, dq16, dk16, dv16, gain_q, gain_k = weights_back(
            tp_size, 4, full_width, (x, x_near, x_far, x_cross), wqk_head,
            dq_seq.reshape(block_shape), dk_seq.reshape(block_shape), dv_seq.reshape(block_shape), seq_cos, seq_sin, *gains_head)
        dw = lax.all_gather(jnp.stack(dw), "cp")
        own_head = jnp.arange(heads)[:, None] == cp_index
        small = jnp.concatenate([jnp.where(own_head, gain, 0.0).reshape(1, width) for gain in (gain_q, gain_k)] + [grad_post], axis=1)
        small = small_sum("cp", cp_size, 7, small)
        dq16, small = lax.optimization_barrier((dq16, small))
        grad_x = chain_sum(tp_size, 6, (dq16, dk16, dv16), turned, gy)
        grad_q_norm = small[0, :width].reshape(heads, head_dim)
        grad_k_norm = small[0, width:2 * width].reshape(heads, head_dim)
        grad_post = small[0, 2 * width:]
        dw = tuple(dw[:, number].transpose(1, 0, 2) for number in range(3))
        return (y_out[None], grad_x[None]) + dw + (grad_w_o.reshape(heads, head_dim, d_model), grad_q_norm, grad_k_norm, grad_post)

    return jax.shard_map(local_run, mesh=mesh, in_specs=in_specs, out_specs=out_specs, check_vma=False)
```

```python
import functools

import jax
import jax.numpy as jnp
from jax import lax
from jax.experimental import pallas as pl
from jax.experimental.pallas import tpu as pltpu
from jax.sharding import PartitionSpec as P


ROPE_THETA = 500000.0
NORM_EPS = 1e-6
MASK_VALUE = -1e30
LOG2E = 1.4426950408889634
MESH = pl.DeviceIdType.MESH
VMEM_SPEC = pl.BlockSpec(memory_space=pltpu.VMEM)
VMEM_LIMIT = 60 * 1024 * 1024
NT = (((1,), (1,)), ((), ()))
TN = (((0,), (0,)), ((), ()))


def dot_nt(a, b):
    return lax.dot_general(a, b, NT, preferred_element_type=jnp.float32)


def dot_tn(a, b):
    return lax.dot_general(a, b, TN, preferred_element_type=jnp.float32)


def dot_nn(a, b):
    return jnp.dot(a, b, preferred_element_type=jnp.float32)


def rope_tables(positions, head_dim):
    half_dim = head_dim // 2
    inv_freq = ROPE_THETA ** (-2.0 * jnp.arange(half_dim, dtype=jnp.float32) / head_dim)
    angles = positions[:, None] * inv_freq[None, :]
    return jnp.cos(angles), jnp.sin(angles)


def rope(values, cos_tab, sin_tab):
    half_dim = values.shape[-1] // 2
    low_half = values[..., :half_dim]
    high_half = values[..., half_dim:]
    return jnp.concatenate([low_half * cos_tab - high_half * sin_tab, high_half * cos_tab + low_half * sin_tab], axis=-1)


def entry_barrier(axis, size):
    me = lax.axis_index(axis)
    barrier = pltpu.get_barrier_semaphore()
    for shift in range(1, size):
        pl.semaphore_signal(barrier, inc=1, device_id={axis: lax.rem(me + shift, size)}, device_id_type=MESH)
    pl.semaphore_wait(barrier, size - 1)


def exchange_kernel(axis, size, count, *refs):
    ins = refs[:count]
    outs = refs[count:2 * count]
    send_sem, recv_sem = refs[2 * count:]
    me = lax.axis_index(axis)
    entry_barrier(axis, size)
    copies = []
    for idx in range(count):
        for shift in (2, 1, 3) if size == 4 else range(1, size):
            dst = lax.rem(me + shift, size)
            copy = pltpu.make_async_remote_copy(
                src_ref=ins[idx].at[dst], dst_ref=outs[idx].at[me],
                send_sem=send_sem.at[idx, shift - 1], recv_sem=recv_sem.at[idx, shift - 1],
                device_id={axis: dst}, device_id_type=MESH)
            copy.start()
            copies.append(copy)
    for idx in range(count):
        outs[idx][me] = ins[idx][me]
    for copy in copies:
        copy.wait()


def peers_barrier():
    me, my_tp = lax.axis_index("cp"), lax.axis_index("tp")
    barrier = pltpu.get_barrier_semaphore()
    for shift in (1, 2, 3):
        pl.semaphore_signal(barrier, inc=1, device_id={"cp": lax.rem(me + shift, 4)}, device_id_type=MESH)
        pl.semaphore_signal(barrier, inc=1, device_id={"tp": lax.rem(my_tp + shift, 4)}, device_id_type=MESH)
    pl.semaphore_wait(barrier, 6)


def flip(index, distance):
    if distance == 1:
        return index + 1 - 2 * lax.rem(index, 2)
    if distance == 2:
        return lax.rem(index + 2, 4)
    return 3 - index if distance == 3 else index


def heads_to_tokens_kernel(in_ref, heads_ref, tokens_ref, cp_send, cp_recv, tp_send, tp_recv):
    me, my_tp = lax.axis_index("cp"), lax.axis_index("tp")
    quarter = in_ref.shape[1] // 4
    peers_barrier()
    first = {}
    for dist in (1, 2, 3):
        peer = flip(me, dist)
        first[dist] = pltpu.make_async_remote_copy(
            src_ref=in_ref.at[peer], dst_ref=heads_ref.at[me], send_sem=cp_send.at[dist - 1], recv_sem=cp_recv.at[dist - 1],
            device_id={"cp": peer}, device_id_type=MESH)
        first[dist].start()

    def rows_of(which):
        return pl.ds(pl.multiple_of(which * quarter, quarter), quarter)

    second = []

    def forward(dist, src_ref, head):
        for shift in (2, 1, 3):
            peer = lax.rem(my_tp + shift, 4)
            copy = pltpu.make_async_remote_copy(
                src_ref=src_ref.at[head, rows_of(peer)], dst_ref=tokens_ref.at[my_tp, head],
                send_sem=tp_send.at[dist, shift - 1], recv_sem=tp_recv.at[dist, shift - 1],
                device_id={"tp": peer}, device_id_type=MESH)
            copy.start()
            second.append(copy)
        tokens_ref[my_tp, head] = src_ref[head, rows_of(my_tp)]

    forward(0, in_ref, me)
    heads_ref[me] = in_ref[me]
    for dist in (1, 2, 3):
        first[dist].wait_recv()
        forward(dist, heads_ref, flip(me, dist))
    for dist in (1, 2, 3):
        first[dist].wait_send()
    for copy in second:
        copy.wait()


def heads_to_tokens(collective_id, array):
    _, rows, head_dim = array.shape
    dma = pltpu.SemaphoreType.DMA
    return pl.pallas_call(
        heads_to_tokens_kernel,
        out_shape=(jax.ShapeDtypeStruct(array.shape, array.dtype), jax.ShapeDtypeStruct((4, 4, rows // 4, head_dim), array.dtype)),
        in_specs=[VMEM_SPEC],
        out_specs=(VMEM_SPEC, VMEM_SPEC),
        scratch_shapes=[dma((3,)), dma((3,)), dma((4, 3)), dma((4, 3))],
        compiler_params=pltpu.CompilerParams(collective_id=collective_id, has_side_effects=True, vmem_limit_bytes=VMEM_LIMIT),
        name="heads_to_tokens",
    )(array)


def tokens_to_heads_kernel(in_ref, seq_ref, block_ref, tp_send, tp_recv, cp_send, cp_recv):
    me, my_tp = lax.axis_index("cp"), lax.axis_index("tp")
    quarter = in_ref.shape[2]
    peers_barrier()
    first = {}
    for shift in (2, 1, 3):
        peer = lax.rem(my_tp + shift, 4)
        first[shift] = pltpu.make_async_remote_copy(
            src_ref=in_ref.at[peer], dst_ref=block_ref.at[my_tp], send_sem=tp_send.at[shift - 1], recv_sem=tp_recv.at[shift - 1],
            device_id={"tp": peer}, device_id_type=MESH)
        first[shift].start()
    second = []

    def forward(shift, src_ref, which):
        rows = pl.ds(pl.multiple_of(which * quarter, quarter), quarter)
        for dist in (2, 3, 1):
            peer = flip(me, dist)
            copy = pltpu.make_async_remote_copy(
                src_ref=src_ref.at[which, peer], dst_ref=seq_ref.at[me, rows],
                send_sem=cp_send.at[shift, dist - 1], recv_sem=cp_recv.at[shift, dist - 1],
                device_id={"cp": peer}, device_id_type=MESH)
            second.append(copy)
            copy.start()
        seq_ref[me, rows] = src_ref[which, me]

    forward(0, in_ref, my_tp)
    for shift in (1, 3, 2):
        first[shift].wait_recv()
        forward(shift, block_ref, lax.rem(my_tp + 4 - shift, 4))
    for shift in (1, 2, 3):
        first[shift].wait_send()
    for copy in second:
        copy.wait_send()
    for copy in second:
        copy.wait_recv()


def tokens_to_heads(collective_id, array):
    tp, heads, quarter, head_dim = array.shape
    dma = pltpu.SemaphoreType.DMA
    return pl.pallas_call(
        tokens_to_heads_kernel,
        out_shape=jax.ShapeDtypeStruct((heads, tp * quarter, head_dim), array.dtype),
        in_specs=[VMEM_SPEC],
        out_specs=VMEM_SPEC,
        scratch_shapes=[pltpu.VMEM(array.shape, array.dtype), dma((3,)), dma((3,)), dma((4, 3)), dma((4, 3))],
        compiler_params=pltpu.CompilerParams(collective_id=collective_id, has_side_effects=True, vmem_limit_bytes=VMEM_LIMIT),
        name="tokens_to_heads",
    )(array)


def exchange(axis, size, collective_id, *arrays):
    count = len(arrays)
    return pl.pallas_call(
        functools.partial(exchange_kernel, axis, size, count),
        out_shape=tuple(jax.ShapeDtypeStruct(a.shape, a.dtype) for a in arrays),
        in_specs=[VMEM_SPEC] * count,
        out_specs=tuple([VMEM_SPEC] * count),
        scratch_shapes=[pltpu.SemaphoreType.DMA((count, size - 1)), pltpu.SemaphoreType.DMA((count, size - 1))],
        compiler_params=pltpu.CompilerParams(collective_id=collective_id, has_side_effects=True, vmem_limit_bytes=VMEM_LIMIT),
    )(*arrays)


def sum_kernel(axis, size, in_ref, out_ref, slots, send_sem, recv_sem):
    me = lax.axis_index(axis)
    entry_barrier(axis, size)
    copies = []
    for shift in range(1, size):
        copy = pltpu.make_async_remote_copy(
            src_ref=in_ref, dst_ref=slots.at[me],
            send_sem=send_sem.at[shift - 1], recv_sem=recv_sem.at[shift - 1],
            device_id={axis: lax.rem(me + shift, size)}, device_id_type=MESH)
        copy.start()
        copies.append(copy)
    slots[me] = in_ref[...]
    for copy in copies:
        copy.wait()
    total = slots[0]
    for idx in range(1, size):
        total = total + slots[idx]
    out_ref[...] = total


def small_sum(axis, size, collective_id, array):
    return pl.pallas_call(
        functools.partial(sum_kernel, axis, size),
        out_shape=jax.ShapeDtypeStruct(array.shape, array.dtype),
        in_specs=[VMEM_SPEC],
        out_specs=VMEM_SPEC,
        scratch_shapes=[pltpu.VMEM((size,) + array.shape, array.dtype), pltpu.SemaphoreType.DMA((size - 1,)), pltpu.SemaphoreType.DMA((size - 1,))],
        compiler_params=pltpu.CompilerParams(collective_id=collective_id, has_side_effects=True),
    )(array)


def causal_mask(scores):
    key_pos = lax.broadcasted_iota(jnp.int32, scores.shape, 0)
    query_pos = lax.broadcasted_iota(jnp.int32, scores.shape, 1)
    return jnp.where(key_pos <= query_pos, scores, MASK_VALUE)


def attend_kernel(block, factor, q_ref, k_ref, v_ref, o_ref, lse_ref):
    blk = pl.program_id(0)
    q_blk = q_ref[...]

    def scores_of(idx):
        rows = pl.ds(pl.multiple_of(idx * block, block), block)
        return dot_nt(k_ref[rows, :], q_blk), v_ref[rows, :]

    scores, v_blk = scores_of(blk)
    scores = causal_mask(scores)
    top = jnp.max(scores, axis=0, keepdims=True)
    probs = jnp.exp2((scores - top) * factor)
    norm = jnp.sum(probs, axis=0, keepdims=True)
    acc = dot_tn(v_blk, probs.astype(jnp.bfloat16))

    def step(idx, state):
        top, norm, acc = state
        scores, v_blk = scores_of(idx)
        new_top = jnp.maximum(top, jnp.max(scores, axis=0, keepdims=True))
        probs = jnp.exp2((scores - new_top) * factor)
        rescale = jnp.exp2((top - new_top) * factor)
        norm = norm * rescale + jnp.sum(probs, axis=0, keepdims=True)
        acc = acc * rescale + dot_tn(v_blk, probs.astype(jnp.bfloat16))
        return new_top, norm, acc

    top, norm, acc = lax.fori_loop(0, blk, step, (top, norm, acc))
    o_ref[...] = (acc / norm).T.astype(jnp.bfloat16)
    lse_ref[...] = top * factor + jnp.log2(norm)


def attend(q, k, v):
    rows, head_dim = q.shape
    block = min(512, rows // 4)
    whole = pl.BlockSpec((rows, head_dim), lambda i: (0, 0))
    part = pl.BlockSpec((block, head_dim), lambda i: (i, 0))
    return pl.pallas_call(
        functools.partial(attend_kernel, block, head_dim ** -0.5 * LOG2E),
        grid=(rows // block,),
        out_shape=(jax.ShapeDtypeStruct(q.shape, jnp.bfloat16), jax.ShapeDtypeStruct((1, rows), jnp.float32)),
        in_specs=[part, whole, whole],
        out_specs=(part, pl.BlockSpec((1, block), lambda i: (0, i))),
        compiler_params=pltpu.CompilerParams(vmem_limit_bytes=VMEM_LIMIT),
        cost_estimate=pl.CostEstimate(flops=2 * rows * rows * head_dim, bytes_accessed=8 * rows * head_dim, transcendentals=rows * rows // 2),
        name="attend",
    )(q, k, v)


def attend_back_kernel(block, scale, q_ref, k_ref, v_ref, o_ref, do_ref, lse_ref, dq_ref, dk_ref, dv_ref, delta_ref, dk_acc, dv_acc):
    blk = pl.program_id(0)
    n_blk = pl.num_programs(0)
    factor = scale * LOG2E

    @pl.when(blk == 0)
    def _():
        def prepare(idx, carry):
            rows = pl.ds(pl.multiple_of(idx * block, block), block)
            prod = do_ref[rows, :].astype(jnp.float32) * o_ref[rows, :].astype(jnp.float32)
            delta_ref[:, rows] = jnp.sum(prod.T, axis=0, keepdims=True)
            dq_ref[rows, :] = jnp.zeros((block, dq_ref.shape[1]), jnp.float32)
            return carry

        lax.fori_loop(0, n_blk, prepare, 0)

    k_blk = k_ref[...]
    v_blk = v_ref[...]

    def one(idx, masked):
        rows = pl.ds(pl.multiple_of(idx * block, block), block)
        q_blk = q_ref[rows, :]
        do_blk = do_ref[rows, :]
        scores = dot_nt(k_blk, q_blk)
        if masked:
            scores = causal_mask(scores)
        probs = jnp.exp2(scores * factor - lse_ref[:, rows])
        grad_v = dot_nn(probs.astype(jnp.bfloat16), do_blk)
        grad_p = dot_nt(v_blk, do_blk)
        grad_s = (probs * ((grad_p - delta_ref[:, rows]) * scale)).astype(jnp.bfloat16)
        dq_ref[rows, :] += dot_tn(grad_s, k_blk)
        return dot_nn(grad_s, q_blk), grad_v

    dk_acc[...], dv_acc[...] = one(blk, True)

    def step(idx, carry):
        grad_k, grad_v = one(idx, False)
        dk_acc[...] += grad_k
        dv_acc[...] += grad_v
        return carry

    lax.fori_loop(blk + 1, n_blk, step, 0)
    dk_ref[...] = dk_acc[...]
    dv_ref[...] = dv_acc[...].astype(jnp.bfloat16)


def attend_back(q, k, v, o, do, lse):
    rows, head_dim = q.shape
    block = min(512, rows // 4)
    whole = pl.BlockSpec((rows, head_dim), lambda i: (0, 0))
    part = pl.BlockSpec((block, head_dim), lambda i: (i, 0))
    stat = pl.BlockSpec((1, rows), lambda i: (0, 0))
    return pl.pallas_call(
        functools.partial(attend_back_kernel, block, head_dim ** -0.5),
        grid=(rows // block,),
        out_shape=(jax.ShapeDtypeStruct(q.shape, jnp.float32), jax.ShapeDtypeStruct(q.shape, jnp.float32), jax.ShapeDtypeStruct(q.shape, jnp.bfloat16)),
        in_specs=[whole, part, part, whole, whole, stat],
        out_specs=(whole, part, part),
        scratch_shapes=[pltpu.VMEM((1, rows), jnp.float32), pltpu.VMEM((block, head_dim), jnp.float32), pltpu.VMEM((block, head_dim), jnp.float32)],
        compiler_params=pltpu.CompilerParams(vmem_limit_bytes=VMEM_LIMIT),
        cost_estimate=pl.CostEstimate(flops=5 * rows * rows * head_dim, bytes_accessed=20 * rows * head_dim, transcendentals=rows * rows // 2),
        name="attend_back",
    )(q, k, v, o, do, lse)


def post_kernel(o_ref, wo_ref, x_ref, gy_ref, pw_ref, y_ref, gp_ref, do_ref, gpost_ref):
    tp_size, heads, _, head_dim = o_ref.shape
    proj = None
    for idx in range(tp_size):
        term = dot_nn(jnp.concatenate([o_ref[idx, head] for head in range(heads)], axis=1), wo_ref[idx])
        proj = term if proj is None else proj + term
    gain = pw_ref[...]
    inv = lax.rsqrt(jnp.mean(proj * proj, axis=-1, keepdims=True) + NORM_EPS)
    hat = proj * inv
    y_ref[...] = (x_ref[...].astype(jnp.float32) + hat * gain).astype(jnp.bfloat16)
    grad = gy_ref[...].astype(jnp.float32)
    gpost = jnp.sum(grad * hat, axis=0, keepdims=True)
    grad_hat = grad * gain
    grad_proj = (inv * (grad_hat - hat * jnp.mean(grad_hat * hat, axis=-1, keepdims=True))).astype(jnp.bfloat16)
    gp_ref[...] = grad_proj
    for idx in range(tp_size):
        grad_o = dot_nt(grad_proj, wo_ref[idx]).astype(jnp.bfloat16)
        for head in range(heads):
            do_ref[idx, head] = grad_o[:, head * head_dim:(head + 1) * head_dim]

    @pl.when(pl.program_id(0) == 0)
    def _():
        gpost_ref[...] = jnp.zeros_like(gpost_ref)

    gpost_ref[...] += gpost


def post(o_all, wo_all, x, gy, gain):
    tp_size, heads, rows, head_dim = o_all.shape
    d_model = x.shape[1]
    block = min(128, rows)
    act = pl.BlockSpec((block, d_model), lambda i: (i, 0))
    by_head = pl.BlockSpec((tp_size, heads, block, head_dim), lambda i: (0, 0, i, 0))
    act_shape = jax.ShapeDtypeStruct((rows, d_model), jnp.bfloat16)
    return pl.pallas_call(
        post_kernel,
        grid=(rows // block,),
        out_shape=(act_shape, act_shape, jax.ShapeDtypeStruct(o_all.shape, jnp.bfloat16), jax.ShapeDtypeStruct((1, d_model), jnp.float32)),
        in_specs=[by_head, pl.BlockSpec(wo_all.shape, lambda i: (0, 0, 0)), act, act, pl.BlockSpec((1, d_model), lambda i: (0, 0))],
        out_specs=(act, act, by_head, pl.BlockSpec((1, d_model), lambda i: (0, 0))),
        compiler_params=pltpu.CompilerParams(vmem_limit_bytes=VMEM_LIMIT),
        cost_estimate=pl.CostEstimate(flops=4 * rows * d_model * d_model, bytes_accessed=4 * d_model * d_model, transcendentals=rows),
        name="post",
    )(o_all, wo_all, x, gy, gain)


def spread_kernel(in_ref, *out_refs):
    for number, out_ref in enumerate(out_refs):
        for head in range(in_ref.shape[0]):
            out_ref[:, head, :] = in_ref[head, number]


def spread(gathered):
    heads, count, d_model, head_dim = gathered.shape
    block = min(256, d_model)
    return pl.pallas_call(
        spread_kernel,
        grid=(d_model // block,),
        out_shape=tuple([jax.ShapeDtypeStruct((d_model, heads, head_dim), gathered.dtype)] * count),
        in_specs=[pl.BlockSpec((heads, count, block, head_dim), lambda i: (0, 0, i, 0))],
        out_specs=tuple([pl.BlockSpec((block, heads, head_dim), lambda i: (i, 0, 0))] * count),
        compiler_params=pltpu.CompilerParams(vmem_limit_bytes=VMEM_LIMIT),
        cost_estimate=pl.CostEstimate(flops=d_model * heads * head_dim * count, bytes_accessed=8 * d_model * heads * head_dim * count, transcendentals=0),
        name="spread",
    )(gathered)


def chain_kernel(size, n_chunk, lag, tile, dq_ref, dk_ref, dv_ref, wq_ref, wk_ref, wv_ref, gy_ref, out_ref, part_ref, sums_a, sums_b, rs_send, rs_recv, ag_send, ag_recv):
    me = lax.axis_index("tp")
    entry_barrier("tp", size)
    half = part_ref.shape[0] // 2
    rows = half // n_chunk
    last = size - 1

    def parts(side, chunk):
        local = pl.ds(pl.multiple_of(chunk * rows, rows), rows)
        glob = pl.ds(pl.multiple_of(side * half + chunk * rows, rows), rows)
        sums = (sums_a, sums_b)[side]
        return local, glob, sums

    def toward(side):
        return jnp.maximum(me - 1, 0) if side == 0 else jnp.minimum(me + 1, last)

    def away(side):
        return jnp.minimum(me + 1, last) if side == 0 else jnp.maximum(me - 1, 0)

    def rs_copy(side, chunk, first):
        local, glob, sums = parts(side, chunk)
        return pltpu.make_async_remote_copy(
            src_ref=part_ref.at[glob] if first else sums.at[local], dst_ref=sums.at[local],
            send_sem=rs_send.at[side, chunk], recv_sem=rs_recv.at[side, chunk],
            device_id={"tp": toward(side)}, device_id_type=MESH)

    def ag_copy(side, chunk):
        _, glob, _ = parts(side, chunk)
        return pltpu.make_async_remote_copy(
            src_ref=out_ref.at[glob], dst_ref=out_ref.at[glob],
            send_sem=ag_send.at[side, chunk], recv_sem=ag_recv.at[side, chunk],
            device_id={"tp": away(side)}, device_id_type=MESH)

    def place(side):
        return me if side == 0 else last - me

    heads = dq_ref.shape[0]
    d_model = out_ref.shape[1]
    block = min(512, d_model)
    n_tile = 2 * half // tile
    per_tile = tile // rows

    def push(number):
        for side in (0, 1):
            @pl.when((lax.rem(number, 2) == side) & (place(side) == last))
            def _(side=side):
                def one(idx, carry):
                    rs_copy(side, (number // 2) * per_tile + idx, True).start()
                    return carry

                lax.fori_loop(0, per_tile, one, 0)

    def product(number, carry):
        tile_rows = pl.ds(pl.multiple_of(lax.rem(number, 2) * half + (number // 2) * tile, tile), tile)

        def columns(idx, carry):
            cols = pl.ds(pl.multiple_of(idx * block, block), block)
            total = None
            for grad_ref, w_ref in ((dq_ref, wq_ref), (dk_ref, wk_ref), (dv_ref, wv_ref)):
                grad = jnp.concatenate([grad_ref[idx_h, tile_rows, :] for idx_h in range(heads)], axis=1)
                term = dot_nn(grad, w_ref[:, cols])
                total = term if total is None else total + term
            part_ref[tile_rows, cols] = total
            return carry

        lax.fori_loop(0, d_model // block, columns, 0)

        @pl.when(number > 0)
        def _():
            push(number - 1)

        return carry

    lax.fori_loop(0, n_tile, product, 0)
    push(jnp.int32(n_tile - 1))

    def pass_on(side, chunk):
        local, glob, sums = parts(side, chunk)
        rs_copy(side, chunk, False).wait_recv()
        sums[local] = sums[local] + part_ref[glob]
        rs_copy(side, chunk, False).start()

    def finish(side, chunk):
        local, glob, sums = parts(side, chunk)
        rs_copy(side, chunk, False).wait_recv()
        out_ref[glob] = (gy_ref[glob].astype(jnp.float32) + (sums[local] + part_ref[glob])).astype(jnp.bfloat16)
        ag_copy(side, chunk).start()

    def reduce_step(idx, carry):
        for far in range(last - 1, 0, -1):
            chunk = idx - (last - 1 - far) * lag
            for side in (0, 1):
                @pl.when((chunk >= 0) & (chunk < n_chunk) & (place(side) == far))
                def _(side=side, chunk=chunk):
                    pass_on(side, chunk)
        for side in (0, 1):
            @pl.when((idx < n_chunk) & (place(side) == 0))
            def _(side=side):
                finish(side, idx)
        return carry

    lax.fori_loop(0, n_chunk + (last - 2) * lag, reduce_step, 0)

    def return_step(idx, carry):
        for far in range(1, last + 1):
            chunk = idx - (far - 1) * lag
            for side in (0, 1):
                @pl.when((chunk >= 0) & (chunk < n_chunk) & (place(side) == far))
                def _(side=side, chunk=chunk, far=far):
                    ag_copy(side, chunk).wait_recv()
                    if far < last:
                        ag_copy(side, chunk).start()
        return carry

    lax.fori_loop(0, n_chunk + (last - 1) * lag, return_step, 0)

    def drain(idx, carry):
        for side in (0, 1):
            @pl.when(place(side) > 0)
            def _(side=side):
                rs_copy(side, idx, False).wait_send()

            @pl.when(place(side) < last)
            def _(side=side):
                ag_copy(side, idx).wait_send()
        return carry

    lax.fori_loop(0, n_chunk, drain, 0)


def chain_sum(size, collective_id, grads, weights, gy):
    rows, d_model = gy.shape
    n_chunk = 32 if rows >= 512 else 4
    sems = [pltpu.SemaphoreType.DMA((2, n_chunk))] * 4
    return pl.pallas_call(
        functools.partial(chain_kernel, size, n_chunk, 2, min(256, rows // 4)),
        out_shape=jax.ShapeDtypeStruct((rows, d_model), jnp.bfloat16),
        in_specs=[VMEM_SPEC] * 7,
        out_specs=VMEM_SPEC,
        scratch_shapes=[pltpu.VMEM((rows, d_model), jnp.float32), pltpu.VMEM((rows // 2, d_model), jnp.float32), pltpu.VMEM((rows // 2, d_model), jnp.float32)] + sems,
        compiler_params=pltpu.CompilerParams(collective_id=collective_id, has_side_effects=True, vmem_limit_bytes=VMEM_LIMIT),
        cost_estimate=pl.CostEstimate(flops=10 ** 11, bytes_accessed=16 * rows * d_model, transcendentals=0),
        name="chain_sum",
    )(*grads, *weights, gy)


def weights_back_kernel(tp_size, full_width, sub, x_ref, far_ref, wq_ref, wk_ref, dq_ref, dk_ref, dv_ref, cos_ref, sin_ref, qg_ref, kg_ref, post_ref, o_ref, gp_ref,
                        dw_ref, exq_ref, exk_ref, exv_ref, gains_ref, post_out, dwo_ref,
                        x_buf, wqk_ref, gp_buf, lin_ref, q16_ref, k16_ref, own, slots_tp, mid, slots_cp, total, gq_ref, gk_ref, my_gains,
                        x_sem, w_sem, pair_send, pair_recv, tp_send, tp_recv, cp_send, cp_recv, ex_send, ex_recv):
    me = lax.axis_index("cp")
    my_tp = lax.axis_index("tp")
    rows, head_dim = dq_ref.shape[1:]
    loads = []
    for idx, (src, dist) in enumerate(((x_ref, 0), (far_ref, 2))):
        load = pltpu.make_async_copy(src, x_buf.at[dist], x_sem.at[idx])
        load.start()
        loads.append(load)
    own_rows = pl.ds(pl.multiple_of(me * head_dim, head_dim), head_dim)
    w_loads = [pltpu.make_async_copy(src.at[own_rows], wqk_ref.at[pl.ds(idx * head_dim, head_dim)], w_sem.at[idx]) for idx, src in enumerate((wq_ref, wk_ref))]
    w_loads.append(pltpu.make_async_copy(gp_ref, gp_buf, w_sem.at[2]))
    for load in w_loads:
        load.start()
    peers_barrier()
    for idx, (src, dist) in enumerate(((x_ref, 1), (far_ref, 3))):
        load = pltpu.make_async_remote_copy(
            src_ref=src, dst_ref=x_buf.at[dist], send_sem=pair_send.at[idx], recv_sem=pair_recv.at[idx],
            device_id={"cp": flip(me, 1)}, device_id_type=MESH)
        load.start()
        loads.append(load)
    own[4:5, :] = jnp.zeros_like(own[4:5, :])
    own[4:5, 0:post_ref.shape[1]] = post_ref[...]

    def ex_copy(idx, src, dst, dist):
        peer = flip(me, dist)
        return pltpu.make_async_remote_copy(
            src_ref=src.at[peer], dst_ref=dst.at[me], send_sem=ex_send.at[idx, dist - 1], recv_sem=ex_recv.at[idx, dist - 1],
            device_id={"cp": peer}, device_id_type=MESH)

    copies = [ex_copy(2, dv_ref, exv_ref, dist) for dist in (2, 3, 1)]
    for copy in copies:
        copy.start()

    def grad_of(ref, blk, part, table):
        g = ref[blk, part, :]
        half_dim = head_dim // 2
        turned = jnp.concatenate([g[:, half_dim:], g[:, :half_dim]], axis=1)
        return g * cos_ref[table, :] - turned * sin_ref[table, :]

    w_loads[0].wait()
    w_loads[1].wait()
    sides = ((dq_ref, qg_ref, 0), (dk_ref, kg_ref, 1))
    for order, dist in enumerate((0, 2, 1, 3)):
        blk = flip(me, dist)
        if order < 2:
            loads[order].wait()
        else:
            loads[order].wait_recv()

        def first(idx, carry, dist=dist, blk=blk):
            part = pl.ds(pl.multiple_of(idx * sub, sub), sub)
            table = pl.ds(pl.multiple_of(blk * rows + idx * sub, sub), sub)
            lin = dot_nt(x_buf[dist, part, :], wqk_ref[...])
            lin_ref[dist, part, :] = lin
            for ref, gain_ref, number in sides:
                mine = lin[:, number * head_dim:(number + 1) * head_dim]
                grad = grad_of(ref, blk, part, table) * gain_ref[...]
                own[2 * number:2 * number + 1, table] = jnp.sum((mine * mine).T, axis=0, keepdims=True)
                own[2 * number + 1:2 * number + 2, table] = jnp.sum((grad * mine).T, axis=0, keepdims=True)
            return carry

        lax.fori_loop(0, rows // sub, first, 0)

    moves = []
    for shift in range(1, tp_size):
        move = pltpu.make_async_remote_copy(
            src_ref=own, dst_ref=slots_tp.at[my_tp], send_sem=tp_send.at[shift - 1], recv_sem=tp_recv.at[shift - 1],
            device_id={"tp": lax.rem(my_tp + shift, tp_size)}, device_id_type=MESH)
        move.start()
        moves.append(move)
    slots_tp[my_tp] = own[...]
    for move in moves:
        move.wait()
    acc = slots_tp[0]
    for idx in range(1, tp_size):
        acc = acc + slots_tp[idx]
    mid[...] = acc
    moves = []
    for dist in (2, 3, 1):
        move = pltpu.make_async_remote_copy(
            src_ref=mid, dst_ref=slots_cp.at[me], send_sem=cp_send.at[dist - 1], recv_sem=cp_recv.at[dist - 1],
            device_id={"cp": flip(me, dist)}, device_id_type=MESH)
        move.start()
        moves.append(move)
    slots_cp[me] = mid[...]
    for move in moves:
        move.wait()
    total[...] = slots_cp[0] + slots_cp[1] + slots_cp[2] + slots_cp[3]

    post_out[...] = total[4:5, 0:post_ref.shape[1]]
    gq_ref[...] = jnp.zeros_like(gq_ref)
    gk_ref[...] = jnp.zeros_like(gk_ref)
    outs = ((q16_ref, exq_ref, gq_ref), (k16_ref, exk_ref, gk_ref))
    for dist in (2, 3, 1, 0):
        blk = flip(me, dist)

        def second(idx, carry, dist=dist, blk=blk):
            part = pl.ds(pl.multiple_of(idx * sub, sub), sub)
            table = pl.ds(pl.multiple_of(blk * rows + idx * sub, sub), sub)
            lin = lin_ref[dist, part, :]
            for (ref, gain_ref, number), (d16_ref, _, gain_out) in zip(sides, outs):
                mine = lin[:, number * head_dim:(number + 1) * head_dim]
                inv = lax.rsqrt(total[2 * number:2 * number + 1, table] / full_width + NORM_EPS)
                dot = inv * total[2 * number + 1:2 * number + 2, table] / full_width
                inv = jnp.broadcast_to(inv, (head_dim, sub)).T
                dot = jnp.broadcast_to(dot, (head_dim, sub)).T
                raw = grad_of(ref, blk, part, table)
                hat = mine * inv
                d16_ref[blk, part, :] = (inv * (raw * gain_ref[...] - hat * dot)).astype(jnp.bfloat16)
                gain_out[...] += jnp.sum(raw * hat, axis=0, keepdims=True)
            return carry

        lax.fori_loop(0, rows // sub, second, 0)
        if dist:
            for idx, (d16_ref, ex_ref, _) in enumerate(outs):
                copy = ex_copy(idx, d16_ref, ex_ref, dist)
                copy.start()
                copies.append(copy)
    my_gains[0:1, :] = gq_ref[...]
    my_gains[1:2, :] = gk_ref[...]
    for src, dst in ((q16_ref, exq_ref), (k16_ref, exk_ref), (dv_ref, exv_ref)):
        dst[me] = src[me]
    gains_ref[me] = my_gains[...]
    for dist in (1, 2, 3):
        copy = pltpu.make_async_remote_copy(
            src_ref=my_gains, dst_ref=gains_ref.at[me], send_sem=ex_send.at[3, dist - 1], recv_sem=ex_recv.at[3, dist - 1],
            device_id={"cp": flip(me, dist)}, device_id_type=MESH)
        copy.start()
        copies.append(copy)

    block = min(512, x_buf.shape[2])

    def weight_step(idx, carry):
        cols = pl.ds(pl.multiple_of(idx * block, block), block)
        acc = None
        for dist in range(4):
            blk = flip(me, dist)
            grads = jnp.concatenate([q16_ref[blk], k16_ref[blk], dv_ref[blk]], axis=1)
            term = dot_tn(grads, x_buf[dist, :, cols])
            acc = term if acc is None else acc + term
        acc = acc.T
        for number in range(3):
            dw_ref[number, cols, :] = acc[:, number * head_dim:(number + 1) * head_dim]
        return carry

    lax.fori_loop(0, x_buf.shape[2] // block, weight_step, 0)
    w_loads[2].wait()

    def output_step(idx, carry):
        cols = pl.ds(pl.multiple_of(idx * block, block), block)
        grads = jnp.concatenate([o_ref[head] for head in range(o_ref.shape[0])], axis=1)
        acc = dot_tn(grads, gp_buf[:, cols])
        for head in range(o_ref.shape[0]):
            dwo_ref[head, :, cols] = acc[head * head_dim:(head + 1) * head_dim, :]
        return carry

    lax.fori_loop(0, x_buf.shape[2] // block, output_step, 0)
    for copy in copies:
        copy.wait()
    loads[2].wait_send()
    loads[3].wait_send()


def weights_back(tp_size, collective_id, full_width, x, x_far, wq, wk, dq, dk, dv, cos_tab, sin_tab, q_gain, k_gain, grad_post, o_heads, grad_proj):
    _, rows, head_dim = dq.shape
    d_model = x.shape[1]
    any_spec = pl.BlockSpec(memory_space=pl.ANY)
    dma = pltpu.SemaphoreType.DMA
    span = max(4 * rows, d_model)
    stat = pltpu.VMEM((5, span), jnp.float32)
    slots = pltpu.VMEM((4, 5, span), jnp.float32)
    ex = jax.ShapeDtypeStruct(dq.shape, jnp.bfloat16)
    return pl.pallas_call(
        functools.partial(weights_back_kernel, tp_size, full_width, min(512, rows)),
        out_shape=(jax.ShapeDtypeStruct((3, d_model, head_dim), jnp.float32), ex, ex, ex,
                   jax.ShapeDtypeStruct((4, 2, head_dim), jnp.float32), jax.ShapeDtypeStruct((1, d_model), jnp.float32),
                   jax.ShapeDtypeStruct((o_heads.shape[0], head_dim, d_model), jnp.float32)),
        in_specs=[any_spec] * 4 + [VMEM_SPEC] * 9 + [any_spec],
        out_specs=tuple([VMEM_SPEC] * 7),
        scratch_shapes=[pltpu.VMEM((4, rows, d_model), jnp.bfloat16), pltpu.VMEM((2 * head_dim, d_model), jnp.bfloat16), pltpu.VMEM((rows, d_model), jnp.bfloat16), pltpu.VMEM((4, rows, 2 * head_dim), jnp.float32),
                        pltpu.VMEM(dq.shape, jnp.bfloat16), pltpu.VMEM(dq.shape, jnp.bfloat16),
                        stat, slots, stat, slots, stat,
                        pltpu.VMEM((1, head_dim), jnp.float32), pltpu.VMEM((1, head_dim), jnp.float32), pltpu.VMEM((2, head_dim), jnp.float32),
                        dma((2,)), dma((3,)), dma((2,)), dma((2,)), dma((tp_size - 1,)), dma((tp_size - 1,)), dma((3,)), dma((3,)), dma((4, 3)), dma((4, 3))],
        compiler_params=pltpu.CompilerParams(collective_id=collective_id, has_side_effects=True, vmem_limit_bytes=VMEM_LIMIT),
        name="weights_back",
    )(x, x_far, wq, wk, dq, dk, dv, cos_tab, sin_tab, q_gain, k_gain, grad_post, o_heads, grad_proj)


def solution(mesh):
    tp_size = mesh.shape["tp"]
    cp_size = mesh.shape["cp"]
    act_spec = P("dp", "cp", None)
    col_spec = P(None, "tp", None)
    part_col = P("dp", "tp", None)
    in_specs = (act_spec, col_spec, col_spec, col_spec, P("tp", None, None), P("tp", None), P("tp", None), P(None), act_spec)
    out_specs = (act_spec, act_spec, part_col, part_col, part_col, P(("dp", "tp"), None, None), P(("dp", "tp"), None), P(("dp", "tp"), None), P("dp"))
    swap_core = [(dev, dev ^ 1) for dev in range(cp_size)]

    def local_run(x_in, w_q, w_k, w_v, w_o, q_norm_w, k_norm_w, post_norm_w, grad_y):
        rows, d_model = x_in.shape[1:]
        heads, head_dim = w_q.shape[1:]
        width = heads * head_dim
        full_width = width * tp_size
        x = x_in[0]
        gy = grad_y[0]
        cp_index = lax.axis_index("cp")
        cos_tab, sin_tab = rope_tables((cp_index * rows + jnp.arange(rows)).astype(jnp.float32), head_dim)
        wq, wk, wv = (w.reshape(d_model, width) for w in (w_q, w_k, w_v))

        core = cp_index % 2
        own_half = lax.dynamic_slice_in_dim(w_o, core * (heads // 2), heads // 2, axis=0)
        mine = lax.all_gather(own_half, "tp")
        other = lax.ppermute(mine, "cp", swap_core)
        wo_all = jnp.where(core == 0, jnp.concatenate([mine, other], axis=1), jnp.concatenate([other, mine], axis=1))
        wo_all = wo_all.reshape(tp_size, width, d_model)

        def by_head(t):
            return t.reshape(rows, heads, head_dim).transpose(1, 0, 2)

        q_lin = jnp.dot(x, wq, preferred_element_type=jnp.float32)
        k_lin = jnp.dot(x, wk, preferred_element_type=jnp.float32)
        v_lin = jnp.dot(x, wv, preferred_element_type=jnp.float32)
        squares = jnp.stack([jnp.sum(q_lin * q_lin, axis=1), jnp.sum(k_lin * k_lin, axis=1)])
        squares = small_sum("tp", tp_size, 0, squares)
        invs = lax.rsqrt(squares / full_width + NORM_EPS)[:, :, None]
        q_hat = by_head(q_lin * invs[0])
        k_hat = by_head(k_lin * invs[1])
        q_gain = q_norm_w[:, None, :]
        k_gain = k_norm_w[:, None, :]
        q_rot = rope(q_hat * q_gain, cos_tab, sin_tab).astype(jnp.bfloat16)
        k_rot = rope(k_hat * k_gain, cos_tab, sin_tab).astype(jnp.bfloat16)
        v_val = by_head(v_lin.astype(jnp.bfloat16))

        seq_shape = (cp_size * rows, head_dim)
        block_shape = (cp_size, rows, head_dim)
        q_seq, k_seq, v_seq = exchange("cp", cp_size, 1, q_rot, k_rot, v_val)
        q_seq, x_send = lax.optimization_barrier((q_seq, x))
        x_far = lax.ppermute(x_send, "cp", [(dev, dev ^ 2) for dev in range(cp_size)])
        q_seq, k_seq, v_seq = (t.reshape(seq_shape) for t in (q_seq, k_seq, v_seq))
        o_seq, lse = attend(q_seq, k_seq, v_seq)
        o_heads, o_tokens = heads_to_tokens(2, o_seq.reshape(block_shape))
        quarter = rows // tp_size
        first_row = lax.axis_index("tp") * quarter
        x_mine, gy_mine = (lax.dynamic_slice_in_dim(t, first_row, quarter, axis=0) for t in (x, gy))
        y_mine, gp_mine, do_tokens, grad_post = post(o_tokens, wo_all, x_mine, gy_mine, post_norm_w[None, :])
        do_seq = tokens_to_heads(3, do_tokens)
        grad_proj = lax.all_gather(gp_mine, "tp", tiled=True)
        y_mine, do_seq = lax.optimization_barrier((y_mine, do_seq))
        y_out = lax.all_gather(y_mine, "tp", tiled=True)

        coarse_cos, coarse_sin = (t[:, None, :] for t in rope_tables(jnp.arange(0, cp_size * rows, 64, dtype=jnp.float32), head_dim))
        fine_cos, fine_sin = (t[None, :, :] for t in rope_tables(jnp.arange(64, dtype=jnp.float32), head_dim))
        seq_cos = (coarse_cos * fine_cos - coarse_sin * fine_sin).reshape(cp_size * rows, head_dim // 2)
        seq_sin = (coarse_sin * fine_cos + coarse_cos * fine_sin).reshape(cp_size * rows, head_dim // 2)
        seq_cos = jnp.concatenate([seq_cos, seq_cos], axis=1)
        seq_sin = jnp.concatenate([-seq_sin, seq_sin], axis=1)
        turned = tuple(w.reshape(d_model, width).T for w in (w_q, w_k, w_v))
        gains_head = tuple(lax.dynamic_slice_in_dim(w, cp_index, 1, axis=0) for w in (q_norm_w, k_norm_w))
        dq_seq, dk_seq, dv_seq = attend_back(q_seq, k_seq, v_seq, o_seq, do_seq.reshape(seq_shape), lse)
        dw, dq16, dk16, dv16, gains, grad_post, grad_w_o = weights_back(
            tp_size, 4, full_width, x, x_far, turned[0], turned[1],
            dq_seq.reshape(block_shape), dk_seq.reshape(block_shape), dv_seq.reshape(block_shape), seq_cos, seq_sin, *gains_head, grad_post, o_heads, grad_proj)
        grad_w_o = lax.psum(grad_w_o, "cp")
        dw = spread(lax.all_gather(dw, "cp"))
        grad_x = chain_sum(tp_size, 6, (dq16, dk16, dv16), turned, gy)
        return (y_out[None], grad_x[None]) + tuple(dw) + (grad_w_o, gains[:, 0], gains[:, 1], grad_post[0])

    return jax.shard_map(local_run, mesh=mesh, in_specs=in_specs, out_specs=out_specs, check_vma=False)
```

```python
import functools

import jax
import jax.numpy as jnp
from jax import lax
from jax.experimental import pallas as pl
from jax.experimental.pallas import tpu as pltpu
from jax.sharding import PartitionSpec as P


ROPE_THETA = 500000.0
NORM_EPS = 1e-6
MASK_VALUE = -1e30
LOG2E = 1.4426950408889634
MESH = pl.DeviceIdType.MESH
VMEM_SPEC = pl.BlockSpec(memory_space=pltpu.VMEM)
VMEM_LIMIT = 60 * 1024 * 1024
NT = (((1,), (1,)), ((), ()))
TN = (((0,), (0,)), ((), ()))


def dot_nt(a, b):
    return lax.dot_general(a, b, NT, preferred_element_type=jnp.float32)


def dot_tn(a, b):
    return lax.dot_general(a, b, TN, preferred_element_type=jnp.float32)


def dot_nn(a, b):
    return jnp.dot(a, b, preferred_element_type=jnp.float32)


def rope_tables(positions, head_dim):
    half_dim = head_dim // 2
    inv_freq = ROPE_THETA ** (-2.0 * jnp.arange(half_dim, dtype=jnp.float32) / head_dim)
    angles = positions[:, None] * inv_freq[None, :]
    return jnp.cos(angles), jnp.sin(angles)


def entry_barrier(axis, size):
    me = lax.axis_index(axis)
    barrier = pltpu.get_barrier_semaphore()
    for shift in range(1, size):
        pl.semaphore_signal(barrier, inc=1, device_id={axis: lax.rem(me + shift, size)}, device_id_type=MESH)
    pl.semaphore_wait(barrier, size - 1)


def peers_barrier():
    me, my_tp = lax.axis_index("cp"), lax.axis_index("tp")
    barrier = pltpu.get_barrier_semaphore()
    for shift in (1, 2, 3):
        pl.semaphore_signal(barrier, inc=1, device_id={"cp": lax.rem(me + shift, 4)}, device_id_type=MESH)
        pl.semaphore_signal(barrier, inc=1, device_id={"tp": lax.rem(my_tp + shift, 4)}, device_id_type=MESH)
    pl.semaphore_wait(barrier, 6)


def flip(index, distance):
    if distance == 1:
        return index + 1 - 2 * lax.rem(index, 2)
    if distance == 2:
        return lax.rem(index + 2, 4)
    return 3 - index if distance == 3 else index


def heads_to_tokens_kernel(in_ref, heads_ref, tokens_ref, cp_send, cp_recv, tp_send, tp_recv):
    me, my_tp = lax.axis_index("cp"), lax.axis_index("tp")
    quarter = in_ref.shape[1] // 4
    peers_barrier()
    first = {}
    for dist in (1, 2, 3):
        peer = flip(me, dist)
        first[dist] = pltpu.make_async_remote_copy(
            src_ref=in_ref.at[peer], dst_ref=heads_ref.at[me], send_sem=cp_send.at[dist - 1], recv_sem=cp_recv.at[dist - 1],
            device_id={"cp": peer}, device_id_type=MESH)
        first[dist].start()

    def rows_of(which):
        return pl.ds(pl.multiple_of(which * quarter, quarter), quarter)

    second = []

    def forward(dist, src_ref, head):
        for shift in (2, 1, 3):
            peer = lax.rem(my_tp + shift, 4)
            copy = pltpu.make_async_remote_copy(
                src_ref=src_ref.at[head, rows_of(peer)], dst_ref=tokens_ref.at[my_tp, head],
                send_sem=tp_send.at[dist, shift - 1], recv_sem=tp_recv.at[dist, shift - 1],
                device_id={"tp": peer}, device_id_type=MESH)
            copy.start()
            second.append(copy)
        tokens_ref[my_tp, head] = src_ref[head, rows_of(my_tp)]

    forward(0, in_ref, me)
    heads_ref[me] = in_ref[me]
    for dist in (1, 2, 3):
        first[dist].wait_recv()
        forward(dist, heads_ref, flip(me, dist))
    for dist in (1, 2, 3):
        first[dist].wait_send()
    for copy in second:
        copy.wait()


def heads_to_tokens(collective_id, array):
    _, rows, head_dim = array.shape
    dma = pltpu.SemaphoreType.DMA
    return pl.pallas_call(
        heads_to_tokens_kernel,
        out_shape=(jax.ShapeDtypeStruct(array.shape, array.dtype), jax.ShapeDtypeStruct((4, 4, rows // 4, head_dim), array.dtype)),
        in_specs=[VMEM_SPEC],
        out_specs=(VMEM_SPEC, VMEM_SPEC),
        scratch_shapes=[dma((3,)), dma((3,)), dma((4, 3)), dma((4, 3))],
        compiler_params=pltpu.CompilerParams(collective_id=collective_id, has_side_effects=True, vmem_limit_bytes=VMEM_LIMIT),
        name="heads_to_tokens",
    )(array)


def tokens_to_heads_kernel(in_ref, seq_ref, block_ref, tp_send, tp_recv, cp_send, cp_recv):
    me, my_tp = lax.axis_index("cp"), lax.axis_index("tp")
    quarter = in_ref.shape[2]
    peers_barrier()
    first = {}
    for shift in (2, 1, 3):
        peer = lax.rem(my_tp + shift, 4)
        first[shift] = pltpu.make_async_remote_copy(
            src_ref=in_ref.at[peer], dst_ref=block_ref.at[my_tp], send_sem=tp_send.at[shift - 1], recv_sem=tp_recv.at[shift - 1],
            device_id={"tp": peer}, device_id_type=MESH)
        first[shift].start()
    second = []

    def forward(shift, src_ref, which):
        rows = pl.ds(pl.multiple_of(which * quarter, quarter), quarter)
        for dist in (2, 3, 1):
            peer = flip(me, dist)
            copy = pltpu.make_async_remote_copy(
                src_ref=src_ref.at[which, peer], dst_ref=seq_ref.at[me, rows],
                send_sem=cp_send.at[shift, dist - 1], recv_sem=cp_recv.at[shift, dist - 1],
                device_id={"cp": peer}, device_id_type=MESH)
            second.append(copy)
            copy.start()
        seq_ref[me, rows] = src_ref[which, me]

    forward(0, in_ref, my_tp)
    for shift in (1, 3, 2):
        first[shift].wait_recv()
        forward(shift, block_ref, lax.rem(my_tp + 4 - shift, 4))
    for shift in (1, 2, 3):
        first[shift].wait_send()
    for copy in second:
        copy.wait_send()
    for copy in second:
        copy.wait_recv()


def tokens_to_heads(collective_id, array):
    tp, heads, quarter, head_dim = array.shape
    dma = pltpu.SemaphoreType.DMA
    return pl.pallas_call(
        tokens_to_heads_kernel,
        out_shape=jax.ShapeDtypeStruct((heads, tp * quarter, head_dim), array.dtype),
        in_specs=[VMEM_SPEC],
        out_specs=VMEM_SPEC,
        scratch_shapes=[pltpu.VMEM(array.shape, array.dtype), dma((3,)), dma((3,)), dma((4, 3)), dma((4, 3))],
        compiler_params=pltpu.CompilerParams(collective_id=collective_id, has_side_effects=True, vmem_limit_bytes=VMEM_LIMIT),
        name="tokens_to_heads",
    )(array)


def turn(values):
    half_dim = values.shape[1] // 2
    return jnp.concatenate([values[:, half_dim:], values[:, :half_dim]], axis=1)


def front_kernel(full_width, sub, x_ref, wq_ref, wk_ref, wv_ref, cos_ref, sin_ref, qg_ref, kg_ref, q_out, k_out, v_out,
                 q_buf, k_buf, v_buf, lin_ref, own, slots, total, tp_send, tp_recv, ex_send, ex_recv):
    me, my_tp = lax.axis_index("cp"), lax.axis_index("tp")
    rows = x_ref.shape[0]
    heads, head_dim = qg_ref.shape
    peers_barrier()
    copies = []

    def send(idx, src, dst):
        for dist in (2, 3, 1):
            peer = flip(me, dist)
            copy = pltpu.make_async_remote_copy(
                src_ref=src.at[peer], dst_ref=dst.at[me], send_sem=ex_send.at[idx, dist - 1], recv_sem=ex_recv.at[idx, dist - 1],
                device_id={"cp": peer}, device_id_type=MESH)
            copy.start()
            copies.append(copy)
        dst[me] = src[me]

    def part_of(idx):
        return pl.ds(pl.multiple_of(idx * sub, sub), sub)

    def values(idx, carry):
        part = part_of(idx)
        out = dot_nt(x_ref[part, :], wv_ref[...]).astype(jnp.bfloat16)
        for head in range(heads):
            v_buf[head, part, :] = out[:, head * head_dim:(head + 1) * head_dim]
        return carry

    lax.fori_loop(0, rows // sub, values, 0)
    send(2, v_buf, v_out)

    def linear(idx, carry):
        part = part_of(idx)
        for number, w_ref in enumerate((wq_ref, wk_ref)):
            out = dot_nt(x_ref[part, :], w_ref[...])
            lin_ref[number, part, :] = out
            square = out * out
            square = sum(square[:, head * head_dim:(head + 1) * head_dim] for head in range(heads))
            own[number:number + 1, part] = jnp.sum(square.T, axis=0, keepdims=True)
        return carry

    lax.fori_loop(0, rows // sub, linear, 0)
    moves = []
    for shift in (1, 2, 3):
        move = pltpu.make_async_remote_copy(
            src_ref=own, dst_ref=slots.at[my_tp], send_sem=tp_send.at[shift - 1], recv_sem=tp_recv.at[shift - 1],
            device_id={"tp": lax.rem(my_tp + shift, 4)}, device_id_type=MESH)
        move.start()
        moves.append(move)
    slots[my_tp] = own[...]
    for move in moves:
        move.wait()
    total[...] = lax.rsqrt((slots[0] + slots[1] + slots[2] + slots[3]) / full_width + NORM_EPS)

    for number, (gain_ref, buf, out_ref) in enumerate(((qg_ref, q_buf, q_out), (kg_ref, k_buf, k_out))):
        def rotate(idx, carry, number=number, gain_ref=gain_ref, buf=buf):
            part = part_of(idx)
            inv = jnp.broadcast_to(total[number:number + 1, part], (head_dim, sub)).T
            for head in range(heads):
                scaled = lin_ref[number, part, head * head_dim:(head + 1) * head_dim] * inv * gain_ref[head:head + 1, :]
                buf[head, part, :] = (scaled * cos_ref[part, :] + turn(scaled) * sin_ref[part, :]).astype(jnp.bfloat16)
            return carry

        lax.fori_loop(0, rows // sub, rotate, 0)
        send(number, buf, out_ref)
    for copy in copies:
        copy.wait()


def front(collective_id, full_width, x, weights, cos_tab, sin_tab, q_gain, k_gain):
    rows, _ = x.shape
    heads, head_dim = q_gain.shape
    dma = pltpu.SemaphoreType.DMA
    block = (heads, rows, head_dim)
    stat = pltpu.VMEM((2, rows), jnp.float32)
    return pl.pallas_call(
        functools.partial(front_kernel, full_width, min(256, rows)),
        out_shape=tuple([jax.ShapeDtypeStruct(block, jnp.bfloat16)] * 3),
        in_specs=[VMEM_SPEC] * 8,
        out_specs=tuple([VMEM_SPEC] * 3),
        scratch_shapes=[pltpu.VMEM(block, jnp.bfloat16)] * 3 + [pltpu.VMEM((2, rows, heads * head_dim), jnp.float32),
                        stat, pltpu.VMEM((4, 2, rows), jnp.float32), stat, dma((3,)), dma((3,)), dma((3, 3)), dma((3, 3))],
        compiler_params=pltpu.CompilerParams(collective_id=collective_id, has_side_effects=True, vmem_limit_bytes=VMEM_LIMIT),
        name="front",
    )(x, *weights, cos_tab, sin_tab, q_gain, k_gain)


def causal_mask(scores):
    key_pos = lax.broadcasted_iota(jnp.int32, scores.shape, 0)
    query_pos = lax.broadcasted_iota(jnp.int32, scores.shape, 1)
    return jnp.where(key_pos <= query_pos, scores, MASK_VALUE)


def attend_kernel(block, factor, q_ref, k_ref, v_ref, o_ref, lse_ref):
    blk = pl.program_id(0)
    q_blk = q_ref[...]

    def scores_of(idx):
        rows = pl.ds(pl.multiple_of(idx * block, block), block)
        return dot_nt(k_ref[rows, :], q_blk), v_ref[rows, :]

    scores, v_blk = scores_of(blk)
    scores = causal_mask(scores)
    top = jnp.max(scores, axis=0, keepdims=True)
    probs = jnp.exp2((scores - top) * factor)
    norm = jnp.sum(probs, axis=0, keepdims=True)
    acc = dot_tn(v_blk, probs.astype(jnp.bfloat16))

    def step(idx, state):
        top, norm, acc = state
        scores, v_blk = scores_of(idx)
        new_top = jnp.maximum(top, jnp.max(scores, axis=0, keepdims=True))
        probs = jnp.exp2((scores - new_top) * factor)
        rescale = jnp.exp2((top - new_top) * factor)
        norm = norm * rescale + jnp.sum(probs, axis=0, keepdims=True)
        acc = acc * rescale + dot_tn(v_blk, probs.astype(jnp.bfloat16))
        return new_top, norm, acc

    top, norm, acc = lax.fori_loop(0, blk, step, (top, norm, acc))
    o_ref[...] = (acc / norm).T.astype(jnp.bfloat16)
    lse_ref[...] = top * factor + jnp.log2(norm)


def attend(q, k, v):
    rows, head_dim = q.shape
    block = min(512, rows // 4)
    whole = pl.BlockSpec((rows, head_dim), lambda i: (0, 0))
    part = pl.BlockSpec((block, head_dim), lambda i: (i, 0))
    return pl.pallas_call(
        functools.partial(attend_kernel, block, head_dim ** -0.5 * LOG2E),
        grid=(rows // block,),
        out_shape=(jax.ShapeDtypeStruct(q.shape, jnp.bfloat16), jax.ShapeDtypeStruct((1, rows), jnp.float32)),
        in_specs=[part, whole, whole],
        out_specs=(part, pl.BlockSpec((1, block), lambda i: (0, i))),
        compiler_params=pltpu.CompilerParams(vmem_limit_bytes=VMEM_LIMIT),
        cost_estimate=pl.CostEstimate(flops=2 * rows * rows * head_dim, bytes_accessed=8 * rows * head_dim, transcendentals=rows * rows // 2),
        name="attend",
    )(q, k, v)


def attend_back_kernel(block, scale, q_ref, k_ref, v_ref, o_ref, do_ref, lse_ref, dq_ref, dk_ref, dv_ref, delta_ref, dk_acc, dv_acc):
    blk = pl.program_id(0)
    n_blk = pl.num_programs(0)
    factor = scale * LOG2E

    @pl.when(blk == 0)
    def _():
        def prepare(idx, carry):
            rows = pl.ds(pl.multiple_of(idx * block, block), block)
            prod = do_ref[rows, :].astype(jnp.float32) * o_ref[rows, :].astype(jnp.float32)
            delta_ref[:, rows] = jnp.sum(prod.T, axis=0, keepdims=True)
            dq_ref[rows, :] = jnp.zeros((block, dq_ref.shape[1]), jnp.float32)
            return carry

        lax.fori_loop(0, n_blk, prepare, 0)

    k_blk = k_ref[...]
    v_blk = v_ref[...]

    def one(idx, masked):
        rows = pl.ds(pl.multiple_of(idx * block, block), block)
        q_blk = q_ref[rows, :]
        do_blk = do_ref[rows, :]
        scores = dot_nt(k_blk, q_blk)
        if masked:
            scores = causal_mask(scores)
        probs = jnp.exp2(scores * factor - lse_ref[:, rows])
        grad_v = dot_nn(probs.astype(jnp.bfloat16), do_blk)
        grad_p = dot_nt(v_blk, do_blk)
        grad_s = (probs * ((grad_p - delta_ref[:, rows]) * scale)).astype(jnp.bfloat16)
        dq_ref[rows, :] += dot_tn(grad_s, k_blk)
        return dot_nn(grad_s, q_blk), grad_v

    dk_acc[...], dv_acc[...] = one(blk, True)

    def step(idx, carry):
        grad_k, grad_v = one(idx, False)
        dk_acc[...] += grad_k
        dv_acc[...] += grad_v
        return carry

    lax.fori_loop(blk + 1, n_blk, step, 0)
    dk_ref[...] = dk_acc[...]
    dv_ref[...] = dv_acc[...].astype(jnp.bfloat16)


def attend_back(q, k, v, o, do, lse):
    rows, head_dim = q.shape
    block = min(512, rows // 4)
    whole = pl.BlockSpec((rows, head_dim), lambda i: (0, 0))
    part = pl.BlockSpec((block, head_dim), lambda i: (i, 0))
    stat = pl.BlockSpec((1, rows), lambda i: (0, 0))
    return pl.pallas_call(
        functools.partial(attend_back_kernel, block, head_dim ** -0.5),
        grid=(rows // block,),
        out_shape=(jax.ShapeDtypeStruct(q.shape, jnp.float32), jax.ShapeDtypeStruct(q.shape, jnp.float32), jax.ShapeDtypeStruct(q.shape, jnp.bfloat16)),
        in_specs=[whole, part, part, whole, whole, stat],
        out_specs=(whole, part, part),
        scratch_shapes=[pltpu.VMEM((1, rows), jnp.float32), pltpu.VMEM((block, head_dim), jnp.float32), pltpu.VMEM((block, head_dim), jnp.float32)],
        compiler_params=pltpu.CompilerParams(vmem_limit_bytes=VMEM_LIMIT),
        cost_estimate=pl.CostEstimate(flops=5 * rows * rows * head_dim, bytes_accessed=20 * rows * head_dim, transcendentals=rows * rows // 2),
        name="attend_back",
    )(q, k, v, o, do, lse)


def post_kernel(o_ref, mine_ref, other_ref, x_ref, gy_ref, pw_ref, y_ref, gp_ref, do_ref, gpost_ref):
    tp_size, heads, _, head_dim = o_ref.shape
    core = lax.rem(lax.axis_index("cp"), 2)
    halves = ((mine_ref, core * (heads // 2)), (other_ref, (1 - core) * (heads // 2)))
    proj = None
    for idx in range(tp_size):
        for w_ref, start in halves:
            term = dot_nn(jnp.concatenate([o_ref[idx, start + head] for head in range(heads // 2)], axis=1), w_ref[idx])
            proj = term if proj is None else proj + term
    gain = pw_ref[...]
    inv = lax.rsqrt(jnp.mean(proj * proj, axis=-1, keepdims=True) + NORM_EPS)
    hat = proj * inv
    y_ref[...] = (x_ref[...].astype(jnp.float32) + hat * gain).astype(jnp.bfloat16)
    grad = gy_ref[...].astype(jnp.float32)
    gpost = jnp.sum(grad * hat, axis=0, keepdims=True)
    grad_hat = grad * gain
    grad_proj = (inv * (grad_hat - hat * jnp.mean(grad_hat * hat, axis=-1, keepdims=True))).astype(jnp.bfloat16)
    gp_ref[...] = grad_proj
    for idx in range(tp_size):
        for w_ref, start in halves:
            grad_o = dot_nt(grad_proj, w_ref[idx]).astype(jnp.bfloat16)
            for head in range(heads // 2):
                do_ref[idx, start + head] = grad_o[:, head * head_dim:(head + 1) * head_dim]

    @pl.when(pl.program_id(0) == 0)
    def _():
        gpost_ref[...] = jnp.zeros_like(gpost_ref)

    gpost_ref[...] += gpost


def post(o_all, wo_mine, wo_other, x, gy, gain):
    tp_size, heads, rows, head_dim = o_all.shape
    d_model = x.shape[1]
    block = min(128, rows)
    act = pl.BlockSpec((block, d_model), lambda i: (i, 0))
    by_head = pl.BlockSpec((tp_size, heads, block, head_dim), lambda i: (0, 0, i, 0))
    act_shape = jax.ShapeDtypeStruct((rows, d_model), jnp.bfloat16)
    return pl.pallas_call(
        post_kernel,
        grid=(rows // block,),
        out_shape=(act_shape, act_shape, jax.ShapeDtypeStruct(o_all.shape, jnp.bfloat16), jax.ShapeDtypeStruct((1, d_model), jnp.float32)),
        in_specs=[by_head] + [pl.BlockSpec(wo_mine.shape, lambda i: (0, 0, 0))] * 2 + [act, act, pl.BlockSpec((1, d_model), lambda i: (0, 0))],
        out_specs=(act, act, by_head, pl.BlockSpec((1, d_model), lambda i: (0, 0))),
        compiler_params=pltpu.CompilerParams(vmem_limit_bytes=VMEM_LIMIT),
        cost_estimate=pl.CostEstimate(flops=4 * rows * d_model * d_model, bytes_accessed=4 * d_model * d_model, transcendentals=rows),
        name="post",
    )(o_all, wo_mine, wo_other, x, gy, gain)


def spread_kernel(in_ref, *out_refs):
    for number, out_ref in enumerate(out_refs):
        for head in range(in_ref.shape[0]):
            out_ref[:, head, :] = in_ref[head, number]


def spread(gathered):
    heads, count, d_model, head_dim = gathered.shape
    block = min(256, d_model)
    return pl.pallas_call(
        spread_kernel,
        grid=(d_model // block,),
        out_shape=tuple([jax.ShapeDtypeStruct((d_model, heads, head_dim), gathered.dtype)] * count),
        in_specs=[pl.BlockSpec((heads, count, block, head_dim), lambda i: (0, 0, i, 0))],
        out_specs=tuple([pl.BlockSpec((block, heads, head_dim), lambda i: (i, 0, 0))] * count),
        compiler_params=pltpu.CompilerParams(vmem_limit_bytes=VMEM_LIMIT),
        cost_estimate=pl.CostEstimate(flops=d_model * heads * head_dim * count, bytes_accessed=8 * d_model * heads * head_dim * count, transcendentals=0),
        name="spread",
    )(gathered)


def chain_kernel(size, n_chunk, lag, tile, dq_ref, dk_ref, dv_ref, wq_ref, wk_ref, wv_ref, gy_ref, out_ref, part_ref, sums_a, sums_b, rs_send, rs_recv, ag_send, ag_recv):
    me = lax.axis_index("tp")
    entry_barrier("tp", size)
    half = part_ref.shape[0] // 2
    rows = half // n_chunk
    last = size - 1

    def parts(side, chunk):
        local = pl.ds(pl.multiple_of(chunk * rows, rows), rows)
        glob = pl.ds(pl.multiple_of(side * half + chunk * rows, rows), rows)
        sums = (sums_a, sums_b)[side]
        return local, glob, sums

    def toward(side):
        return jnp.maximum(me - 1, 0) if side == 0 else jnp.minimum(me + 1, last)

    def away(side):
        return jnp.minimum(me + 1, last) if side == 0 else jnp.maximum(me - 1, 0)

    def rs_copy(side, chunk, first):
        local, glob, sums = parts(side, chunk)
        return pltpu.make_async_remote_copy(
            src_ref=part_ref.at[glob] if first else sums.at[local], dst_ref=sums.at[local],
            send_sem=rs_send.at[side, chunk], recv_sem=rs_recv.at[side, chunk],
            device_id={"tp": toward(side)}, device_id_type=MESH)

    def ag_copy(side, chunk):
        _, glob, _ = parts(side, chunk)
        return pltpu.make_async_remote_copy(
            src_ref=out_ref.at[glob], dst_ref=out_ref.at[glob],
            send_sem=ag_send.at[side, chunk], recv_sem=ag_recv.at[side, chunk],
            device_id={"tp": away(side)}, device_id_type=MESH)

    def place(side):
        return me if side == 0 else last - me

    heads = dq_ref.shape[0]
    d_model = out_ref.shape[1]
    block = min(512, d_model)
    n_tile = 2 * half // tile
    per_tile = tile // rows

    def push(number):
        for side in (0, 1):
            @pl.when((lax.rem(number, 2) == side) & (place(side) == last))
            def _(side=side):
                def one(idx, carry):
                    rs_copy(side, (number // 2) * per_tile + idx, True).start()
                    return carry

                lax.fori_loop(0, per_tile, one, 0)

    def product(number, carry):
        tile_rows = pl.ds(pl.multiple_of(lax.rem(number, 2) * half + (number // 2) * tile, tile), tile)

        def columns(idx, carry):
            cols = pl.ds(pl.multiple_of(idx * block, block), block)
            total = None
            for grad_ref, w_ref in ((dq_ref, wq_ref), (dk_ref, wk_ref), (dv_ref, wv_ref)):
                grad = jnp.concatenate([grad_ref[idx_h, tile_rows, :] for idx_h in range(heads)], axis=1)
                term = dot_nn(grad, w_ref[:, cols])
                total = term if total is None else total + term
            part_ref[tile_rows, cols] = total
            return carry

        lax.fori_loop(0, d_model // block, columns, 0)

        @pl.when(number > 0)
        def _():
            push(number - 1)

        return carry

    lax.fori_loop(0, n_tile, product, 0)
    push(jnp.int32(n_tile - 1))

    def pass_on(side, chunk):
        local, glob, sums = parts(side, chunk)
        rs_copy(side, chunk, False).wait_recv()
        sums[local] = sums[local] + part_ref[glob]
        rs_copy(side, chunk, False).start()

    def finish(side, chunk):
        local, glob, sums = parts(side, chunk)
        rs_copy(side, chunk, False).wait_recv()
        out_ref[glob] = (gy_ref[glob].astype(jnp.float32) + (sums[local] + part_ref[glob])).astype(jnp.bfloat16)
        ag_copy(side, chunk).start()

    def reduce_step(idx, carry):
        for far in range(last - 1, 0, -1):
            chunk = idx - (last - 1 - far) * lag
            for side in (0, 1):
                @pl.when((chunk >= 0) & (chunk < n_chunk) & (place(side) == far))
                def _(side=side, chunk=chunk):
                    pass_on(side, chunk)
        for side in (0, 1):
            @pl.when((idx < n_chunk) & (place(side) == 0))
            def _(side=side):
                finish(side, idx)
        return carry

    lax.fori_loop(0, n_chunk + (last - 2) * lag, reduce_step, 0)

    def return_step(idx, carry):
        for far in range(1, last + 1):
            chunk = idx - (far - 1) * lag
            for side in (0, 1):
                @pl.when((chunk >= 0) & (chunk < n_chunk) & (place(side) == far))
                def _(side=side, chunk=chunk, far=far):
                    ag_copy(side, chunk).wait_recv()
                    if far < last:
                        ag_copy(side, chunk).start()
        return carry

    lax.fori_loop(0, n_chunk + (last - 1) * lag, return_step, 0)

    def drain(idx, carry):
        for side in (0, 1):
            @pl.when(place(side) > 0)
            def _(side=side):
                rs_copy(side, idx, False).wait_send()

            @pl.when(place(side) < last)
            def _(side=side):
                ag_copy(side, idx).wait_send()
        return carry

    lax.fori_loop(0, n_chunk, drain, 0)


def chain_sum(size, collective_id, grads, weights, gy):
    rows, d_model = gy.shape
    n_chunk = 32 if rows >= 512 else 4
    sems = [pltpu.SemaphoreType.DMA((2, n_chunk))] * 4
    return pl.pallas_call(
        functools.partial(chain_kernel, size, n_chunk, 2, min(256, rows // 4)),
        out_shape=jax.ShapeDtypeStruct((rows, d_model), jnp.bfloat16),
        in_specs=[VMEM_SPEC] * 7,
        out_specs=VMEM_SPEC,
        scratch_shapes=[pltpu.VMEM((rows, d_model), jnp.float32), pltpu.VMEM((rows // 2, d_model), jnp.float32), pltpu.VMEM((rows // 2, d_model), jnp.float32)] + sems,
        compiler_params=pltpu.CompilerParams(collective_id=collective_id, has_side_effects=True, vmem_limit_bytes=VMEM_LIMIT),
        cost_estimate=pl.CostEstimate(flops=10 ** 11, bytes_accessed=16 * rows * d_model, transcendentals=0),
        name="chain_sum",
    )(*grads, *weights, gy)


def weights_back_kernel(tp_size, full_width, sub, x_ref, far0_ref, far1_ref, far2_ref, wq_ref, wk_ref, dq_ref, dk_ref, dv_ref, cos_ref, sin_ref, qg_ref, kg_ref, post_ref, o_ref, gp_ref,
                        dw_ref, exq_ref, exk_ref, exv_ref, gains_ref, post_out, dwo_ref,
                        x_buf, wqk_ref, gp_buf, lin_ref, q16_ref, k16_ref, own, slots_tp, mid, slots_cp, total, gq_ref, gk_ref, my_gains,
                        x_sem, w_sem, pair_send, pair_recv, tp_send, tp_recv, cp_send, cp_recv, ex_send, ex_recv):
    me = lax.axis_index("cp")
    my_tp = lax.axis_index("tp")
    rows, head_dim = dq_ref.shape[1:]
    loads = []
    step = far0_ref.shape[0]
    fars = ((far0_ref, pl.ds(0, step)), (far1_ref, pl.ds(step, step)), (far2_ref, pl.ds(2 * step, rows - 2 * step)))
    pieces = ((x_ref, 0, pl.ds(0, rows)),) + tuple((ref, 2, part) for ref, part in fars)
    for idx, (src, dist, part) in enumerate(pieces):
        load = pltpu.make_async_copy(src, x_buf.at[dist, part], x_sem.at[idx])
        load.start()
        loads.append(load)
    own_rows = pl.ds(pl.multiple_of(me * head_dim, head_dim), head_dim)
    w_loads = [pltpu.make_async_copy(src.at[own_rows], wqk_ref.at[pl.ds(idx * head_dim, head_dim)], w_sem.at[idx]) for idx, src in enumerate((wq_ref, wk_ref))]
    w_loads.append(pltpu.make_async_copy(gp_ref, gp_buf, w_sem.at[2]))
    for load in w_loads:
        load.start()
    peers_barrier()
    for idx, (src, dist, part) in enumerate(pieces):
        load = pltpu.make_async_remote_copy(
            src_ref=src, dst_ref=x_buf.at[dist + 1, part], send_sem=pair_send.at[idx], recv_sem=pair_recv.at[idx],
            device_id={"cp": flip(me, 1)}, device_id_type=MESH)
        load.start()
        loads.append(load)
    own[4:5, :] = jnp.zeros_like(own[4:5, :])
    own[4:5, 0:post_ref.shape[1]] = post_ref[...]

    def ex_copy(idx, src, dst, dist):
        peer = flip(me, dist)
        return pltpu.make_async_remote_copy(
            src_ref=src.at[peer], dst_ref=dst.at[me], send_sem=ex_send.at[idx, dist - 1], recv_sem=ex_recv.at[idx, dist - 1],
            device_id={"cp": peer}, device_id_type=MESH)

    copies = [ex_copy(2, dv_ref, exv_ref, dist) for dist in (2, 3, 1)]
    for copy in copies:
        copy.start()

    def grad_of(ref, blk, part, table):
        g = ref[blk, part, :]
        return g * cos_ref[table, :] - turn(g) * sin_ref[table, :]

    w_loads[0].wait()
    w_loads[1].wait()
    sides = ((dq_ref, qg_ref, 0), (dk_ref, kg_ref, 1))
    for order, dist in enumerate((0, 2, 1, 3)):
        blk = flip(me, dist)
        for load in (loads[0:1], loads[1:4], loads[4:5], loads[5:8])[order]:
            if order < 2:
                load.wait()
            else:
                load.wait_recv()

        def first(idx, carry, dist=dist, blk=blk):
            part = pl.ds(pl.multiple_of(idx * sub, sub), sub)
            table = pl.ds(pl.multiple_of(blk * rows + idx * sub, sub), sub)
            lin = dot_nt(x_buf[dist, part, :], wqk_ref[...])
            lin_ref[dist, part, :] = lin
            for ref, gain_ref, number in sides:
                mine = lin[:, number * head_dim:(number + 1) * head_dim]
                grad = grad_of(ref, blk, part, table) * gain_ref[...]
                own[2 * number:2 * number + 1, table] = jnp.sum((mine * mine).T, axis=0, keepdims=True)
                own[2 * number + 1:2 * number + 2, table] = jnp.sum((grad * mine).T, axis=0, keepdims=True)
            return carry

        lax.fori_loop(0, rows // sub, first, 0)

    moves = []
    for shift in range(1, tp_size):
        move = pltpu.make_async_remote_copy(
            src_ref=own, dst_ref=slots_tp.at[my_tp], send_sem=tp_send.at[shift - 1], recv_sem=tp_recv.at[shift - 1],
            device_id={"tp": lax.rem(my_tp + shift, tp_size)}, device_id_type=MESH)
        move.start()
        moves.append(move)
    slots_tp[my_tp] = own[...]
    for move in moves:
        move.wait()
    acc = slots_tp[0]
    for idx in range(1, tp_size):
        acc = acc + slots_tp[idx]
    mid[...] = acc
    moves = []
    for dist in (2, 3, 1):
        move = pltpu.make_async_remote_copy(
            src_ref=mid, dst_ref=slots_cp.at[me], send_sem=cp_send.at[dist - 1], recv_sem=cp_recv.at[dist - 1],
            device_id={"cp": flip(me, dist)}, device_id_type=MESH)
        move.start()
        moves.append(move)
    slots_cp[me] = mid[...]
    for move in moves:
        move.wait()
    total[...] = slots_cp[0] + slots_cp[1] + slots_cp[2] + slots_cp[3]

    post_out[...] = total[4:5, 0:post_ref.shape[1]]
    gq_ref[...] = jnp.zeros_like(gq_ref)
    gk_ref[...] = jnp.zeros_like(gk_ref)
    outs = ((q16_ref, exq_ref, gq_ref), (k16_ref, exk_ref, gk_ref))
    for dist in (2, 3, 1, 0):
        blk = flip(me, dist)

        def second(idx, carry, dist=dist, blk=blk):
            part = pl.ds(pl.multiple_of(idx * sub, sub), sub)
            table = pl.ds(pl.multiple_of(blk * rows + idx * sub, sub), sub)
            lin = lin_ref[dist, part, :]
            for (ref, gain_ref, number), (d16_ref, _, gain_out) in zip(sides, outs):
                mine = lin[:, number * head_dim:(number + 1) * head_dim]
                inv = lax.rsqrt(total[2 * number:2 * number + 1, table] / full_width + NORM_EPS)
                dot = inv * total[2 * number + 1:2 * number + 2, table] / full_width
                inv = jnp.broadcast_to(inv, (head_dim, sub)).T
                dot = jnp.broadcast_to(dot, (head_dim, sub)).T
                raw = grad_of(ref, blk, part, table)
                hat = mine * inv
                d16_ref[blk, part, :] = (inv * (raw * gain_ref[...] - hat * dot)).astype(jnp.bfloat16)
                gain_out[...] += jnp.sum(raw * hat, axis=0, keepdims=True)
            return carry

        lax.fori_loop(0, rows // sub, second, 0)
        if dist:
            for idx, (d16_ref, ex_ref, _) in enumerate(outs):
                copy = ex_copy(idx, d16_ref, ex_ref, dist)
                copy.start()
                copies.append(copy)
    my_gains[0:1, :] = gq_ref[...]
    my_gains[1:2, :] = gk_ref[...]
    for src, dst in ((q16_ref, exq_ref), (k16_ref, exk_ref), (dv_ref, exv_ref)):
        dst[me] = src[me]
    gains_ref[me] = my_gains[...]
    for dist in (1, 2, 3):
        copy = pltpu.make_async_remote_copy(
            src_ref=my_gains, dst_ref=gains_ref.at[me], send_sem=ex_send.at[3, dist - 1], recv_sem=ex_recv.at[3, dist - 1],
            device_id={"cp": flip(me, dist)}, device_id_type=MESH)
        copy.start()
        copies.append(copy)

    block = min(512, x_buf.shape[2])

    def weight_step(idx, carry):
        cols = pl.ds(pl.multiple_of(idx * block, block), block)
        acc = None
        for dist in range(4):
            blk = flip(me, dist)
            grads = jnp.concatenate([q16_ref[blk], k16_ref[blk], dv_ref[blk]], axis=1)
            term = dot_tn(grads, x_buf[dist, :, cols])
            acc = term if acc is None else acc + term
        acc = acc.T
        for number in range(3):
            dw_ref[number, cols, :] = acc[:, number * head_dim:(number + 1) * head_dim]
        return carry

    lax.fori_loop(0, x_buf.shape[2] // block, weight_step, 0)
    w_loads[2].wait()

    def output_step(idx, carry):
        cols = pl.ds(pl.multiple_of(idx * block, block), block)
        grads = jnp.concatenate([o_ref[head] for head in range(o_ref.shape[0])], axis=1)
        acc = dot_tn(grads, gp_buf[:, cols])
        for head in range(o_ref.shape[0]):
            dwo_ref[head, :, cols] = acc[head * head_dim:(head + 1) * head_dim, :]
        return carry

    lax.fori_loop(0, x_buf.shape[2] // block, output_step, 0)
    for copy in copies:
        copy.wait()
    for load in loads[4:]:
        load.wait_send()


def weights_back(tp_size, collective_id, full_width, x, x_far, wq, wk, dq, dk, dv, cos_tab, sin_tab, q_gain, k_gain, grad_post, o_heads, grad_proj):
    _, rows, head_dim = dq.shape
    d_model = x.shape[1]
    any_spec = pl.BlockSpec(memory_space=pl.ANY)
    dma = pltpu.SemaphoreType.DMA
    span = max(4 * rows, d_model)
    stat = pltpu.VMEM((5, span), jnp.float32)
    slots = pltpu.VMEM((4, 5, span), jnp.float32)
    ex = jax.ShapeDtypeStruct(dq.shape, jnp.bfloat16)
    return pl.pallas_call(
        functools.partial(weights_back_kernel, tp_size, full_width, min(512, rows)),
        out_shape=(jax.ShapeDtypeStruct((3, d_model, head_dim), jnp.float32), ex, ex, ex,
                   jax.ShapeDtypeStruct((4, 2, head_dim), jnp.float32), jax.ShapeDtypeStruct((1, d_model), jnp.float32),
                   jax.ShapeDtypeStruct((o_heads.shape[0], head_dim, d_model), jnp.float32)),
        in_specs=[any_spec] * 6 + [VMEM_SPEC] * 9 + [any_spec],
        out_specs=tuple([VMEM_SPEC] * 7),
        scratch_shapes=[pltpu.VMEM((4, rows, d_model), jnp.bfloat16), pltpu.VMEM((2 * head_dim, d_model), jnp.bfloat16), pltpu.VMEM((rows, d_model), jnp.bfloat16), pltpu.VMEM((4, rows, 2 * head_dim), jnp.float32),
                        pltpu.VMEM(dq.shape, jnp.bfloat16), pltpu.VMEM(dq.shape, jnp.bfloat16),
                        stat, slots, stat, slots, stat,
                        pltpu.VMEM((1, head_dim), jnp.float32), pltpu.VMEM((1, head_dim), jnp.float32), pltpu.VMEM((2, head_dim), jnp.float32),
                        dma((4,)), dma((3,)), dma((4,)), dma((4,)), dma((tp_size - 1,)), dma((tp_size - 1,)), dma((3,)), dma((3,)), dma((4, 3)), dma((4, 3))],
        compiler_params=pltpu.CompilerParams(collective_id=collective_id, has_side_effects=True, vmem_limit_bytes=VMEM_LIMIT),
        name="weights_back",
    )(x, *x_far, wq, wk, dq, dk, dv, cos_tab, sin_tab, q_gain, k_gain, grad_post, o_heads, grad_proj)


def solution(mesh):
    tp_size = mesh.shape["tp"]
    cp_size = mesh.shape["cp"]
    act_spec = P("dp", "cp", None)
    col_spec = P(None, "tp", None)
    part_col = P("dp", "tp", None)
    in_specs = (act_spec, col_spec, col_spec, col_spec, P("tp", None, None), P("tp", None), P("tp", None), P(None), act_spec)
    out_specs = (act_spec, act_spec, part_col, part_col, part_col, P(("dp", "tp"), None, None), P(("dp", "tp"), None), P(("dp", "tp"), None), P("dp"))
    swap_core = [(dev, dev ^ 1) for dev in range(cp_size)]

    def local_run(x_in, w_q, w_k, w_v, w_o, q_norm_w, k_norm_w, post_norm_w, grad_y):
        rows, d_model = x_in.shape[1:]
        heads, head_dim = w_q.shape[1:]
        width = heads * head_dim
        full_width = width * tp_size
        x = x_in[0]
        gy = grad_y[0]
        cp_index = lax.axis_index("cp")

        def wide_tables(cos_tab, sin_tab):
            return jnp.concatenate([cos_tab, cos_tab], axis=1), jnp.concatenate([-sin_tab, sin_tab], axis=1)

        cos_tab, sin_tab = wide_tables(*rope_tables((cp_index * rows + jnp.arange(rows)).astype(jnp.float32), head_dim))
        turned = tuple(w.reshape(d_model, width).T for w in (w_q, w_k, w_v))

        core = cp_index % 2
        own_half = lax.dynamic_slice_in_dim(w_o, core * (heads // 2), heads // 2, axis=0)
        wo_mine = lax.all_gather(own_half, "tp").reshape(tp_size, width // 2, d_model)
        q_seq, k_seq, v_seq = front(1, full_width, x, turned, cos_tab, sin_tab, q_norm_w, k_norm_w)
        seq_shape = (cp_size * rows, head_dim)
        block_shape = (cp_size, rows, head_dim)
        piece = rows // 4

        def fetch(start, size):
            return lax.ppermute(x_free[start:start + size], "cp", [(dev, dev ^ 2) for dev in range(cp_size)])

        q_seq, x_free = lax.optimization_barrier((q_seq, x))
        far0 = fetch(0, piece)
        q_seq, k_seq, v_seq = (t.reshape(seq_shape) for t in (q_seq, k_seq, v_seq))
        o_seq, lse = attend(q_seq, k_seq, v_seq)
        o_seq, wo_mine = lax.optimization_barrier((o_seq, wo_mine))
        wo_other = lax.ppermute(wo_mine, "cp", swap_core)
        o_heads, o_tokens = heads_to_tokens(2, o_seq.reshape(block_shape))
        o_tokens, x_free = lax.optimization_barrier((o_tokens, x))
        far1 = fetch(piece, piece)
        quarter = rows // tp_size
        first_row = lax.axis_index("tp") * quarter
        x_mine, gy_mine = (lax.dynamic_slice_in_dim(t, first_row, quarter, axis=0) for t in (x, gy))
        y_mine, gp_mine, do_tokens, grad_post = post(o_tokens, wo_mine, wo_other, x_mine, gy_mine, post_norm_w[None, :])
        do_seq = tokens_to_heads(3, do_tokens)
        grad_proj = lax.all_gather(gp_mine, "tp", tiled=True)
        y_mine, do_seq, x_free = lax.optimization_barrier((y_mine, do_seq, x))
        far2 = fetch(2 * piece, rows - 2 * piece)
        y_out = lax.all_gather(y_mine, "tp", tiled=True)

        coarse_cos, coarse_sin = (t[:, None, :] for t in rope_tables(jnp.arange(0, cp_size * rows, 64, dtype=jnp.float32), head_dim))
        fine_cos, fine_sin = (t[None, :, :] for t in rope_tables(jnp.arange(64, dtype=jnp.float32), head_dim))
        seq_cos = (coarse_cos * fine_cos - coarse_sin * fine_sin).reshape(cp_size * rows, head_dim // 2)
        seq_sin = (coarse_sin * fine_cos + coarse_cos * fine_sin).reshape(cp_size * rows, head_dim // 2)
        seq_cos, seq_sin = wide_tables(seq_cos, seq_sin)
        gains_head = tuple(lax.dynamic_slice_in_dim(w, cp_index, 1, axis=0) for w in (q_norm_w, k_norm_w))
        dq_seq, dk_seq, dv_seq = attend_back(q_seq, k_seq, v_seq, o_seq, do_seq.reshape(seq_shape), lse)
        dw, dq16, dk16, dv16, gains, grad_post, grad_w_o = weights_back(
            tp_size, 4, full_width, x, (far0, far1, far2), turned[0], turned[1],
            dq_seq.reshape(block_shape), dk_seq.reshape(block_shape), dv_seq.reshape(block_shape), seq_cos, seq_sin, *gains_head, grad_post, o_heads, grad_proj)
        grad_w_o = lax.psum(grad_w_o, "cp")
        dw = spread(lax.all_gather(dw, "cp"))
        grad_x = chain_sum(tp_size, 6, (dq16, dk16, dv16), turned, gy)
        return (y_out[None], grad_x[None]) + tuple(dw) + (grad_w_o, gains[:, 0], gains[:, 1], grad_post[0])

    return jax.shard_map(local_run, mesh=mesh, in_specs=in_specs, out_specs=out_specs, check_vma=False)
```

```python
import functools

import jax
import jax.numpy as jnp
from jax import lax
from jax.experimental import pallas as pl
from jax.experimental.pallas import tpu as pltpu
from jax.sharding import PartitionSpec as P


ROPE_THETA = 500000.0
NORM_EPS = 1e-6
MASK_VALUE = -1e30
LOG2E = 1.4426950408889634
MESH = pl.DeviceIdType.MESH
VMEM_SPEC = pl.BlockSpec(memory_space=pltpu.VMEM)
VMEM_LIMIT = 60 * 1024 * 1024
NT = (((1,), (1,)), ((), ()))
TN = (((0,), (0,)), ((), ()))


def dot_nt(a, b):
    return lax.dot_general(a, b, NT, preferred_element_type=jnp.float32)


def dot_tn(a, b):
    return lax.dot_general(a, b, TN, preferred_element_type=jnp.float32)


def dot_nn(a, b):
    return jnp.dot(a, b, preferred_element_type=jnp.float32)


def rope_tables(positions, head_dim):
    half_dim = head_dim // 2
    inv_freq = ROPE_THETA ** (-2.0 * jnp.arange(half_dim, dtype=jnp.float32) / head_dim)
    angles = positions[:, None] * inv_freq[None, :]
    return jnp.cos(angles), jnp.sin(angles)


def entry_barrier(axis, size):
    me = lax.axis_index(axis)
    barrier = pltpu.get_barrier_semaphore()
    for shift in range(1, size):
        pl.semaphore_signal(barrier, inc=1, device_id={axis: lax.rem(me + shift, size)}, device_id_type=MESH)
    pl.semaphore_wait(barrier, size - 1)


def peers_barrier():
    me, my_tp = lax.axis_index("cp"), lax.axis_index("tp")
    barrier = pltpu.get_barrier_semaphore()
    for shift in (1, 2, 3):
        pl.semaphore_signal(barrier, inc=1, device_id={"cp": lax.rem(me + shift, 4)}, device_id_type=MESH)
        pl.semaphore_signal(barrier, inc=1, device_id={"tp": lax.rem(my_tp + shift, 4)}, device_id_type=MESH)
    pl.semaphore_wait(barrier, 6)


def flip(index, distance):
    if distance == 1:
        return index + 1 - 2 * lax.rem(index, 2)
    if distance == 2:
        return lax.rem(index + 2, 4)
    return 3 - index if distance == 3 else index


def heads_to_tokens_kernel(in_ref, heads_ref, tokens_ref, cp_send, cp_recv, tp_send, tp_recv):
    me, my_tp = lax.axis_index("cp"), lax.axis_index("tp")
    quarter = in_ref.shape[1] // 4
    peers_barrier()
    first = {}
    for dist in (1, 2, 3):
        peer = flip(me, dist)
        first[dist] = pltpu.make_async_remote_copy(
            src_ref=in_ref.at[peer], dst_ref=heads_ref.at[me], send_sem=cp_send.at[dist - 1], recv_sem=cp_recv.at[dist - 1],
            device_id={"cp": peer}, device_id_type=MESH)
        first[dist].start()

    def rows_of(which):
        return pl.ds(pl.multiple_of(which * quarter, quarter), quarter)

    second = []

    def forward(dist, src_ref, head):
        for shift in (2, 1, 3):
            peer = lax.rem(my_tp + shift, 4)
            copy = pltpu.make_async_remote_copy(
                src_ref=src_ref.at[head, rows_of(peer)], dst_ref=tokens_ref.at[my_tp, head],
                send_sem=tp_send.at[dist, shift - 1], recv_sem=tp_recv.at[dist, shift - 1],
                device_id={"tp": peer}, device_id_type=MESH)
            copy.start()
            second.append(copy)
        tokens_ref[my_tp, head] = src_ref[head, rows_of(my_tp)]

    forward(0, in_ref, me)
    heads_ref[me] = in_ref[me]
    for dist in (1, 2, 3):
        first[dist].wait_recv()
        forward(dist, heads_ref, flip(me, dist))
    for dist in (1, 2, 3):
        first[dist].wait_send()
    for copy in second:
        copy.wait()


def heads_to_tokens(collective_id, array):
    _, rows, head_dim = array.shape
    dma = pltpu.SemaphoreType.DMA
    return pl.pallas_call(
        heads_to_tokens_kernel,
        out_shape=(jax.ShapeDtypeStruct(array.shape, array.dtype), jax.ShapeDtypeStruct((4, 4, rows // 4, head_dim), array.dtype)),
        in_specs=[VMEM_SPEC],
        out_specs=(VMEM_SPEC, VMEM_SPEC),
        scratch_shapes=[dma((3,)), dma((3,)), dma((4, 3)), dma((4, 3))],
        compiler_params=pltpu.CompilerParams(collective_id=collective_id, has_side_effects=True, vmem_limit_bytes=VMEM_LIMIT),
        name="heads_to_tokens",
    )(array)


def tokens_to_heads_kernel(in_ref, seq_ref, block_ref, tp_send, tp_recv, cp_send, cp_recv):
    me, my_tp = lax.axis_index("cp"), lax.axis_index("tp")
    quarter = in_ref.shape[2]
    peers_barrier()
    first = {}
    for shift in (2, 1, 3):
        peer = lax.rem(my_tp + shift, 4)
        first[shift] = pltpu.make_async_remote_copy(
            src_ref=in_ref.at[peer], dst_ref=block_ref.at[my_tp], send_sem=tp_send.at[shift - 1], recv_sem=tp_recv.at[shift - 1],
            device_id={"tp": peer}, device_id_type=MESH)
        first[shift].start()
    second = []

    def forward(shift, src_ref, which):
        rows = pl.ds(pl.multiple_of(which * quarter, quarter), quarter)
        for dist in (2, 3, 1):
            peer = flip(me, dist)
            copy = pltpu.make_async_remote_copy(
                src_ref=src_ref.at[which, peer], dst_ref=seq_ref.at[me, rows],
                send_sem=cp_send.at[shift, dist - 1], recv_sem=cp_recv.at[shift, dist - 1],
                device_id={"cp": peer}, device_id_type=MESH)
            second.append(copy)
            copy.start()
        seq_ref[me, rows] = src_ref[which, me]

    forward(0, in_ref, my_tp)
    for shift in (1, 3, 2):
        first[shift].wait_recv()
        forward(shift, block_ref, lax.rem(my_tp + 4 - shift, 4))
    for shift in (1, 2, 3):
        first[shift].wait_send()
    for copy in second:
        copy.wait_send()
    for copy in second:
        copy.wait_recv()


def tokens_to_heads(collective_id, array):
    tp, heads, quarter, head_dim = array.shape
    dma = pltpu.SemaphoreType.DMA
    return pl.pallas_call(
        tokens_to_heads_kernel,
        out_shape=jax.ShapeDtypeStruct((heads, tp * quarter, head_dim), array.dtype),
        in_specs=[VMEM_SPEC],
        out_specs=VMEM_SPEC,
        scratch_shapes=[pltpu.VMEM(array.shape, array.dtype), dma((3,)), dma((3,)), dma((4, 3)), dma((4, 3))],
        compiler_params=pltpu.CompilerParams(collective_id=collective_id, has_side_effects=True, vmem_limit_bytes=VMEM_LIMIT),
        name="tokens_to_heads",
    )(array)


def turn(values):
    half_dim = values.shape[1] // 2
    return jnp.concatenate([values[:, half_dim:], values[:, :half_dim]], axis=1)


def front_kernel(full_width, sub, x_ref, wq_ref, wk_ref, wv_ref, cos_ref, sin_ref, qg_ref, kg_ref, q_out, k_out, v_out,
                 q_buf, k_buf, v_buf, lin_ref, own, slots, total, tp_send, tp_recv, ex_send, ex_recv):
    me, my_tp = lax.axis_index("cp"), lax.axis_index("tp")
    rows = x_ref.shape[0]
    heads, head_dim = qg_ref.shape
    peers_barrier()
    copies = []

    def send(idx, src, dst):
        for dist in (2, 3, 1):
            peer = flip(me, dist)
            copy = pltpu.make_async_remote_copy(
                src_ref=src.at[peer], dst_ref=dst.at[me], send_sem=ex_send.at[idx, dist - 1], recv_sem=ex_recv.at[idx, dist - 1],
                device_id={"cp": peer}, device_id_type=MESH)
            copy.start()
            copies.append(copy)
        dst[me] = src[me]

    def part_of(idx):
        return pl.ds(pl.multiple_of(idx * sub, sub), sub)

    def values(idx, carry):
        part = part_of(idx)
        out = dot_nt(x_ref[part, :], wv_ref[...]).astype(jnp.bfloat16)
        for head in range(heads):
            v_buf[head, part, :] = out[:, head * head_dim:(head + 1) * head_dim]
        return carry

    lax.fori_loop(0, rows // sub, values, 0)
    send(2, v_buf, v_out)

    def linear(idx, carry):
        part = part_of(idx)
        for number, w_ref in enumerate((wq_ref, wk_ref)):
            out = dot_nt(x_ref[part, :], w_ref[...])
            lin_ref[number, part, :] = out
            square = out * out
            square = sum(square[:, head * head_dim:(head + 1) * head_dim] for head in range(heads))
            own[number:number + 1, part] = jnp.sum(square.T, axis=0, keepdims=True)
        return carry

    lax.fori_loop(0, rows // sub, linear, 0)
    moves = []
    for shift in (1, 2, 3):
        move = pltpu.make_async_remote_copy(
            src_ref=own, dst_ref=slots.at[my_tp], send_sem=tp_send.at[shift - 1], recv_sem=tp_recv.at[shift - 1],
            device_id={"tp": lax.rem(my_tp + shift, 4)}, device_id_type=MESH)
        move.start()
        moves.append(move)
    slots[my_tp] = own[...]
    for move in moves:
        move.wait()
    total[...] = lax.rsqrt((slots[0] + slots[1] + slots[2] + slots[3]) / full_width + NORM_EPS)

    for number, (gain_ref, buf, out_ref) in enumerate(((qg_ref, q_buf, q_out), (kg_ref, k_buf, k_out))):
        def rotate(idx, carry, number=number, gain_ref=gain_ref, buf=buf):
            part = part_of(idx)
            inv = jnp.broadcast_to(total[number:number + 1, part], (head_dim, sub)).T
            for head in range(heads):
                scaled = lin_ref[number, part, head * head_dim:(head + 1) * head_dim] * inv * gain_ref[head:head + 1, :]
                buf[head, part, :] = (scaled * cos_ref[part, :] + turn(scaled) * sin_ref[part, :]).astype(jnp.bfloat16)
            return carry

        lax.fori_loop(0, rows // sub, rotate, 0)
        send(number, buf, out_ref)
    for copy in copies:
        copy.wait()


def front(collective_id, full_width, x, weights, cos_tab, sin_tab, q_gain, k_gain):
    rows, _ = x.shape
    heads, head_dim = q_gain.shape
    dma = pltpu.SemaphoreType.DMA
    block = (heads, rows, head_dim)
    stat = pltpu.VMEM((2, rows), jnp.float32)
    return pl.pallas_call(
        functools.partial(front_kernel, full_width, min(256, rows)),
        out_shape=tuple([jax.ShapeDtypeStruct(block, jnp.bfloat16)] * 3),
        in_specs=[VMEM_SPEC] * 8,
        out_specs=tuple([VMEM_SPEC] * 3),
        scratch_shapes=[pltpu.VMEM(block, jnp.bfloat16)] * 3 + [pltpu.VMEM((2, rows, heads * head_dim), jnp.float32),
                        stat, pltpu.VMEM((4, 2, rows), jnp.float32), stat, dma((3,)), dma((3,)), dma((3, 3)), dma((3, 3))],
        compiler_params=pltpu.CompilerParams(collective_id=collective_id, has_side_effects=True, vmem_limit_bytes=VMEM_LIMIT),
        name="front",
    )(x, *weights, cos_tab, sin_tab, q_gain, k_gain)


def causal_mask(scores):
    key_pos = lax.broadcasted_iota(jnp.int32, scores.shape, 0)
    query_pos = lax.broadcasted_iota(jnp.int32, scores.shape, 1)
    return jnp.where(key_pos <= query_pos, scores, MASK_VALUE)


def attend_kernel(block, factor, q_ref, k_ref, v_ref, o_ref, lse_ref):
    blk = pl.program_id(0)
    q_blk = q_ref[...]

    def scores_of(idx):
        rows = pl.ds(pl.multiple_of(idx * block, block), block)
        return dot_nt(k_ref[rows, :], q_blk), v_ref[rows, :]

    scores, v_blk = scores_of(blk)
    scores = causal_mask(scores)
    top = jnp.max(scores, axis=0, keepdims=True)
    probs = jnp.exp2((scores - top) * factor)
    norm = jnp.sum(probs, axis=0, keepdims=True)
    acc = dot_tn(v_blk, probs.astype(jnp.bfloat16))

    def step(idx, state):
        top, norm, acc = state
        scores, v_blk = scores_of(idx)
        new_top = jnp.maximum(top, jnp.max(scores, axis=0, keepdims=True))
        probs = jnp.exp2((scores - new_top) * factor)
        rescale = jnp.exp2((top - new_top) * factor)
        norm = norm * rescale + jnp.sum(probs, axis=0, keepdims=True)
        acc = acc * rescale + dot_tn(v_blk, probs.astype(jnp.bfloat16))
        return new_top, norm, acc

    top, norm, acc = lax.fori_loop(0, blk, step, (top, norm, acc))
    o_ref[...] = (acc / norm).T.astype(jnp.bfloat16)
    lse_ref[...] = top * factor + jnp.log2(norm)


def attend(q, k, v):
    rows, head_dim = q.shape
    block = min(512, rows // 4)
    whole = pl.BlockSpec((rows, head_dim), lambda i: (0, 0))
    part = pl.BlockSpec((block, head_dim), lambda i: (i, 0))
    return pl.pallas_call(
        functools.partial(attend_kernel, block, head_dim ** -0.5 * LOG2E),
        grid=(rows // block,),
        out_shape=(jax.ShapeDtypeStruct(q.shape, jnp.bfloat16), jax.ShapeDtypeStruct((1, rows), jnp.float32)),
        in_specs=[part, whole, whole],
        out_specs=(part, pl.BlockSpec((1, block), lambda i: (0, i))),
        compiler_params=pltpu.CompilerParams(vmem_limit_bytes=VMEM_LIMIT),
        cost_estimate=pl.CostEstimate(flops=2 * rows * rows * head_dim, bytes_accessed=8 * rows * head_dim, transcendentals=rows * rows // 2),
        name="attend",
    )(q, k, v)


def attend_back_kernel(block, scale, q_ref, k_ref, v_ref, o_ref, do_ref, lse_ref, dq_ref, dk_ref, dv_ref, delta_ref, dk_acc, dv_acc):
    blk = pl.program_id(0)
    n_blk = pl.num_programs(0)
    factor = scale * LOG2E

    @pl.when(blk == 0)
    def _():
        def prepare(idx, carry):
            rows = pl.ds(pl.multiple_of(idx * block, block), block)
            prod = do_ref[rows, :].astype(jnp.float32) * o_ref[rows, :].astype(jnp.float32)
            delta_ref[:, rows] = jnp.sum(prod.T, axis=0, keepdims=True)
            dq_ref[rows, :] = jnp.zeros((block, dq_ref.shape[1]), jnp.float32)
            return carry

        lax.fori_loop(0, n_blk, prepare, 0)

    k_blk = k_ref[...]
    v_blk = v_ref[...]

    def one(idx, masked):
        rows = pl.ds(pl.multiple_of(idx * block, block), block)
        q_blk = q_ref[rows, :]
        do_blk = do_ref[rows, :]
        scores = dot_nt(k_blk, q_blk)
        if masked:
            scores = causal_mask(scores)
        probs = jnp.exp2(scores * factor - lse_ref[:, rows])
        grad_v = dot_nn(probs.astype(jnp.bfloat16), do_blk)
        grad_p = dot_nt(v_blk, do_blk)
        grad_s = (probs * ((grad_p - delta_ref[:, rows]) * scale)).astype(jnp.bfloat16)
        dq_ref[rows, :] += dot_tn(grad_s, k_blk)
        return dot_nn(grad_s, q_blk), grad_v

    dk_acc[...], dv_acc[...] = one(blk, True)

    def step(idx, carry):
        grad_k, grad_v = one(idx, False)
        dk_acc[...] += grad_k
        dv_acc[...] += grad_v
        return carry

    lax.fori_loop(blk + 1, n_blk, step, 0)
    dk_ref[...] = dk_acc[...]
    dv_ref[...] = dv_acc[...].astype(jnp.bfloat16)


def attend_back(q, k, v, o, do, lse):
    rows, head_dim = q.shape
    block = min(512, rows // 4)
    whole = pl.BlockSpec((rows, head_dim), lambda i: (0, 0))
    part = pl.BlockSpec((block, head_dim), lambda i: (i, 0))
    stat = pl.BlockSpec((1, rows), lambda i: (0, 0))
    return pl.pallas_call(
        functools.partial(attend_back_kernel, block, head_dim ** -0.5),
        grid=(rows // block,),
        out_shape=(jax.ShapeDtypeStruct(q.shape, jnp.float32), jax.ShapeDtypeStruct(q.shape, jnp.float32), jax.ShapeDtypeStruct(q.shape, jnp.bfloat16)),
        in_specs=[whole, part, part, whole, whole, stat],
        out_specs=(whole, part, part),
        scratch_shapes=[pltpu.VMEM((1, rows), jnp.float32), pltpu.VMEM((block, head_dim), jnp.float32), pltpu.VMEM((block, head_dim), jnp.float32)],
        compiler_params=pltpu.CompilerParams(vmem_limit_bytes=VMEM_LIMIT),
        cost_estimate=pl.CostEstimate(flops=5 * rows * rows * head_dim, bytes_accessed=20 * rows * head_dim, transcendentals=rows * rows // 2),
        name="attend_back",
    )(q, k, v, o, do, lse)


def post_kernel(o_ref, mine_ref, other_ref, x_any, gy_any, pw_ref, y_ref, gp_ref, do_ref, gpost_ref, x_ref, gy_ref, sems):
    tp_size, heads, _, head_dim = o_ref.shape
    block = x_ref.shape[0]
    first_row = (lax.axis_index("tp") * pl.num_programs(0) + pl.program_id(0)) * block
    loads = []
    for idx, (src, dst) in enumerate(((x_any, x_ref), (gy_any, gy_ref))):
        load = pltpu.make_async_copy(src.at[pl.ds(pl.multiple_of(first_row, block), block)], dst, sems.at[idx])
        load.start()
        loads.append(load)
    core = lax.rem(lax.axis_index("cp"), 2)
    halves = ((mine_ref, core * (heads // 2)), (other_ref, (1 - core) * (heads // 2)))
    proj = None
    for idx in range(tp_size):
        for w_ref, start in halves:
            term = dot_nn(jnp.concatenate([o_ref[idx, start + head] for head in range(heads // 2)], axis=1), w_ref[idx])
            proj = term if proj is None else proj + term
    for load in loads:
        load.wait()
    gain = pw_ref[...]
    inv = lax.rsqrt(jnp.mean(proj * proj, axis=-1, keepdims=True) + NORM_EPS)
    hat = proj * inv
    y_ref[...] = (x_ref[...].astype(jnp.float32) + hat * gain).astype(jnp.bfloat16)
    grad = gy_ref[...].astype(jnp.float32)
    gpost = jnp.sum(grad * hat, axis=0, keepdims=True)
    grad_hat = grad * gain
    grad_proj = (inv * (grad_hat - hat * jnp.mean(grad_hat * hat, axis=-1, keepdims=True))).astype(jnp.bfloat16)
    gp_ref[...] = grad_proj
    for idx in range(tp_size):
        for w_ref, start in halves:
            grad_o = dot_nt(grad_proj, w_ref[idx]).astype(jnp.bfloat16)
            for head in range(heads // 2):
                do_ref[idx, start + head] = grad_o[:, head * head_dim:(head + 1) * head_dim]

    @pl.when(pl.program_id(0) == 0)
    def _():
        gpost_ref[...] = jnp.zeros_like(gpost_ref)

    gpost_ref[...] += gpost


def post(o_all, wo_mine, wo_other, x, gy, gain):
    tp_size, heads, rows, head_dim = o_all.shape
    d_model = x.shape[1]
    block = min(128, rows)
    any_spec = pl.BlockSpec(memory_space=pl.ANY)
    piece = pltpu.VMEM((block, d_model), jnp.bfloat16)
    act = pl.BlockSpec((block, d_model), lambda i: (i, 0))
    by_head = pl.BlockSpec((tp_size, heads, block, head_dim), lambda i: (0, 0, i, 0))
    act_shape = jax.ShapeDtypeStruct((rows, d_model), jnp.bfloat16)
    return pl.pallas_call(
        post_kernel,
        grid=(rows // block,),
        out_shape=(act_shape, act_shape, jax.ShapeDtypeStruct(o_all.shape, jnp.bfloat16), jax.ShapeDtypeStruct((1, d_model), jnp.float32)),
        in_specs=[by_head] + [pl.BlockSpec(wo_mine.shape, lambda i: (0, 0, 0))] * 2 + [any_spec, any_spec, pl.BlockSpec((1, d_model), lambda i: (0, 0))],
        out_specs=(act, act, by_head, pl.BlockSpec((1, d_model), lambda i: (0, 0))),
        scratch_shapes=[piece, piece, pltpu.SemaphoreType.DMA((2,))],
        compiler_params=pltpu.CompilerParams(vmem_limit_bytes=VMEM_LIMIT),
        cost_estimate=pl.CostEstimate(flops=4 * rows * d_model * d_model, bytes_accessed=4 * d_model * d_model, transcendentals=rows),
        name="post",
    )(o_all, wo_mine, wo_other, x, gy, gain)


def output_weights_kernel(o_ref, gp_ref, out_ref):
    heads, _, head_dim = o_ref.shape
    acc = dot_tn(jnp.concatenate([o_ref[head] for head in range(heads)], axis=1), gp_ref[...])
    for head in range(heads):
        out_ref[head] = acc[head * head_dim:(head + 1) * head_dim, :]


def output_weights(o_heads, grad_proj):
    heads, rows, head_dim = o_heads.shape
    d_model = grad_proj.shape[1]
    block = min(512, d_model)
    return pl.pallas_call(
        output_weights_kernel,
        grid=(d_model // block,),
        out_shape=jax.ShapeDtypeStruct((heads, head_dim, d_model), jnp.float32),
        in_specs=[pl.BlockSpec(o_heads.shape, lambda i: (0, 0, 0)), pl.BlockSpec((rows, block), lambda i: (0, i))],
        out_specs=pl.BlockSpec((heads, head_dim, block), lambda i: (0, 0, i)),
        compiler_params=pltpu.CompilerParams(vmem_limit_bytes=VMEM_LIMIT),
        cost_estimate=pl.CostEstimate(flops=2 * rows * d_model * heads * head_dim, bytes_accessed=12 * rows * d_model, transcendentals=0),
        name="output_weights",
    )(o_heads, grad_proj)


def spread_kernel(in_ref, *out_refs):
    for number, out_ref in enumerate(out_refs):
        for head in range(in_ref.shape[0]):
            out_ref[:, head, :] = in_ref[head, number]


def spread(gathered):
    heads, count, d_model, head_dim = gathered.shape
    block = min(256, d_model)
    return pl.pallas_call(
        spread_kernel,
        grid=(d_model // block,),
        out_shape=tuple([jax.ShapeDtypeStruct((d_model, heads, head_dim), gathered.dtype)] * count),
        in_specs=[pl.BlockSpec((heads, count, block, head_dim), lambda i: (0, 0, i, 0))],
        out_specs=tuple([pl.BlockSpec((block, heads, head_dim), lambda i: (i, 0, 0))] * count),
        compiler_params=pltpu.CompilerParams(vmem_limit_bytes=VMEM_LIMIT),
        cost_estimate=pl.CostEstimate(flops=d_model * heads * head_dim * count, bytes_accessed=8 * d_model * heads * head_dim * count, transcendentals=0),
        name="spread",
    )(gathered)


def chain_kernel(size, n_chunk, lag, tile, dq_ref, dk_ref, dv_ref, wq_ref, wk_ref, wv_ref, gy_ref, out_ref, part_ref, sums_a, sums_b, rs_send, rs_recv, ag_send, ag_recv):
    me = lax.axis_index("tp")
    entry_barrier("tp", size)
    half = part_ref.shape[0] // 2
    rows = half // n_chunk
    last = size - 1

    def parts(side, chunk):
        local = pl.ds(pl.multiple_of(chunk * rows, rows), rows)
        glob = pl.ds(pl.multiple_of(side * half + chunk * rows, rows), rows)
        sums = (sums_a, sums_b)[side]
        return local, glob, sums

    def toward(side):
        return jnp.maximum(me - 1, 0) if side == 0 else jnp.minimum(me + 1, last)

    def away(side):
        return jnp.minimum(me + 1, last) if side == 0 else jnp.maximum(me - 1, 0)

    def rs_copy(side, chunk, first):
        local, glob, sums = parts(side, chunk)
        return pltpu.make_async_remote_copy(
            src_ref=part_ref.at[glob] if first else sums.at[local], dst_ref=sums.at[local],
            send_sem=rs_send.at[side, chunk], recv_sem=rs_recv.at[side, chunk],
            device_id={"tp": toward(side)}, device_id_type=MESH)

    def ag_copy(side, chunk):
        _, glob, _ = parts(side, chunk)
        return pltpu.make_async_remote_copy(
            src_ref=out_ref.at[glob], dst_ref=out_ref.at[glob],
            send_sem=ag_send.at[side, chunk], recv_sem=ag_recv.at[side, chunk],
            device_id={"tp": away(side)}, device_id_type=MESH)

    def place(side):
        return me if side == 0 else last - me

    heads = dq_ref.shape[0]
    d_model = out_ref.shape[1]
    block = min(512, d_model)
    n_tile = 2 * half // tile
    per_tile = tile // rows

    def push(number):
        for side in (0, 1):
            @pl.when((lax.rem(number, 2) == side) & (place(side) == last))
            def _(side=side):
                def one(idx, carry):
                    rs_copy(side, (number // 2) * per_tile + idx, True).start()
                    return carry

                lax.fori_loop(0, per_tile, one, 0)

    def product(number, carry):
        tile_rows = pl.ds(pl.multiple_of(lax.rem(number, 2) * half + (number // 2) * tile, tile), tile)

        def columns(idx, carry):
            cols = pl.ds(pl.multiple_of(idx * block, block), block)
            total = None
            for grad_ref, w_ref in ((dq_ref, wq_ref), (dk_ref, wk_ref), (dv_ref, wv_ref)):
                grad = jnp.concatenate([grad_ref[idx_h, tile_rows, :] for idx_h in range(heads)], axis=1)
                term = dot_nn(grad, w_ref[:, cols])
                total = term if total is None else total + term
            part_ref[tile_rows, cols] = total
            return carry

        lax.fori_loop(0, d_model // block, columns, 0)

        @pl.when(number > 0)
        def _():
            push(number - 1)

        return carry

    lax.fori_loop(0, n_tile, product, 0)
    push(jnp.int32(n_tile - 1))

    def pass_on(side, chunk):
        local, glob, sums = parts(side, chunk)
        rs_copy(side, chunk, False).wait_recv()
        sums[local] = sums[local] + part_ref[glob]
        rs_copy(side, chunk, False).start()

    def finish(side, chunk):
        local, glob, sums = parts(side, chunk)
        rs_copy(side, chunk, False).wait_recv()
        out_ref[glob] = (gy_ref[glob].astype(jnp.float32) + (sums[local] + part_ref[glob])).astype(jnp.bfloat16)
        ag_copy(side, chunk).start()

    def reduce_step(idx, carry):
        for far in range(last - 1, 0, -1):
            chunk = idx - (last - 1 - far) * lag
            for side in (0, 1):
                @pl.when((chunk >= 0) & (chunk < n_chunk) & (place(side) == far))
                def _(side=side, chunk=chunk):
                    pass_on(side, chunk)
        for side in (0, 1):
            @pl.when((idx < n_chunk) & (place(side) == 0))
            def _(side=side):
                finish(side, idx)
        return carry

    lax.fori_loop(0, n_chunk + (last - 2) * lag, reduce_step, 0)

    def return_step(idx, carry):
        for far in range(1, last + 1):
            chunk = idx - (far - 1) * lag
            for side in (0, 1):
                @pl.when((chunk >= 0) & (chunk < n_chunk) & (place(side) == far))
                def _(side=side, chunk=chunk, far=far):
                    ag_copy(side, chunk).wait_recv()
                    if far < last:
                        ag_copy(side, chunk).start()
        return carry

    lax.fori_loop(0, n_chunk + (last - 1) * lag, return_step, 0)

    def drain(idx, carry):
        for side in (0, 1):
            @pl.when(place(side) > 0)
            def _(side=side):
                rs_copy(side, idx, False).wait_send()

            @pl.when(place(side) < last)
            def _(side=side):
                ag_copy(side, idx).wait_send()
        return carry

    lax.fori_loop(0, n_chunk, drain, 0)


def chain_sum(size, collective_id, grads, weights, gy):
    rows, d_model = gy.shape
    n_chunk = 32 if rows >= 512 else 4
    sems = [pltpu.SemaphoreType.DMA((2, n_chunk))] * 4
    return pl.pallas_call(
        functools.partial(chain_kernel, size, n_chunk, 2, min(256, rows // 4)),
        out_shape=jax.ShapeDtypeStruct((rows, d_model), jnp.bfloat16),
        in_specs=[VMEM_SPEC] * 7,
        out_specs=VMEM_SPEC,
        scratch_shapes=[pltpu.VMEM((rows, d_model), jnp.float32), pltpu.VMEM((rows // 2, d_model), jnp.float32), pltpu.VMEM((rows // 2, d_model), jnp.float32)] + sems,
        compiler_params=pltpu.CompilerParams(collective_id=collective_id, has_side_effects=True, vmem_limit_bytes=VMEM_LIMIT),
        cost_estimate=pl.CostEstimate(flops=10 ** 11, bytes_accessed=16 * rows * d_model, transcendentals=0),
        name="chain_sum",
    )(*grads, *weights, gy)


def weights_back_kernel(full_width, sub, x_ref, far0_ref, far1_ref, far2_ref, wq_ref, wk_ref, dq_ref, dk_ref, dv_ref, cos_ref, sin_ref, qg_ref, kg_ref, post_ref,
                        dw_ref, exq_ref, exk_ref, exv_ref, gains_ref, post_out,
                        x_buf, wqk_ref, lin_ref, q16_ref, k16_ref, own, slots_tp, mid, slots_cp, done, total, gq_ref, gk_ref, my_gains,
                        x_sem, w_sem, pair_send, pair_recv, tp_send, tp_recv, cp_send, cp_recv, back_send, back_recv, ex_send, ex_recv):
    me = lax.axis_index("cp")
    my_tp = lax.axis_index("tp")
    rows, head_dim = dq_ref.shape[1:]
    loads = []
    step = far0_ref.shape[0]
    fars = ((far0_ref, pl.ds(0, step)), (far1_ref, pl.ds(step, step)), (far2_ref, pl.ds(2 * step, rows - 2 * step)))
    pieces = ((x_ref, 0, pl.ds(0, rows)),) + tuple((ref, 2, part) for ref, part in fars)
    for idx, (src, dist, part) in enumerate(pieces):
        load = pltpu.make_async_copy(src, x_buf.at[dist, part], x_sem.at[idx])
        load.start()
        loads.append(load)
    own_rows = pl.ds(pl.multiple_of(me * head_dim, head_dim), head_dim)
    w_loads = [pltpu.make_async_copy(src.at[own_rows], wqk_ref.at[pl.ds(idx * head_dim, head_dim)], w_sem.at[idx]) for idx, src in enumerate((wq_ref, wk_ref))]
    for load in w_loads:
        load.start()
    peers_barrier()
    for idx, (src, dist, part) in enumerate(pieces):
        load = pltpu.make_async_remote_copy(
            src_ref=src, dst_ref=x_buf.at[dist + 1, part], send_sem=pair_send.at[idx], recv_sem=pair_recv.at[idx],
            device_id={"cp": flip(me, 1)}, device_id_type=MESH)
        load.start()
        loads.append(load)
    own[4:5, :] = jnp.zeros_like(own[4:5, :])
    own[4:5, 0:post_ref.shape[1]] = post_ref[...]

    def ex_copy(idx, src, dst, dist):
        peer = flip(me, dist)
        return pltpu.make_async_remote_copy(
            src_ref=src.at[peer], dst_ref=dst.at[me], send_sem=ex_send.at[idx, dist - 1], recv_sem=ex_recv.at[idx, dist - 1],
            device_id={"cp": peer}, device_id_type=MESH)

    copies = [ex_copy(2, dv_ref, exv_ref, dist) for dist in (2, 3, 1)]
    for copy in copies:
        copy.start()

    def grad_of(ref, blk, part, table):
        g = ref[blk, part, :]
        return g * cos_ref[table, :] - turn(g) * sin_ref[table, :]

    w_loads[0].wait()
    w_loads[1].wait()
    sides = ((dq_ref, qg_ref, 0), (dk_ref, kg_ref, 1))
    for order, dist in enumerate((0, 2, 1, 3)):
        blk = flip(me, dist)
        for load in (loads[0:1], loads[1:4], loads[4:5], loads[5:8])[order]:
            if order < 2:
                load.wait()
            else:
                load.wait_recv()

        def first(idx, carry, dist=dist, blk=blk):
            part = pl.ds(pl.multiple_of(idx * sub, sub), sub)
            table = pl.ds(pl.multiple_of(blk * rows + idx * sub, sub), sub)
            lin = dot_nt(x_buf[dist, part, :], wqk_ref[...])
            lin_ref[dist, part, :] = lin
            for ref, gain_ref, number in sides:
                mine = lin[:, number * head_dim:(number + 1) * head_dim]
                grad = grad_of(ref, blk, part, table) * gain_ref[...]
                own[2 * number:2 * number + 1, table] = jnp.sum((mine * mine).T, axis=0, keepdims=True)
                own[2 * number + 1:2 * number + 2, table] = jnp.sum((grad * mine).T, axis=0, keepdims=True)
            return carry

        lax.fori_loop(0, rows // sub, first, 0)

    quarter = own.shape[1] // 4

    def quarter_of(which):
        return pl.ds(pl.multiple_of(which * quarter, quarter), quarter)

    moves = []
    for shift in (2, 1, 3):
        peer = lax.rem(my_tp + shift, 4)
        move = pltpu.make_async_remote_copy(
            src_ref=own.at[:, quarter_of(peer)], dst_ref=slots_tp.at[my_tp], send_sem=tp_send.at[shift - 1], recv_sem=tp_recv.at[shift - 1],
            device_id={"tp": peer}, device_id_type=MESH)
        move.start()
        moves.append(move)
    slots_tp[my_tp] = own[:, quarter_of(my_tp)]
    for move in moves:
        move.wait()
    mid[...] = slots_tp[0] + slots_tp[1] + slots_tp[2] + slots_tp[3]
    moves = []
    for dist in (2, 3, 1):
        move = pltpu.make_async_remote_copy(
            src_ref=mid, dst_ref=slots_cp.at[me], send_sem=cp_send.at[dist - 1], recv_sem=cp_recv.at[dist - 1],
            device_id={"cp": flip(me, dist)}, device_id_type=MESH)
        move.start()
        moves.append(move)
    slots_cp[me] = mid[...]
    for move in moves:
        move.wait()
    done[...] = slots_cp[0] + slots_cp[1] + slots_cp[2] + slots_cp[3]
    moves = []
    for shift in (2, 1, 3):
        move = pltpu.make_async_remote_copy(
            src_ref=done, dst_ref=total.at[:, quarter_of(my_tp)], send_sem=back_send.at[shift - 1], recv_sem=back_recv.at[shift - 1],
            device_id={"tp": lax.rem(my_tp + shift, 4)}, device_id_type=MESH)
        move.start()
        moves.append(move)
    total[:, quarter_of(my_tp)] = done[...]
    for move in moves:
        move.wait()

    post_out[...] = total[4:5, 0:post_ref.shape[1]]
    gq_ref[...] = jnp.zeros_like(gq_ref)
    gk_ref[...] = jnp.zeros_like(gk_ref)
    outs = ((q16_ref, exq_ref, gq_ref), (k16_ref, exk_ref, gk_ref))
    for dist in (2, 3, 1, 0):
        blk = flip(me, dist)

        def second(idx, carry, dist=dist, blk=blk):
            part = pl.ds(pl.multiple_of(idx * sub, sub), sub)
            table = pl.ds(pl.multiple_of(blk * rows + idx * sub, sub), sub)
            lin = lin_ref[dist, part, :]
            for (ref, gain_ref, number), (d16_ref, _, gain_out) in zip(sides, outs):
                mine = lin[:, number * head_dim:(number + 1) * head_dim]
                inv = lax.rsqrt(total[2 * number:2 * number + 1, table] / full_width + NORM_EPS)
                dot = inv * total[2 * number + 1:2 * number + 2, table] / full_width
                inv = jnp.broadcast_to(inv, (head_dim, sub)).T
                dot = jnp.broadcast_to(dot, (head_dim, sub)).T
                raw = grad_of(ref, blk, part, table)
                hat = mine * inv
                d16_ref[blk, part, :] = (inv * (raw * gain_ref[...] - hat * dot)).astype(jnp.bfloat16)
                gain_out[...] += jnp.sum(raw * hat, axis=0, keepdims=True)
            return carry

        lax.fori_loop(0, rows // sub, second, 0)
        if dist:
            for idx, (d16_ref, ex_ref, _) in enumerate(outs):
                copy = ex_copy(idx, d16_ref, ex_ref, dist)
                copy.start()
                copies.append(copy)
    my_gains[0:1, :] = gq_ref[...]
    my_gains[1:2, :] = gk_ref[...]
    for src, dst in ((q16_ref, exq_ref), (k16_ref, exk_ref), (dv_ref, exv_ref)):
        dst[me] = src[me]
    gains_ref[me] = my_gains[...]
    for dist in (1, 2, 3):
        copy = pltpu.make_async_remote_copy(
            src_ref=my_gains, dst_ref=gains_ref.at[me], send_sem=ex_send.at[3, dist - 1], recv_sem=ex_recv.at[3, dist - 1],
            device_id={"cp": flip(me, dist)}, device_id_type=MESH)
        copy.start()
        copies.append(copy)

    block = min(512, x_buf.shape[2])

    def weight_step(idx, carry):
        cols = pl.ds(pl.multiple_of(idx * block, block), block)
        acc = None
        for dist in range(4):
            blk = flip(me, dist)
            grads = jnp.concatenate([q16_ref[blk], k16_ref[blk], dv_ref[blk]], axis=1)
            term = dot_tn(grads, x_buf[dist, :, cols])
            acc = term if acc is None else acc + term
        acc = acc.T
        for number in range(3):
            dw_ref[number, cols, :] = acc[:, number * head_dim:(number + 1) * head_dim]
        return carry

    lax.fori_loop(0, x_buf.shape[2] // block, weight_step, 0)
    for copy in copies:
        copy.wait()
    for load in loads[4:]:
        load.wait_send()


def weights_back(collective_id, full_width, x, x_far, wq, wk, dq, dk, dv, cos_tab, sin_tab, q_gain, k_gain, grad_post):
    _, rows, head_dim = dq.shape
    d_model = x.shape[1]
    any_spec = pl.BlockSpec(memory_space=pl.ANY)
    dma = pltpu.SemaphoreType.DMA
    span = max(4 * rows, d_model)
    stat = pltpu.VMEM((5, span), jnp.float32)
    slots = pltpu.VMEM((4, 5, span // 4), jnp.float32)
    small = pltpu.VMEM((5, span // 4), jnp.float32)
    ex = jax.ShapeDtypeStruct(dq.shape, jnp.bfloat16)
    return pl.pallas_call(
        functools.partial(weights_back_kernel, full_width, min(512, rows)),
        out_shape=(jax.ShapeDtypeStruct((3, d_model, head_dim), jnp.float32), ex, ex, ex,
                   jax.ShapeDtypeStruct((4, 2, head_dim), jnp.float32), jax.ShapeDtypeStruct((1, d_model), jnp.float32)),
        in_specs=[any_spec] * 6 + [VMEM_SPEC] * 8,
        out_specs=tuple([VMEM_SPEC] * 6),
        scratch_shapes=[pltpu.VMEM((4, rows, d_model), jnp.bfloat16), pltpu.VMEM((2 * head_dim, d_model), jnp.bfloat16), pltpu.VMEM((4, rows, 2 * head_dim), jnp.float32),
                        pltpu.VMEM(dq.shape, jnp.bfloat16), pltpu.VMEM(dq.shape, jnp.bfloat16),
                        stat, slots, small, slots, small, stat,
                        pltpu.VMEM((1, head_dim), jnp.float32), pltpu.VMEM((1, head_dim), jnp.float32), pltpu.VMEM((2, head_dim), jnp.float32),
                        dma((4,)), dma((2,)), dma((4,)), dma((4,)), dma((3,)), dma((3,)), dma((3,)), dma((3,)), dma((3,)), dma((3,)), dma((4, 3)), dma((4, 3))],
        compiler_params=pltpu.CompilerParams(collective_id=collective_id, has_side_effects=True, vmem_limit_bytes=VMEM_LIMIT),
        name="weights_back",
    )(x, *x_far, wq, wk, dq, dk, dv, cos_tab, sin_tab, q_gain, k_gain, grad_post)


def solution(mesh):
    tp_size = mesh.shape["tp"]
    cp_size = mesh.shape["cp"]
    act_spec = P("dp", "cp", None)
    col_spec = P(None, "tp", None)
    part_col = P("dp", "tp", None)
    in_specs = (act_spec, col_spec, col_spec, col_spec, P("tp", None, None), P("tp", None), P("tp", None), P(None), act_spec)
    out_specs = (act_spec, act_spec, part_col, part_col, part_col, P(("dp", "tp"), None, None), P(("dp", "tp"), None), P(("dp", "tp"), None), P("dp"))
    swap_core = [(dev, dev ^ 1) for dev in range(cp_size)]

    def local_run(x_in, w_q, w_k, w_v, w_o, q_norm_w, k_norm_w, post_norm_w, grad_y):
        rows, d_model = x_in.shape[1:]
        heads, head_dim = w_q.shape[1:]
        width = heads * head_dim
        full_width = width * tp_size
        x = x_in[0]
        gy = grad_y[0]
        cp_index = lax.axis_index("cp")

        def wide_tables(cos_tab, sin_tab):
            return jnp.concatenate([cos_tab, cos_tab], axis=1), jnp.concatenate([-sin_tab, sin_tab], axis=1)

        cos_tab, sin_tab = wide_tables(*rope_tables((cp_index * rows + jnp.arange(rows)).astype(jnp.float32), head_dim))
        turned = tuple(w.reshape(d_model, width).T for w in (w_q, w_k, w_v))

        core = cp_index % 2
        own_half = lax.dynamic_slice_in_dim(w_o, core * (heads // 2), heads // 2, axis=0)
        wo_mine = lax.all_gather(own_half, "tp").reshape(tp_size, width // 2, d_model)
        q_seq, k_seq, v_seq = front(1, full_width, x, turned, cos_tab, sin_tab, q_norm_w, k_norm_w)
        seq_shape = (cp_size * rows, head_dim)
        block_shape = (cp_size, rows, head_dim)
        piece = rows // 4

        def fetch(start, size):
            return lax.ppermute(x_free[start:start + size], "cp", [(dev, dev ^ 2) for dev in range(cp_size)])

        q_seq, x_free = lax.optimization_barrier((q_seq, x))
        far0 = fetch(0, piece)
        q_seq, k_seq, v_seq = (t.reshape(seq_shape) for t in (q_seq, k_seq, v_seq))
        o_seq, lse = attend(q_seq, k_seq, v_seq)
        o_seq, wo_mine = lax.optimization_barrier((o_seq, wo_mine))
        wo_other = lax.ppermute(wo_mine, "cp", swap_core)
        o_heads, o_tokens = heads_to_tokens(2, o_seq.reshape(block_shape))
        o_tokens, x_free = lax.optimization_barrier((o_tokens, x))
        far1 = fetch(piece, piece)
        y_mine, gp_mine, do_tokens, grad_post = post(o_tokens, wo_mine, wo_other, x, gy, post_norm_w[None, :])
        do_seq = tokens_to_heads(3, do_tokens)
        y_mine, gp_mine, do_seq, x_free = lax.optimization_barrier((y_mine, gp_mine, do_seq, x))
        grad_proj = lax.all_gather(gp_mine, "tp", tiled=True)
        far2 = fetch(2 * piece, rows - 2 * piece)

        coarse_cos, coarse_sin = rope_tables(jnp.arange(0, cp_size * rows, 64, dtype=jnp.float32), head_dim)
        fine_cos, fine_sin = (jnp.concatenate([t, t], axis=1)[None] for t in rope_tables(jnp.arange(64, dtype=jnp.float32), head_dim))
        wide_cos, wide_sin, sign_cos, sign_sin = lax.optimization_barrier(tuple(
            jnp.concatenate([sign * t, t], axis=1)[:, None, :] for sign in (1.0, -1.0) for t in (coarse_cos, coarse_sin)))
        fine_cos, fine_sin = lax.optimization_barrier((fine_cos, fine_sin))
        seq_cos = (wide_cos * fine_cos - wide_sin * fine_sin).reshape(cp_size * rows, head_dim)
        seq_sin = (sign_sin * fine_cos + sign_cos * fine_sin).reshape(cp_size * rows, head_dim)
        gains_head = tuple(lax.dynamic_slice_in_dim(w, cp_index, 1, axis=0) for w in (q_norm_w, k_norm_w))
        dq_seq, dk_seq, dv_seq = attend_back(q_seq, k_seq, v_seq, o_seq, do_seq.reshape(seq_shape), lse)
        y_mine, dq_seq = lax.optimization_barrier((y_mine, dq_seq))
        y_out = lax.all_gather(y_mine, "tp", tiled=True)
        dw, dq16, dk16, dv16, gains, grad_post = weights_back(
            4, full_width, x, (far0, far1, far2), turned[0], turned[1],
            dq_seq.reshape(block_shape), dk_seq.reshape(block_shape), dv_seq.reshape(block_shape), seq_cos, seq_sin, *gains_head, grad_post)
        o_heads, dw = lax.optimization_barrier((o_heads, dw))
        grad_w_o = lax.psum(output_weights(o_heads, grad_proj), "cp")
        dw = spread(lax.all_gather(dw, "cp"))
        grad_x = chain_sum(tp_size, 6, (dq16, dk16, dv16), turned, gy)
        return (y_out[None], grad_x[None]) + tuple(dw) + (grad_w_o, gains[:, 0], gains[:, 1], grad_post[0])

    return jax.shard_map(local_run, mesh=mesh, in_specs=in_specs, out_specs=out_specs, check_vma=False)
```

```python
import functools

import jax
import jax.numpy as jnp
from jax import lax
from jax.experimental import pallas as pl
from jax.experimental.pallas import tpu as pltpu
from jax.sharding import PartitionSpec as P


ROPE_THETA = 500000.0
NORM_EPS = 1e-6
MASK_VALUE = -1e30
LOG2E = 1.4426950408889634
MESH = pl.DeviceIdType.MESH
VMEM_SPEC = pl.BlockSpec(memory_space=pltpu.VMEM)
VMEM_LIMIT = 60 * 1024 * 1024
NT = (((1,), (1,)), ((), ()))
TN = (((0,), (0,)), ((), ()))


def dot_nt(a, b):
    return lax.dot_general(a, b, NT, preferred_element_type=jnp.float32)


def dot_tn(a, b):
    return lax.dot_general(a, b, TN, preferred_element_type=jnp.float32)


def dot_nn(a, b):
    return jnp.dot(a, b, preferred_element_type=jnp.float32)


def rope_tables(positions, head_dim):
    half_dim = head_dim // 2
    inv_freq = ROPE_THETA ** (-2.0 * jnp.arange(half_dim, dtype=jnp.float32) / head_dim)
    angles = positions[:, None] * inv_freq[None, :]
    return jnp.cos(angles), jnp.sin(angles)


def entry_barrier(axis, size):
    me = lax.axis_index(axis)
    barrier = pltpu.get_barrier_semaphore()
    for shift in range(1, size):
        pl.semaphore_signal(barrier, inc=1, device_id={axis: lax.rem(me + shift, size)}, device_id_type=MESH)
    pl.semaphore_wait(barrier, size - 1)


def peers_barrier():
    me, my_tp = lax.axis_index("cp"), lax.axis_index("tp")
    barrier = pltpu.get_barrier_semaphore()
    for shift in (1, 2, 3):
        pl.semaphore_signal(barrier, inc=1, device_id={"cp": lax.rem(me + shift, 4)}, device_id_type=MESH)
        pl.semaphore_signal(barrier, inc=1, device_id={"tp": lax.rem(my_tp + shift, 4)}, device_id_type=MESH)
    pl.semaphore_wait(barrier, 6)


def flip(index, distance):
    if distance == 1:
        return index + 1 - 2 * lax.rem(index, 2)
    if distance == 2:
        return lax.rem(index + 2, 4)
    return 3 - index if distance == 3 else index


def heads_to_tokens_kernel(in_ref, heads_ref, tokens_ref, cp_send, cp_recv, tp_send, tp_recv):
    me, my_tp = lax.axis_index("cp"), lax.axis_index("tp")
    quarter = in_ref.shape[1] // 4
    peers_barrier()
    first = {}
    for dist in (1, 2, 3):
        peer = flip(me, dist)
        first[dist] = pltpu.make_async_remote_copy(
            src_ref=in_ref.at[peer], dst_ref=heads_ref.at[me], send_sem=cp_send.at[dist - 1], recv_sem=cp_recv.at[dist - 1],
            device_id={"cp": peer}, device_id_type=MESH)
        first[dist].start()

    def rows_of(which):
        return pl.ds(pl.multiple_of(which * quarter, quarter), quarter)

    second = []

    def forward(dist, src_ref, head):
        for shift in (2, 1, 3):
            peer = lax.rem(my_tp + shift, 4)
            copy = pltpu.make_async_remote_copy(
                src_ref=src_ref.at[head, rows_of(peer)], dst_ref=tokens_ref.at[my_tp, head],
                send_sem=tp_send.at[dist, shift - 1], recv_sem=tp_recv.at[dist, shift - 1],
                device_id={"tp": peer}, device_id_type=MESH)
            copy.start()
            second.append(copy)
        tokens_ref[my_tp, head] = src_ref[head, rows_of(my_tp)]

    forward(0, in_ref, me)
    heads_ref[me] = in_ref[me]
    for dist in (1, 2, 3):
        first[dist].wait_recv()
        forward(dist, heads_ref, flip(me, dist))
    for dist in (1, 2, 3):
        first[dist].wait_send()
    for copy in second:
        copy.wait()


def heads_to_tokens(collective_id, array):
    _, rows, head_dim = array.shape
    dma = pltpu.SemaphoreType.DMA
    return pl.pallas_call(
        heads_to_tokens_kernel,
        out_shape=(jax.ShapeDtypeStruct(array.shape, array.dtype), jax.ShapeDtypeStruct((4, 4, rows // 4, head_dim), array.dtype)),
        in_specs=[VMEM_SPEC],
        out_specs=(VMEM_SPEC, VMEM_SPEC),
        scratch_shapes=[dma((3,)), dma((3,)), dma((4, 3)), dma((4, 3))],
        compiler_params=pltpu.CompilerParams(collective_id=collective_id, has_side_effects=True, vmem_limit_bytes=VMEM_LIMIT),
        name="heads_to_tokens",
    )(array)


def tokens_to_heads_kernel(in_ref, seq_ref, block_ref, tp_send, tp_recv, cp_send, cp_recv):
    me, my_tp = lax.axis_index("cp"), lax.axis_index("tp")
    quarter = in_ref.shape[2]
    peers_barrier()
    first = {}
    for shift in (2, 1, 3):
        peer = lax.rem(my_tp + shift, 4)
        first[shift] = pltpu.make_async_remote_copy(
            src_ref=in_ref.at[peer], dst_ref=block_ref.at[my_tp], send_sem=tp_send.at[shift - 1], recv_sem=tp_recv.at[shift - 1],
            device_id={"tp": peer}, device_id_type=MESH)
        first[shift].start()
    second = []

    def forward(shift, src_ref, which):
        rows = pl.ds(pl.multiple_of(which * quarter, quarter), quarter)
        for dist in (2, 3, 1):
            peer = flip(me, dist)
            copy = pltpu.make_async_remote_copy(
                src_ref=src_ref.at[which, peer], dst_ref=seq_ref.at[me, rows],
                send_sem=cp_send.at[shift, dist - 1], recv_sem=cp_recv.at[shift, dist - 1],
                device_id={"cp": peer}, device_id_type=MESH)
            second.append(copy)
            copy.start()
        seq_ref[me, rows] = src_ref[which, me]

    forward(0, in_ref, my_tp)
    for shift in (1, 3, 2):
        first[shift].wait_recv()
        forward(shift, block_ref, lax.rem(my_tp + 4 - shift, 4))
    for shift in (1, 2, 3):
        first[shift].wait_send()
    for copy in second:
        copy.wait_send()
    for copy in second:
        copy.wait_recv()


def tokens_to_heads(collective_id, array):
    tp, heads, quarter, head_dim = array.shape
    dma = pltpu.SemaphoreType.DMA
    return pl.pallas_call(
        tokens_to_heads_kernel,
        out_shape=jax.ShapeDtypeStruct((heads, tp * quarter, head_dim), array.dtype),
        in_specs=[VMEM_SPEC],
        out_specs=VMEM_SPEC,
        scratch_shapes=[pltpu.VMEM(array.shape, array.dtype), dma((3,)), dma((3,)), dma((4, 3)), dma((4, 3))],
        compiler_params=pltpu.CompilerParams(collective_id=collective_id, has_side_effects=True, vmem_limit_bytes=VMEM_LIMIT),
        name="tokens_to_heads",
    )(array)


def turn(values):
    half_dim = values.shape[1] // 2
    return jnp.concatenate([values[:, half_dim:], values[:, :half_dim]], axis=1)


def front_kernel(full_width, sub, x_ref, wq_ref, wk_ref, wv_ref, cos_ref, sin_ref, qg_ref, kg_ref, q_out, k_out, v_out,
                 q_buf, k_buf, v_buf, lin_ref, own, slots, total, tp_send, tp_recv, ex_send, ex_recv):
    me, my_tp = lax.axis_index("cp"), lax.axis_index("tp")
    rows = x_ref.shape[0]
    heads, head_dim = qg_ref.shape
    peers_barrier()
    copies = []

    def send(idx, src, dst):
        for dist in (2, 3, 1):
            peer = flip(me, dist)
            copy = pltpu.make_async_remote_copy(
                src_ref=src.at[peer], dst_ref=dst.at[me], send_sem=ex_send.at[idx, dist - 1], recv_sem=ex_recv.at[idx, dist - 1],
                device_id={"cp": peer}, device_id_type=MESH)
            copy.start()
            copies.append(copy)
        dst[me] = src[me]

    def part_of(idx):
        return pl.ds(pl.multiple_of(idx * sub, sub), sub)

    def values(idx, carry):
        part = part_of(idx)
        out = dot_nt(x_ref[part, :], wv_ref[...]).astype(jnp.bfloat16)
        for head in range(heads):
            v_buf[head, part, :] = out[:, head * head_dim:(head + 1) * head_dim]
        return carry

    lax.fori_loop(0, rows // sub, values, 0)
    send(2, v_buf, v_out)

    def linear(idx, carry):
        part = part_of(idx)
        for number, w_ref in enumerate((wq_ref, wk_ref)):
            out = dot_nt(x_ref[part, :], w_ref[...])
            lin_ref[number, part, :] = out
            square = out * out
            square = sum(square[:, head * head_dim:(head + 1) * head_dim] for head in range(heads))
            own[number:number + 1, part] = jnp.sum(square.T, axis=0, keepdims=True)
        return carry

    lax.fori_loop(0, rows // sub, linear, 0)
    moves = []
    for shift in (1, 2, 3):
        move = pltpu.make_async_remote_copy(
            src_ref=own, dst_ref=slots.at[my_tp], send_sem=tp_send.at[shift - 1], recv_sem=tp_recv.at[shift - 1],
            device_id={"tp": lax.rem(my_tp + shift, 4)}, device_id_type=MESH)
        move.start()
        moves.append(move)
    slots[my_tp] = own[...]
    for move in moves:
        move.wait()
    total[...] = lax.rsqrt((slots[0] + slots[1] + slots[2] + slots[3]) / full_width + NORM_EPS)

    for number, (gain_ref, buf, out_ref) in enumerate(((qg_ref, q_buf, q_out), (kg_ref, k_buf, k_out))):
        def rotate(idx, carry, number=number, gain_ref=gain_ref, buf=buf):
            part = part_of(idx)
            inv = jnp.broadcast_to(total[number:number + 1, part], (head_dim, sub)).T
            for head in range(heads):
                scaled = lin_ref[number, part, head * head_dim:(head + 1) * head_dim] * inv * gain_ref[head:head + 1, :]
                buf[head, part, :] = (scaled * cos_ref[part, :] + turn(scaled) * sin_ref[part, :]).astype(jnp.bfloat16)
            return carry

        lax.fori_loop(0, rows // sub, rotate, 0)
        send(number, buf, out_ref)
    for copy in copies:
        copy.wait()


def front(collective_id, full_width, x, weights, cos_tab, sin_tab, q_gain, k_gain):
    rows, _ = x.shape
    heads, head_dim = q_gain.shape
    dma = pltpu.SemaphoreType.DMA
    block = (heads, rows, head_dim)
    stat = pltpu.VMEM((2, rows), jnp.float32)
    return pl.pallas_call(
        functools.partial(front_kernel, full_width, min(256, rows)),
        out_shape=tuple([jax.ShapeDtypeStruct(block, jnp.bfloat16)] * 3),
        in_specs=[VMEM_SPEC] * 8,
        out_specs=tuple([VMEM_SPEC] * 3),
        scratch_shapes=[pltpu.VMEM(block, jnp.bfloat16)] * 3 + [pltpu.VMEM((2, rows, heads * head_dim), jnp.float32),
                        stat, pltpu.VMEM((4, 2, rows), jnp.float32), stat, dma((3,)), dma((3,)), dma((3, 3)), dma((3, 3))],
        compiler_params=pltpu.CompilerParams(collective_id=collective_id, has_side_effects=True, vmem_limit_bytes=VMEM_LIMIT),
        name="front",
    )(x, *weights, cos_tab, sin_tab, q_gain, k_gain)


def causal_mask(scores):
    key_pos = lax.broadcasted_iota(jnp.int32, scores.shape, 0)
    query_pos = lax.broadcasted_iota(jnp.int32, scores.shape, 1)
    return jnp.where(key_pos <= query_pos, scores, MASK_VALUE)


def attend_kernel(block, factor, q_ref, k_ref, v_ref, o_ref, lse_ref):
    blk = pl.program_id(0)
    q_blk = q_ref[...]

    def scores_of(idx):
        rows = pl.ds(pl.multiple_of(idx * block, block), block)
        return dot_nt(k_ref[rows, :], q_blk), v_ref[rows, :]

    scores, v_blk = scores_of(blk)
    scores = causal_mask(scores)
    top = jnp.max(scores, axis=0, keepdims=True)
    probs = jnp.exp2((scores - top) * factor)
    norm = jnp.sum(probs, axis=0, keepdims=True)
    acc = dot_tn(v_blk, probs.astype(jnp.bfloat16))

    def step(idx, state):
        top, norm, acc = state
        scores, v_blk = scores_of(idx)
        new_top = jnp.maximum(top, jnp.max(scores, axis=0, keepdims=True))
        probs = jnp.exp2((scores - new_top) * factor)
        rescale = jnp.exp2((top - new_top) * factor)
        norm = norm * rescale + jnp.sum(probs, axis=0, keepdims=True)
        acc = acc * rescale + dot_tn(v_blk, probs.astype(jnp.bfloat16))
        return new_top, norm, acc

    top, norm, acc = lax.fori_loop(0, blk, step, (top, norm, acc))
    o_ref[...] = (acc / norm).T.astype(jnp.bfloat16)
    lse_ref[...] = top * factor + jnp.log2(norm)


def attend(q, k, v):
    rows, head_dim = q.shape
    block = min(512, rows // 4)
    whole = pl.BlockSpec((rows, head_dim), lambda i: (0, 0))
    part = pl.BlockSpec((block, head_dim), lambda i: (i, 0))
    return pl.pallas_call(
        functools.partial(attend_kernel, block, head_dim ** -0.5 * LOG2E),
        grid=(rows // block,),
        out_shape=(jax.ShapeDtypeStruct(q.shape, jnp.bfloat16), jax.ShapeDtypeStruct((1, rows), jnp.float32)),
        in_specs=[part, whole, whole],
        out_specs=(part, pl.BlockSpec((1, block), lambda i: (0, i))),
        compiler_params=pltpu.CompilerParams(vmem_limit_bytes=VMEM_LIMIT),
        cost_estimate=pl.CostEstimate(flops=2 * rows * rows * head_dim, bytes_accessed=8 * rows * head_dim, transcendentals=rows * rows // 2),
        name="attend",
    )(q, k, v)


def attend_back_kernel(block, scale, q_ref, k_ref, v_ref, o_ref, do_ref, lse_ref, dq_ref, dk_ref, dv_ref, delta_ref, dk_acc, dv_acc):
    blk = pl.program_id(0)
    n_blk = pl.num_programs(0)
    factor = scale * LOG2E

    @pl.when(blk == 0)
    def _():
        def prepare(idx, carry):
            rows = pl.ds(pl.multiple_of(idx * block, block), block)
            prod = do_ref[rows, :].astype(jnp.float32) * o_ref[rows, :].astype(jnp.float32)
            delta_ref[:, rows] = jnp.sum(prod.T, axis=0, keepdims=True)
            dq_ref[rows, :] = jnp.zeros((block, dq_ref.shape[1]), jnp.float32)
            return carry

        lax.fori_loop(0, n_blk, prepare, 0)

    k_blk = k_ref[...]
    v_blk = v_ref[...]

    def one(idx, masked):
        rows = pl.ds(pl.multiple_of(idx * block, block), block)
        q_blk = q_ref[rows, :]
        do_blk = do_ref[rows, :]
        scores = dot_nt(k_blk, q_blk)
        if masked:
            scores = causal_mask(scores)
        probs = jnp.exp2(scores * factor - lse_ref[:, rows])
        grad_v = dot_nn(probs.astype(jnp.bfloat16), do_blk)
        grad_p = dot_nt(v_blk, do_blk)
        grad_s = (probs * ((grad_p - delta_ref[:, rows]) * scale)).astype(jnp.bfloat16)
        dq_ref[rows, :] += dot_tn(grad_s, k_blk)
        return dot_nn(grad_s, q_blk), grad_v

    dk_acc[...], dv_acc[...] = one(blk, True)

    def step(idx, carry):
        grad_k, grad_v = one(idx, False)
        dk_acc[...] += grad_k
        dv_acc[...] += grad_v
        return carry

    lax.fori_loop(blk + 1, n_blk, step, 0)
    dk_ref[...] = dk_acc[...]
    dv_ref[...] = dv_acc[...].astype(jnp.bfloat16)


def attend_back(q, k, v, o, do, lse):
    rows, head_dim = q.shape
    block = min(512, rows // 4)
    whole = pl.BlockSpec((rows, head_dim), lambda i: (0, 0))
    part = pl.BlockSpec((block, head_dim), lambda i: (i, 0))
    stat = pl.BlockSpec((1, rows), lambda i: (0, 0))
    return pl.pallas_call(
        functools.partial(attend_back_kernel, block, head_dim ** -0.5),
        grid=(rows // block,),
        out_shape=(jax.ShapeDtypeStruct(q.shape, jnp.float32), jax.ShapeDtypeStruct(q.shape, jnp.float32), jax.ShapeDtypeStruct(q.shape, jnp.bfloat16)),
        in_specs=[whole, part, part, whole, whole, stat],
        out_specs=(whole, part, part),
        scratch_shapes=[pltpu.VMEM((1, rows), jnp.float32), pltpu.VMEM((block, head_dim), jnp.float32), pltpu.VMEM((block, head_dim), jnp.float32)],
        compiler_params=pltpu.CompilerParams(vmem_limit_bytes=VMEM_LIMIT),
        cost_estimate=pl.CostEstimate(flops=5 * rows * rows * head_dim, bytes_accessed=20 * rows * head_dim, transcendentals=rows * rows // 2),
        name="attend_back",
    )(q, k, v, o, do, lse)


def post_kernel(o_ref, mine_ref, other_ref, x_any, gy_any, pw_ref, both_ref, do_ref, gpost_ref, x_ref, gy_ref, sems):
    tp_size, heads, _, head_dim = o_ref.shape
    block = x_ref.shape[0]
    first_row = (lax.axis_index("tp") * pl.num_programs(0) + pl.program_id(0)) * block
    loads = []
    for idx, (src, dst) in enumerate(((x_any, x_ref), (gy_any, gy_ref))):
        load = pltpu.make_async_copy(src.at[pl.ds(pl.multiple_of(first_row, block), block)], dst, sems.at[idx])
        load.start()
        loads.append(load)
    core = lax.rem(lax.axis_index("cp"), 2)
    halves = ((mine_ref, core * (heads // 2)), (other_ref, (1 - core) * (heads // 2)))
    proj = None
    for idx in range(tp_size):
        for w_ref, start in halves:
            term = dot_nn(jnp.concatenate([o_ref[idx, start + head] for head in range(heads // 2)], axis=1), w_ref[idx])
            proj = term if proj is None else proj + term
    for load in loads:
        load.wait()
    gain = pw_ref[...]
    inv = lax.rsqrt(jnp.mean(proj * proj, axis=-1, keepdims=True) + NORM_EPS)
    hat = proj * inv
    d_model = x_ref.shape[1]
    both_ref[:, d_model:] = (x_ref[...].astype(jnp.float32) + hat * gain).astype(jnp.bfloat16)
    grad = gy_ref[...].astype(jnp.float32)
    gpost = jnp.sum(grad * hat, axis=0, keepdims=True)
    grad_hat = grad * gain
    grad_proj = (inv * (grad_hat - hat * jnp.mean(grad_hat * hat, axis=-1, keepdims=True))).astype(jnp.bfloat16)
    both_ref[:, :d_model] = grad_proj
    for idx in range(tp_size):
        for w_ref, start in halves:
            grad_o = dot_nt(grad_proj, w_ref[idx]).astype(jnp.bfloat16)
            for head in range(heads // 2):
                do_ref[idx, start + head] = grad_o[:, head * head_dim:(head + 1) * head_dim]

    @pl.when(pl.program_id(0) == 0)
    def _():
        gpost_ref[...] = jnp.zeros_like(gpost_ref)

    gpost_ref[...] += gpost


def post(o_all, wo_mine, wo_other, x, gy, gain):
    tp_size, heads, rows, head_dim = o_all.shape
    d_model = x.shape[1]
    block = min(128, rows)
    any_spec = pl.BlockSpec(memory_space=pl.ANY)
    piece = pltpu.VMEM((block, d_model), jnp.bfloat16)
    both = pl.BlockSpec((block, 2 * d_model), lambda i: (i, 0))
    by_head = pl.BlockSpec((tp_size, heads, block, head_dim), lambda i: (0, 0, i, 0))
    return pl.pallas_call(
        post_kernel,
        grid=(rows // block,),
        out_shape=(jax.ShapeDtypeStruct((rows, 2 * d_model), jnp.bfloat16), jax.ShapeDtypeStruct(o_all.shape, jnp.bfloat16), jax.ShapeDtypeStruct((1, d_model), jnp.float32)),
        in_specs=[by_head] + [pl.BlockSpec(wo_mine.shape, lambda i: (0, 0, 0))] * 2 + [any_spec, any_spec, pl.BlockSpec((1, d_model), lambda i: (0, 0))],
        out_specs=(both, by_head, pl.BlockSpec((1, d_model), lambda i: (0, 0))),
        scratch_shapes=[piece, piece, pltpu.SemaphoreType.DMA((2,))],
        compiler_params=pltpu.CompilerParams(vmem_limit_bytes=VMEM_LIMIT),
        cost_estimate=pl.CostEstimate(flops=4 * rows * d_model * d_model, bytes_accessed=4 * d_model * d_model, transcendentals=rows),
        name="post",
    )(o_all, wo_mine, wo_other, x, gy, gain)


def output_weights_kernel(o_ref, gp_ref, out_ref):
    heads, _, head_dim = o_ref.shape
    acc = dot_tn(jnp.concatenate([o_ref[head] for head in range(heads)], axis=1), gp_ref[...])
    for head in range(heads):
        out_ref[head] = acc[head * head_dim:(head + 1) * head_dim, :]


def output_weights(o_heads, both):
    heads, rows, head_dim = o_heads.shape
    d_model = both.shape[1] // 2
    block = min(512, d_model)
    return pl.pallas_call(
        output_weights_kernel,
        grid=(d_model // block,),
        out_shape=jax.ShapeDtypeStruct((heads, head_dim, d_model), jnp.float32),
        in_specs=[pl.BlockSpec(o_heads.shape, lambda i: (0, 0, 0)), pl.BlockSpec((rows, block), lambda i: (0, i))],
        out_specs=pl.BlockSpec((heads, head_dim, block), lambda i: (0, 0, i)),
        compiler_params=pltpu.CompilerParams(vmem_limit_bytes=VMEM_LIMIT),
        cost_estimate=pl.CostEstimate(flops=2 * rows * d_model * heads * head_dim, bytes_accessed=12 * rows * d_model, transcendentals=0),
        name="output_weights",
    )(o_heads, both)


def spread_kernel(in_ref, *out_refs):
    for number, out_ref in enumerate(out_refs):
        for head in range(in_ref.shape[0]):
            out_ref[:, head, :] = in_ref[head, number]


def spread(gathered):
    heads, count, d_model, head_dim = gathered.shape
    block = min(256, d_model)
    return pl.pallas_call(
        spread_kernel,
        grid=(d_model // block,),
        out_shape=tuple([jax.ShapeDtypeStruct((d_model, heads, head_dim), gathered.dtype)] * count),
        in_specs=[pl.BlockSpec((heads, count, block, head_dim), lambda i: (0, 0, i, 0))],
        out_specs=tuple([pl.BlockSpec((block, heads, head_dim), lambda i: (i, 0, 0))] * count),
        compiler_params=pltpu.CompilerParams(vmem_limit_bytes=VMEM_LIMIT),
        cost_estimate=pl.CostEstimate(flops=d_model * heads * head_dim * count, bytes_accessed=8 * d_model * heads * head_dim * count, transcendentals=0),
        name="spread",
    )(gathered)


def chain_kernel(size, n_chunk, lag, tile, dq_ref, dk_ref, dv_ref, wq_ref, wk_ref, wv_ref, gy_ref, out_ref, part_ref, sums_a, sums_b, rs_send, rs_recv, ag_send, ag_recv):
    me = lax.axis_index("tp")
    entry_barrier("tp", size)
    half = part_ref.shape[0] // 2
    rows = half // n_chunk
    last = size - 1

    def parts(side, chunk):
        local = pl.ds(pl.multiple_of(chunk * rows, rows), rows)
        glob = pl.ds(pl.multiple_of(side * half + chunk * rows, rows), rows)
        sums = (sums_a, sums_b)[side]
        return local, glob, sums

    def toward(side):
        return jnp.maximum(me - 1, 0) if side == 0 else jnp.minimum(me + 1, last)

    def away(side):
        return jnp.minimum(me + 1, last) if side == 0 else jnp.maximum(me - 1, 0)

    def rs_copy(side, chunk, first):
        local, glob, sums = parts(side, chunk)
        return pltpu.make_async_remote_copy(
            src_ref=part_ref.at[glob] if first else sums.at[local], dst_ref=sums.at[local],
            send_sem=rs_send.at[side, chunk], recv_sem=rs_recv.at[side, chunk],
            device_id={"tp": toward(side)}, device_id_type=MESH)

    def ag_copy(side, chunk):
        _, glob, _ = parts(side, chunk)
        return pltpu.make_async_remote_copy(
            src_ref=out_ref.at[glob], dst_ref=out_ref.at[glob],
            send_sem=ag_send.at[side, chunk], recv_sem=ag_recv.at[side, chunk],
            device_id={"tp": away(side)}, device_id_type=MESH)

    def place(side):
        return me if side == 0 else last - me

    heads = dq_ref.shape[0]
    d_model = out_ref.shape[1]
    block = min(512, d_model)
    n_tile = 2 * half // tile
    per_tile = tile // rows

    def push(number):
        for side in (0, 1):
            @pl.when((lax.rem(number, 2) == side) & (place(side) == last))
            def _(side=side):
                def one(idx, carry):
                    rs_copy(side, (number // 2) * per_tile + idx, True).start()
                    return carry

                lax.fori_loop(0, per_tile, one, 0)

    def product(number, carry):
        tile_rows = pl.ds(pl.multiple_of(lax.rem(number, 2) * half + (number // 2) * tile, tile), tile)

        def columns(idx, carry):
            cols = pl.ds(pl.multiple_of(idx * block, block), block)
            total = None
            for grad_ref, w_ref in ((dq_ref, wq_ref), (dk_ref, wk_ref), (dv_ref, wv_ref)):
                grad = jnp.concatenate([grad_ref[idx_h, tile_rows, :] for idx_h in range(heads)], axis=1)
                term = dot_nn(grad, w_ref[:, cols])
                total = term if total is None else total + term
            part_ref[tile_rows, cols] = total
            return carry

        lax.fori_loop(0, d_model // block, columns, 0)

        @pl.when(number > 0)
        def _():
            push(number - 1)

        return carry

    lax.fori_loop(0, n_tile, product, 0)
    push(jnp.int32(n_tile - 1))

    def pass_on(side, chunk):
        local, glob, sums = parts(side, chunk)
        rs_copy(side, chunk, False).wait_recv()
        sums[local] = sums[local] + part_ref[glob]
        rs_copy(side, chunk, False).start()

    def finish(side, chunk):
        local, glob, sums = parts(side, chunk)
        rs_copy(side, chunk, False).wait_recv()
        out_ref[glob] = (gy_ref[glob].astype(jnp.float32) + (sums[local] + part_ref[glob])).astype(jnp.bfloat16)
        ag_copy(side, chunk).start()

    def reduce_step(idx, carry):
        for far in range(last - 1, 0, -1):
            chunk = idx - (last - 1 - far) * lag
            for side in (0, 1):
                @pl.when((chunk >= 0) & (chunk < n_chunk) & (place(side) == far))
                def _(side=side, chunk=chunk):
                    pass_on(side, chunk)
        for side in (0, 1):
            @pl.when((idx < n_chunk) & (place(side) == 0))
            def _(side=side):
                finish(side, idx)
        return carry

    lax.fori_loop(0, n_chunk + (last - 2) * lag, reduce_step, 0)

    def return_step(idx, carry):
        for far in range(1, last + 1):
            chunk = idx - (far - 1) * lag
            for side in (0, 1):
                @pl.when((chunk >= 0) & (chunk < n_chunk) & (place(side) == far))
                def _(side=side, chunk=chunk, far=far):
                    ag_copy(side, chunk).wait_recv()
                    if far < last:
                        ag_copy(side, chunk).start()
        return carry

    lax.fori_loop(0, n_chunk + (last - 1) * lag, return_step, 0)

    def drain(idx, carry):
        for side in (0, 1):
            @pl.when(place(side) > 0)
            def _(side=side):
                rs_copy(side, idx, False).wait_send()

            @pl.when(place(side) < last)
            def _(side=side):
                ag_copy(side, idx).wait_send()
        return carry

    lax.fori_loop(0, n_chunk, drain, 0)


def chain_sum(size, collective_id, grads, weights, gy):
    rows, d_model = gy.shape
    n_chunk = 32 if rows >= 512 else 4
    sems = [pltpu.SemaphoreType.DMA((2, n_chunk))] * 4
    return pl.pallas_call(
        functools.partial(chain_kernel, size, n_chunk, 2, min(256, rows // 4)),
        out_shape=jax.ShapeDtypeStruct((rows, d_model), jnp.bfloat16),
        in_specs=[VMEM_SPEC] * 7,
        out_specs=VMEM_SPEC,
        scratch_shapes=[pltpu.VMEM((rows, d_model), jnp.float32), pltpu.VMEM((rows // 2, d_model), jnp.float32), pltpu.VMEM((rows // 2, d_model), jnp.float32)] + sems,
        compiler_params=pltpu.CompilerParams(collective_id=collective_id, has_side_effects=True, vmem_limit_bytes=VMEM_LIMIT),
        cost_estimate=pl.CostEstimate(flops=10 ** 11, bytes_accessed=16 * rows * d_model, transcendentals=0),
        name="chain_sum",
    )(*grads, *weights, gy)


def weights_back_kernel(full_width, sub, x_ref, far0_ref, far1_ref, far2_ref, wq_ref, wk_ref, dq_ref, dk_ref, dv_ref, cos_ref, sin_ref, qg_ref, kg_ref, post_ref,
                        dw_ref, exq_ref, exk_ref, exv_ref, gains_ref, post_out,
                        x_buf, wqk_ref, lin_ref, q16_ref, k16_ref, own, slots_tp, mid, slots_cp, done, total, gq_ref, gk_ref, my_gains,
                        x_sem, w_sem, pair_send, pair_recv, tp_send, tp_recv, cp_send, cp_recv, back_send, back_recv, ex_send, ex_recv):
    me = lax.axis_index("cp")
    my_tp = lax.axis_index("tp")
    rows, head_dim = dq_ref.shape[1:]
    loads = []
    step = far0_ref.shape[0]
    fars = ((far0_ref, pl.ds(0, step)), (far1_ref, pl.ds(step, step)), (far2_ref, pl.ds(2 * step, rows - 2 * step)))
    pieces = ((x_ref, 0, pl.ds(0, rows)),) + tuple((ref, 2, part) for ref, part in fars)
    for idx, (src, dist, part) in enumerate(pieces):
        load = pltpu.make_async_copy(src, x_buf.at[dist, part], x_sem.at[idx])
        load.start()
        loads.append(load)
    own_rows = pl.ds(pl.multiple_of(me * head_dim, head_dim), head_dim)
    w_loads = [pltpu.make_async_copy(src.at[own_rows], wqk_ref.at[pl.ds(idx * head_dim, head_dim)], w_sem.at[idx]) for idx, src in enumerate((wq_ref, wk_ref))]
    for load in w_loads:
        load.start()
    peers_barrier()
    for idx, (src, dist, part) in enumerate(pieces):
        load = pltpu.make_async_remote_copy(
            src_ref=src, dst_ref=x_buf.at[dist + 1, part], send_sem=pair_send.at[idx], recv_sem=pair_recv.at[idx],
            device_id={"cp": flip(me, 1)}, device_id_type=MESH)
        load.start()
        loads.append(load)
    own[4:5, :] = jnp.zeros_like(own[4:5, :])
    own[4:5, 0:post_ref.shape[1]] = post_ref[...]

    def ex_copy(idx, src, dst, dist):
        peer = flip(me, dist)
        return pltpu.make_async_remote_copy(
            src_ref=src.at[peer], dst_ref=dst.at[me], send_sem=ex_send.at[idx, dist - 1], recv_sem=ex_recv.at[idx, dist - 1],
            device_id={"cp": peer}, device_id_type=MESH)

    copies = [ex_copy(2, dv_ref, exv_ref, dist) for dist in (2, 3, 1)]
    for copy in copies:
        copy.start()

    def grad_of(ref, blk, part, table):
        g = ref[blk, part, :]
        return g * cos_ref[table, :] - turn(g) * sin_ref[table, :]

    w_loads[0].wait()
    w_loads[1].wait()
    sides = ((dq_ref, qg_ref, 0), (dk_ref, kg_ref, 1))
    for order, dist in enumerate((0, 2, 1, 3)):
        blk = flip(me, dist)
        for load in (loads[0:1], loads[1:4], loads[4:5], loads[5:8])[order]:
            if order < 2:
                load.wait()
            else:
                load.wait_recv()

        def first(idx, carry, dist=dist, blk=blk):
            part = pl.ds(pl.multiple_of(idx * sub, sub), sub)
            table = pl.ds(pl.multiple_of(blk * rows + idx * sub, sub), sub)
            lin = dot_nt(x_buf[dist, part, :], wqk_ref[...])
            lin_ref[dist, part, :] = lin
            for ref, gain_ref, number in sides:
                mine = lin[:, number * head_dim:(number + 1) * head_dim]
                grad = grad_of(ref, blk, part, table) * gain_ref[...]
                own[2 * number:2 * number + 1, table] = jnp.sum((mine * mine).T, axis=0, keepdims=True)
                own[2 * number + 1:2 * number + 2, table] = jnp.sum((grad * mine).T, axis=0, keepdims=True)
            return carry

        lax.fori_loop(0, rows // sub, first, 0)

    quarter = own.shape[1] // 4

    def quarter_of(which):
        return pl.ds(pl.multiple_of(which * quarter, quarter), quarter)

    moves = []
    for shift in (2, 1, 3):
        peer = lax.rem(my_tp + shift, 4)
        move = pltpu.make_async_remote_copy(
            src_ref=own.at[:, quarter_of(peer)], dst_ref=slots_tp.at[my_tp], send_sem=tp_send.at[shift - 1], recv_sem=tp_recv.at[shift - 1],
            device_id={"tp": peer}, device_id_type=MESH)
        move.start()
        moves.append(move)
    slots_tp[my_tp] = own[:, quarter_of(my_tp)]
    for move in moves:
        move.wait()
    mid[...] = slots_tp[0] + slots_tp[1] + slots_tp[2] + slots_tp[3]
    moves = []
    for dist in (2, 3, 1):
        move = pltpu.make_async_remote_copy(
            src_ref=mid, dst_ref=slots_cp.at[me], send_sem=cp_send.at[dist - 1], recv_sem=cp_recv.at[dist - 1],
            device_id={"cp": flip(me, dist)}, device_id_type=MESH)
        move.start()
        moves.append(move)
    slots_cp[me] = mid[...]
    for move in moves:
        move.wait()
    done[...] = slots_cp[0] + slots_cp[1] + slots_cp[2] + slots_cp[3]
    moves = []
    for shift in (2, 1, 3):
        move = pltpu.make_async_remote_copy(
            src_ref=done, dst_ref=total.at[:, quarter_of(my_tp)], send_sem=back_send.at[shift - 1], recv_sem=back_recv.at[shift - 1],
            device_id={"tp": lax.rem(my_tp + shift, 4)}, device_id_type=MESH)
        move.start()
        moves.append(move)
    total[:, quarter_of(my_tp)] = done[...]
    for move in moves:
        move.wait()

    post_out[...] = total[4:5, 0:post_ref.shape[1]]
    gq_ref[...] = jnp.zeros_like(gq_ref)
    gk_ref[...] = jnp.zeros_like(gk_ref)
    outs = ((q16_ref, exq_ref, gq_ref), (k16_ref, exk_ref, gk_ref))
    for dist in (2, 3, 1, 0):
        blk = flip(me, dist)

        def second(idx, carry, dist=dist, blk=blk):
            part = pl.ds(pl.multiple_of(idx * sub, sub), sub)
            table = pl.ds(pl.multiple_of(blk * rows + idx * sub, sub), sub)
            lin = lin_ref[dist, part, :]
            for (ref, gain_ref, number), (d16_ref, _, gain_out) in zip(sides, outs):
                mine = lin[:, number * head_dim:(number + 1) * head_dim]
                inv = lax.rsqrt(total[2 * number:2 * number + 1, table] / full_width + NORM_EPS)
                dot = inv * total[2 * number + 1:2 * number + 2, table] / full_width
                inv = jnp.broadcast_to(inv, (head_dim, sub)).T
                dot = jnp.broadcast_to(dot, (head_dim, sub)).T
                raw = grad_of(ref, blk, part, table)
                hat = mine * inv
                d16_ref[blk, part, :] = (inv * (raw * gain_ref[...] - hat * dot)).astype(jnp.bfloat16)
                gain_out[...] += jnp.sum(raw * hat, axis=0, keepdims=True)
            return carry

        lax.fori_loop(0, rows // sub, second, 0)
        if dist:
            for idx, (d16_ref, ex_ref, _) in enumerate(outs):
                copy = ex_copy(idx, d16_ref, ex_ref, dist)
                copy.start()
                copies.append(copy)
    my_gains[0:1, :] = gq_ref[...]
    my_gains[1:2, :] = gk_ref[...]
    for src, dst in ((q16_ref, exq_ref), (k16_ref, exk_ref), (dv_ref, exv_ref)):
        dst[me] = src[me]
    gains_ref[me] = my_gains[...]
    for dist in (1, 2, 3):
        copy = pltpu.make_async_remote_copy(
            src_ref=my_gains, dst_ref=gains_ref.at[me], send_sem=ex_send.at[3, dist - 1], recv_sem=ex_recv.at[3, dist - 1],
            device_id={"cp": flip(me, dist)}, device_id_type=MESH)
        copy.start()
        copies.append(copy)

    block = min(512, x_buf.shape[2])

    def weight_step(idx, carry):
        cols = pl.ds(pl.multiple_of(idx * block, block), block)
        acc = None
        for dist in range(4):
            blk = flip(me, dist)
            grads = jnp.concatenate([q16_ref[blk], k16_ref[blk], dv_ref[blk]], axis=1)
            term = dot_tn(grads, x_buf[dist, :, cols])
            acc = term if acc is None else acc + term
        acc = acc.T
        for number in range(3):
            dw_ref[number, cols, :] = acc[:, number * head_dim:(number + 1) * head_dim]
        return carry

    lax.fori_loop(0, x_buf.shape[2] // block, weight_step, 0)
    for copy in copies:
        copy.wait()
    for load in loads[4:]:
        load.wait_send()


def weights_back(collective_id, full_width, x, x_far, wq, wk, dq, dk, dv, cos_tab, sin_tab, q_gain, k_gain, grad_post):
    _, rows, head_dim = dq.shape
    d_model = x.shape[1]
    any_spec = pl.BlockSpec(memory_space=pl.ANY)
    dma = pltpu.SemaphoreType.DMA
    span = max(4 * rows, d_model)
    stat = pltpu.VMEM((5, span), jnp.float32)
    slots = pltpu.VMEM((4, 5, span // 4), jnp.float32)
    small = pltpu.VMEM((5, span // 4), jnp.float32)
    ex = jax.ShapeDtypeStruct(dq.shape, jnp.bfloat16)
    return pl.pallas_call(
        functools.partial(weights_back_kernel, full_width, min(512, rows)),
        out_shape=(jax.ShapeDtypeStruct((3, d_model, head_dim), jnp.float32), ex, ex, ex,
                   jax.ShapeDtypeStruct((4, 2, head_dim), jnp.float32), jax.ShapeDtypeStruct((1, d_model), jnp.float32)),
        in_specs=[any_spec] * 6 + [VMEM_SPEC] * 8,
        out_specs=tuple([VMEM_SPEC] * 6),
        scratch_shapes=[pltpu.VMEM((4, rows, d_model), jnp.bfloat16), pltpu.VMEM((2 * head_dim, d_model), jnp.bfloat16), pltpu.VMEM((4, rows, 2 * head_dim), jnp.float32),
                        pltpu.VMEM(dq.shape, jnp.bfloat16), pltpu.VMEM(dq.shape, jnp.bfloat16),
                        stat, slots, small, slots, small, stat,
                        pltpu.VMEM((1, head_dim), jnp.float32), pltpu.VMEM((1, head_dim), jnp.float32), pltpu.VMEM((2, head_dim), jnp.float32),
                        dma((4,)), dma((2,)), dma((4,)), dma((4,)), dma((3,)), dma((3,)), dma((3,)), dma((3,)), dma((3,)), dma((3,)), dma((4, 3)), dma((4, 3))],
        compiler_params=pltpu.CompilerParams(collective_id=collective_id, has_side_effects=True, vmem_limit_bytes=VMEM_LIMIT),
        name="weights_back",
    )(x, *x_far, wq, wk, dq, dk, dv, cos_tab, sin_tab, q_gain, k_gain, grad_post)


def solution(mesh):
    tp_size = mesh.shape["tp"]
    cp_size = mesh.shape["cp"]
    act_spec = P("dp", "cp", None)
    col_spec = P(None, "tp", None)
    part_col = P("dp", "tp", None)
    in_specs = (act_spec, col_spec, col_spec, col_spec, P("tp", None, None), P("tp", None), P("tp", None), P(None), act_spec)
    out_specs = (act_spec, act_spec, part_col, part_col, part_col, P(("dp", "tp"), None, None), P(("dp", "tp"), None), P(("dp", "tp"), None), P("dp"))
    swap_core = [(dev, dev ^ 1) for dev in range(cp_size)]

    def local_run(x_in, w_q, w_k, w_v, w_o, q_norm_w, k_norm_w, post_norm_w, grad_y):
        rows, d_model = x_in.shape[1:]
        heads, head_dim = w_q.shape[1:]
        width = heads * head_dim
        full_width = width * tp_size
        x = x_in[0]
        gy = grad_y[0]
        cp_index = lax.axis_index("cp")

        def wide_tables(cos_tab, sin_tab):
            return jnp.concatenate([cos_tab, cos_tab], axis=1), jnp.concatenate([-sin_tab, sin_tab], axis=1)

        cos_tab, sin_tab = wide_tables(*rope_tables((cp_index * rows + jnp.arange(rows)).astype(jnp.float32), head_dim))
        turned = tuple(w.reshape(d_model, width).T for w in (w_q, w_k, w_v))

        core = cp_index % 2
        own_half = lax.dynamic_slice_in_dim(w_o, core * (heads // 2), heads // 2, axis=0)
        wo_mine = lax.all_gather(own_half, "tp").reshape(tp_size, width // 2, d_model)
        q_seq, k_seq, v_seq = front(1, full_width, x, turned, cos_tab, sin_tab, q_norm_w, k_norm_w)
        seq_shape = (cp_size * rows, head_dim)
        block_shape = (cp_size, rows, head_dim)
        piece = rows // 4

        def fetch(start, size):
            return lax.ppermute(x_free[start:start + size], "cp", [(dev, dev ^ 2) for dev in range(cp_size)])

        q_seq, x_free = lax.optimization_barrier((q_seq, x))
        far0 = fetch(0, piece)
        q_seq, k_seq, v_seq = (t.reshape(seq_shape) for t in (q_seq, k_seq, v_seq))
        o_seq, lse = attend(q_seq, k_seq, v_seq)
        o_seq, wo_mine = lax.optimization_barrier((o_seq, wo_mine))
        wo_other = lax.ppermute(wo_mine, "cp", swap_core)
        o_heads, o_tokens = heads_to_tokens(2, o_seq.reshape(block_shape))
        o_tokens, x_free = lax.optimization_barrier((o_tokens, x))
        far1 = fetch(piece, piece)
        both, do_tokens, grad_post = post(o_tokens, wo_mine, wo_other, x, gy, post_norm_w[None, :])
        do_seq = tokens_to_heads(3, do_tokens)
        both, do_seq, x_free = lax.optimization_barrier((both, do_seq, x))
        both = lax.all_gather(both, "tp", tiled=True)
        far2 = fetch(2 * piece, rows - 2 * piece)

        coarse_cos, coarse_sin = rope_tables(jnp.arange(0, cp_size * rows, 64, dtype=jnp.float32), head_dim)
        fine_cos, fine_sin = (jnp.concatenate([t, t], axis=1)[None] for t in rope_tables(jnp.arange(64, dtype=jnp.float32), head_dim))
        wide_cos, wide_sin, sign_cos, sign_sin = lax.optimization_barrier(tuple(
            jnp.concatenate([sign * t, t], axis=1)[:, None, :] for sign in (1.0, -1.0) for t in (coarse_cos, coarse_sin)))
        fine_cos, fine_sin = lax.optimization_barrier((fine_cos, fine_sin))
        seq_cos = (wide_cos * fine_cos - wide_sin * fine_sin).reshape(cp_size * rows, head_dim)
        seq_sin = (sign_sin * fine_cos + sign_cos * fine_sin).reshape(cp_size * rows, head_dim)
        gains_head = tuple(lax.dynamic_slice_in_dim(w, cp_index, 1, axis=0) for w in (q_norm_w, k_norm_w))
        dq_seq, dk_seq, dv_seq = attend_back(q_seq, k_seq, v_seq, o_seq, do_seq.reshape(seq_shape), lse)
        dw, dq16, dk16, dv16, gains, grad_post = weights_back(
            4, full_width, x, (far0, far1, far2), turned[0], turned[1],
            dq_seq.reshape(block_shape), dk_seq.reshape(block_shape), dv_seq.reshape(block_shape), seq_cos, seq_sin, *gains_head, grad_post)
        o_heads, dw = lax.optimization_barrier((o_heads, dw))
        grad_w_o = lax.psum(output_weights(o_heads, both), "cp")
        y_out = both[:, d_model:]
        dw = spread(lax.all_gather(dw, "cp"))
        grad_x = chain_sum(tp_size, 6, (dq16, dk16, dv16), turned, gy)
        return (y_out[None], grad_x[None]) + tuple(dw) + (grad_w_o, gains[:, 0], gains[:, 1], grad_post[0])

    return jax.shard_map(local_run, mesh=mesh, in_specs=in_specs, out_specs=out_specs, check_vma=False)
```

```python
import functools

import jax
import jax.numpy as jnp
from jax import lax
from jax.experimental import pallas as pl
from jax.experimental.pallas import tpu as pltpu
from jax.sharding import PartitionSpec as P


ROPE_THETA = 500000.0
NORM_EPS = 1e-6
MASK_VALUE = -1e30
LOG2E = 1.4426950408889634
MESH = pl.DeviceIdType.MESH
VMEM_SPEC = pl.BlockSpec(memory_space=pltpu.VMEM)
VMEM_LIMIT = 60 * 1024 * 1024
NT = (((1,), (1,)), ((), ()))
TN = (((0,), (0,)), ((), ()))


def dot_nt(a, b):
    return lax.dot_general(a, b, NT, preferred_element_type=jnp.float32)


def dot_tn(a, b):
    return lax.dot_general(a, b, TN, preferred_element_type=jnp.float32)


def dot_nn(a, b):
    return jnp.dot(a, b, preferred_element_type=jnp.float32)


def rope_tables(positions, head_dim):
    half_dim = head_dim // 2
    inv_freq = ROPE_THETA ** (-2.0 * jnp.arange(half_dim, dtype=jnp.float32) / head_dim)
    angles = positions[:, None] * inv_freq[None, :]
    return jnp.cos(angles), jnp.sin(angles)


def entry_barrier(axis, size):
    me = lax.axis_index(axis)
    barrier = pltpu.get_barrier_semaphore()
    for shift in range(1, size):
        pl.semaphore_signal(barrier, inc=1, device_id={axis: lax.rem(me + shift, size)}, device_id_type=MESH)
    pl.semaphore_wait(barrier, size - 1)


def peers_barrier():
    me, my_tp = lax.axis_index("cp"), lax.axis_index("tp")
    barrier = pltpu.get_barrier_semaphore()
    for shift in (1, 2, 3):
        pl.semaphore_signal(barrier, inc=1, device_id={"cp": lax.rem(me + shift, 4)}, device_id_type=MESH)
        pl.semaphore_signal(barrier, inc=1, device_id={"tp": lax.rem(my_tp + shift, 4)}, device_id_type=MESH)
    pl.semaphore_wait(barrier, 6)


def flip(index, distance):
    if distance == 1:
        return index + 1 - 2 * lax.rem(index, 2)
    if distance == 2:
        return lax.rem(index + 2, 4)
    return 3 - index if distance == 3 else index


def heads_to_tokens_kernel(in_ref, heads_ref, tokens_ref, cp_send, cp_recv, tp_send, tp_recv):
    me, my_tp = lax.axis_index("cp"), lax.axis_index("tp")
    quarter = in_ref.shape[1] // 4
    peers_barrier()
    first = {}
    for dist in (1, 2, 3):
        peer = flip(me, dist)
        first[dist] = pltpu.make_async_remote_copy(
            src_ref=in_ref.at[peer], dst_ref=heads_ref.at[me], send_sem=cp_send.at[dist - 1], recv_sem=cp_recv.at[dist - 1],
            device_id={"cp": peer}, device_id_type=MESH)
        first[dist].start()

    def rows_of(which):
        return pl.ds(pl.multiple_of(which * quarter, quarter), quarter)

    second = []

    def forward(dist, src_ref, head):
        for shift in (2, 1, 3):
            peer = lax.rem(my_tp + shift, 4)
            copy = pltpu.make_async_remote_copy(
                src_ref=src_ref.at[head, rows_of(peer)], dst_ref=tokens_ref.at[my_tp, head],
                send_sem=tp_send.at[dist, shift - 1], recv_sem=tp_recv.at[dist, shift - 1],
                device_id={"tp": peer}, device_id_type=MESH)
            copy.start()
            second.append(copy)
        tokens_ref[my_tp, head] = src_ref[head, rows_of(my_tp)]

    forward(0, in_ref, me)
    heads_ref[me] = in_ref[me]
    for dist in (1, 2, 3):
        first[dist].wait_recv()
        forward(dist, heads_ref, flip(me, dist))
    for dist in (1, 2, 3):
        first[dist].wait_send()
    for copy in second:
        copy.wait()


def heads_to_tokens(collective_id, array):
    _, rows, head_dim = array.shape
    dma = pltpu.SemaphoreType.DMA
    return pl.pallas_call(
        heads_to_tokens_kernel,
        out_shape=(jax.ShapeDtypeStruct(array.shape, array.dtype), jax.ShapeDtypeStruct((4, 4, rows // 4, head_dim), array.dtype)),
        in_specs=[VMEM_SPEC],
        out_specs=(VMEM_SPEC, VMEM_SPEC),
        scratch_shapes=[dma((3,)), dma((3,)), dma((4, 3)), dma((4, 3))],
        compiler_params=pltpu.CompilerParams(collective_id=collective_id, has_side_effects=True, vmem_limit_bytes=VMEM_LIMIT),
        name="heads_to_tokens",
    )(array)


def tokens_to_heads_kernel(in_ref, seq_ref, block_ref, tp_send, tp_recv, cp_send, cp_recv):
    me, my_tp = lax.axis_index("cp"), lax.axis_index("tp")
    quarter = in_ref.shape[2]
    peers_barrier()
    first = {}
    for shift in (2, 1, 3):
        peer = lax.rem(my_tp + shift, 4)
        first[shift] = pltpu.make_async_remote_copy(
            src_ref=in_ref.at[peer], dst_ref=block_ref.at[my_tp], send_sem=tp_send.at[shift - 1], recv_sem=tp_recv.at[shift - 1],
            device_id={"tp": peer}, device_id_type=MESH)
        first[shift].start()
    second = []

    def forward(shift, src_ref, which):
        rows = pl.ds(pl.multiple_of(which * quarter, quarter), quarter)
        for dist in (2, 3, 1):
            peer = flip(me, dist)
            copy = pltpu.make_async_remote_copy(
                src_ref=src_ref.at[which, peer], dst_ref=seq_ref.at[me, rows],
                send_sem=cp_send.at[shift, dist - 1], recv_sem=cp_recv.at[shift, dist - 1],
                device_id={"cp": peer}, device_id_type=MESH)
            second.append(copy)
            copy.start()
        seq_ref[me, rows] = src_ref[which, me]

    forward(0, in_ref, my_tp)
    for shift in (1, 3, 2):
        first[shift].wait_recv()
        forward(shift, block_ref, lax.rem(my_tp + 4 - shift, 4))
    for shift in (1, 2, 3):
        first[shift].wait_send()
    for copy in second:
        copy.wait_send()
    for copy in second:
        copy.wait_recv()


def tokens_to_heads(collective_id, array):
    tp, heads, quarter, head_dim = array.shape
    dma = pltpu.SemaphoreType.DMA
    return pl.pallas_call(
        tokens_to_heads_kernel,
        out_shape=jax.ShapeDtypeStruct((heads, tp * quarter, head_dim), array.dtype),
        in_specs=[VMEM_SPEC],
        out_specs=VMEM_SPEC,
        scratch_shapes=[pltpu.VMEM(array.shape, array.dtype), dma((3,)), dma((3,)), dma((4, 3)), dma((4, 3))],
        compiler_params=pltpu.CompilerParams(collective_id=collective_id, has_side_effects=True, vmem_limit_bytes=VMEM_LIMIT),
        name="tokens_to_heads",
    )(array)


def turn(values):
    half_dim = values.shape[1] // 2
    return jnp.concatenate([values[:, half_dim:], values[:, :half_dim]], axis=1)


def front_kernel(full_width, sub, x_ref, wq_ref, wk_ref, wv_ref, cos_ref, sin_ref, qg_ref, kg_ref, q_out, k_out, v_out,
                 q_buf, k_buf, v_buf, lin_ref, own, slots, total, tp_send, tp_recv, ex_send, ex_recv):
    me, my_tp = lax.axis_index("cp"), lax.axis_index("tp")
    rows = x_ref.shape[0]
    heads, head_dim = qg_ref.shape
    peers_barrier()
    copies = []

    def send(idx, src, dst):
        for dist in (2, 3, 1):
            peer = flip(me, dist)
            copy = pltpu.make_async_remote_copy(
                src_ref=src.at[peer], dst_ref=dst.at[me], send_sem=ex_send.at[idx, dist - 1], recv_sem=ex_recv.at[idx, dist - 1],
                device_id={"cp": peer}, device_id_type=MESH)
            copy.start()
            copies.append(copy)
        dst[me] = src[me]

    def part_of(idx):
        return pl.ds(pl.multiple_of(idx * sub, sub), sub)

    def values(idx, carry):
        part = part_of(idx)
        out = dot_nt(x_ref[part, :], wv_ref[...]).astype(jnp.bfloat16)
        for head in range(heads):
            v_buf[head, part, :] = out[:, head * head_dim:(head + 1) * head_dim]
        return carry

    lax.fori_loop(0, rows // sub, values, 0)
    send(2, v_buf, v_out)

    def linear(idx, carry):
        part = part_of(idx)
        for number, w_ref in enumerate((wq_ref, wk_ref)):
            out = dot_nt(x_ref[part, :], w_ref[...])
            lin_ref[number, part, :] = out
            square = out * out
            square = sum(square[:, head * head_dim:(head + 1) * head_dim] for head in range(heads))
            own[number:number + 1, part] = jnp.sum(square.T, axis=0, keepdims=True)
        return carry

    lax.fori_loop(0, rows // sub, linear, 0)
    moves = []
    for shift in (1, 2, 3):
        move = pltpu.make_async_remote_copy(
            src_ref=own, dst_ref=slots.at[my_tp], send_sem=tp_send.at[shift - 1], recv_sem=tp_recv.at[shift - 1],
            device_id={"tp": lax.rem(my_tp + shift, 4)}, device_id_type=MESH)
        move.start()
        moves.append(move)
    slots[my_tp] = own[...]
    for move in moves:
        move.wait()
    total[...] = lax.rsqrt((slots[0] + slots[1] + slots[2] + slots[3]) / full_width + NORM_EPS)

    for number, (gain_ref, buf, out_ref) in enumerate(((qg_ref, q_buf, q_out), (kg_ref, k_buf, k_out))):
        def rotate(idx, carry, number=number, gain_ref=gain_ref, buf=buf):
            part = part_of(idx)
            inv = jnp.broadcast_to(total[number:number + 1, part], (head_dim, sub)).T
            for head in range(heads):
                scaled = lin_ref[number, part, head * head_dim:(head + 1) * head_dim] * inv * gain_ref[head:head + 1, :]
                buf[head, part, :] = (scaled * cos_ref[part, :] + turn(scaled) * sin_ref[part, :]).astype(jnp.bfloat16)
            return carry

        lax.fori_loop(0, rows // sub, rotate, 0)
        send(number, buf, out_ref)
    for copy in copies:
        copy.wait()


def front(collective_id, full_width, x, weights, cos_tab, sin_tab, q_gain, k_gain):
    rows, _ = x.shape
    heads, head_dim = q_gain.shape
    dma = pltpu.SemaphoreType.DMA
    block = (heads, rows, head_dim)
    stat = pltpu.VMEM((2, rows), jnp.float32)
    return pl.pallas_call(
        functools.partial(front_kernel, full_width, min(256, rows)),
        out_shape=tuple([jax.ShapeDtypeStruct(block, jnp.bfloat16)] * 3),
        in_specs=[VMEM_SPEC] * 8,
        out_specs=tuple([VMEM_SPEC] * 3),
        scratch_shapes=[pltpu.VMEM(block, jnp.bfloat16)] * 3 + [pltpu.VMEM((2, rows, heads * head_dim), jnp.float32),
                        stat, pltpu.VMEM((4, 2, rows), jnp.float32), stat, dma((3,)), dma((3,)), dma((3, 3)), dma((3, 3))],
        compiler_params=pltpu.CompilerParams(collective_id=collective_id, has_side_effects=True, vmem_limit_bytes=VMEM_LIMIT),
        name="front",
    )(x, *weights, cos_tab, sin_tab, q_gain, k_gain)


def causal_mask(scores):
    key_pos = lax.broadcasted_iota(jnp.int32, scores.shape, 0)
    query_pos = lax.broadcasted_iota(jnp.int32, scores.shape, 1)
    return jnp.where(key_pos <= query_pos, scores, MASK_VALUE)


def attend_kernel(block, factor, q_ref, k_ref, v_ref, o_ref, lse_ref):
    blk = pl.program_id(0)
    q_blk = q_ref[...]

    def scores_of(idx):
        rows = pl.ds(pl.multiple_of(idx * block, block), block)
        return dot_nt(k_ref[rows, :], q_blk), v_ref[rows, :]

    scores, v_blk = scores_of(blk)
    scores = causal_mask(scores)
    top = jnp.max(scores, axis=0, keepdims=True)
    probs = jnp.exp2((scores - top) * factor)
    norm = jnp.sum(probs, axis=0, keepdims=True)
    acc = dot_tn(v_blk, probs.astype(jnp.bfloat16))

    def step(idx, state):
        top, norm, acc = state
        scores, v_blk = scores_of(idx)
        new_top = jnp.maximum(top, jnp.max(scores, axis=0, keepdims=True))
        probs = jnp.exp2((scores - new_top) * factor)
        rescale = jnp.exp2((top - new_top) * factor)
        norm = norm * rescale + jnp.sum(probs, axis=0, keepdims=True)
        acc = acc * rescale + dot_tn(v_blk, probs.astype(jnp.bfloat16))
        return new_top, norm, acc

    top, norm, acc = lax.fori_loop(0, blk, step, (top, norm, acc))
    o_ref[...] = (acc / norm).T.astype(jnp.bfloat16)
    lse_ref[...] = top * factor + jnp.log2(norm)


def attend(q, k, v):
    rows, head_dim = q.shape
    block = min(512, rows // 4)
    whole = pl.BlockSpec((rows, head_dim), lambda i: (0, 0))
    part = pl.BlockSpec((block, head_dim), lambda i: (i, 0))
    return pl.pallas_call(
        functools.partial(attend_kernel, block, head_dim ** -0.5 * LOG2E),
        grid=(rows // block,),
        out_shape=(jax.ShapeDtypeStruct(q.shape, jnp.bfloat16), jax.ShapeDtypeStruct((1, rows), jnp.float32)),
        in_specs=[part, whole, whole],
        out_specs=(part, pl.BlockSpec((1, block), lambda i: (0, i))),
        compiler_params=pltpu.CompilerParams(vmem_limit_bytes=VMEM_LIMIT),
        cost_estimate=pl.CostEstimate(flops=2 * rows * rows * head_dim, bytes_accessed=8 * rows * head_dim, transcendentals=rows * rows // 2),
        name="attend",
    )(q, k, v)


def attend_back_kernel(block, scale, q_ref, k_ref, v_ref, o_ref, do_ref, lse_ref, dq_ref, dk_ref, dv_ref, delta_ref, dk_acc, dv_acc):
    blk = pl.program_id(0)
    n_blk = pl.num_programs(0)
    factor = scale * LOG2E

    @pl.when(blk == 0)
    def _():
        def prepare(idx, carry):
            rows = pl.ds(pl.multiple_of(idx * block, block), block)
            prod = do_ref[rows, :].astype(jnp.float32) * o_ref[rows, :].astype(jnp.float32)
            delta_ref[:, rows] = jnp.sum(prod.T, axis=0, keepdims=True)
            dq_ref[rows, :] = jnp.zeros((block, dq_ref.shape[1]), jnp.float32)
            return carry

        lax.fori_loop(0, n_blk, prepare, 0)

    k_blk = k_ref[...]
    v_blk = v_ref[...]

    def one(idx, masked):
        rows = pl.ds(pl.multiple_of(idx * block, block), block)
        q_blk = q_ref[rows, :]
        do_blk = do_ref[rows, :]
        scores = dot_nt(k_blk, q_blk)
        if masked:
            scores = causal_mask(scores)
        probs = jnp.exp2(scores * factor - lse_ref[:, rows])
        grad_v = dot_nn(probs.astype(jnp.bfloat16), do_blk)
        grad_p = dot_nt(v_blk, do_blk)
        grad_s = (probs * ((grad_p - delta_ref[:, rows]) * scale)).astype(jnp.bfloat16)
        dq_ref[rows, :] += dot_tn(grad_s, k_blk)
        return dot_nn(grad_s, q_blk), grad_v

    dk_acc[...], dv_acc[...] = one(blk, True)

    def step(idx, carry):
        grad_k, grad_v = one(idx, False)
        dk_acc[...] += grad_k
        dv_acc[...] += grad_v
        return carry

    lax.fori_loop(blk + 1, n_blk, step, 0)
    dk_ref[...] = dk_acc[...]
    dv_ref[...] = dv_acc[...].astype(jnp.bfloat16)


def attend_back(q, k, v, o, do, lse):
    rows, head_dim = q.shape
    block = min(512, rows // 4)
    whole = pl.BlockSpec((rows, head_dim), lambda i: (0, 0))
    part = pl.BlockSpec((block, head_dim), lambda i: (i, 0))
    stat = pl.BlockSpec((1, rows), lambda i: (0, 0))
    return pl.pallas_call(
        functools.partial(attend_back_kernel, block, head_dim ** -0.5),
        grid=(rows // block,),
        out_shape=(jax.ShapeDtypeStruct(q.shape, jnp.float32), jax.ShapeDtypeStruct(q.shape, jnp.float32), jax.ShapeDtypeStruct(q.shape, jnp.bfloat16)),
        in_specs=[whole, part, part, whole, whole, stat],
        out_specs=(whole, part, part),
        scratch_shapes=[pltpu.VMEM((1, rows), jnp.float32), pltpu.VMEM((block, head_dim), jnp.float32), pltpu.VMEM((block, head_dim), jnp.float32)],
        compiler_params=pltpu.CompilerParams(vmem_limit_bytes=VMEM_LIMIT),
        cost_estimate=pl.CostEstimate(flops=5 * rows * rows * head_dim, bytes_accessed=20 * rows * head_dim, transcendentals=rows * rows // 2),
        name="attend_back",
    )(q, k, v, o, do, lse)


def post_kernel(o_ref, mine_ref, other_ref, x_any, gy_any, pw_ref, both_ref, do_ref, gpost_ref, x_ref, gy_ref, sems):
    tp_size, heads, _, head_dim = o_ref.shape
    block = x_ref.shape[0]
    first_row = (lax.axis_index("tp") * pl.num_programs(0) + pl.program_id(0)) * block
    loads = []
    for idx, (src, dst) in enumerate(((x_any, x_ref), (gy_any, gy_ref))):
        load = pltpu.make_async_copy(src.at[pl.ds(pl.multiple_of(first_row, block), block)], dst, sems.at[idx])
        load.start()
        loads.append(load)
    core = lax.rem(lax.axis_index("cp"), 2)
    halves = ((mine_ref, core * (heads // 2)), (other_ref, (1 - core) * (heads // 2)))
    proj = None
    for idx in range(tp_size):
        for w_ref, start in halves:
            term = dot_nn(jnp.concatenate([o_ref[idx, start + head] for head in range(heads // 2)], axis=1), w_ref[idx])
            proj = term if proj is None else proj + term
    for load in loads:
        load.wait()
    gain = pw_ref[...]
    inv = lax.rsqrt(jnp.mean(proj * proj, axis=-1, keepdims=True) + NORM_EPS)
    hat = proj * inv
    d_model = x_ref.shape[1]
    both_ref[:, d_model:] = (x_ref[...].astype(jnp.float32) + hat * gain).astype(jnp.bfloat16)
    grad = gy_ref[...].astype(jnp.float32)
    gpost = jnp.sum(grad * hat, axis=0, keepdims=True)
    grad_hat = grad * gain
    grad_proj = (inv * (grad_hat - hat * jnp.mean(grad_hat * hat, axis=-1, keepdims=True))).astype(jnp.bfloat16)
    both_ref[:, :d_model] = grad_proj
    for idx in range(tp_size):
        for w_ref, start in halves:
            grad_o = dot_nt(grad_proj, w_ref[idx]).astype(jnp.bfloat16)
            for head in range(heads // 2):
                do_ref[idx, start + head] = grad_o[:, head * head_dim:(head + 1) * head_dim]

    @pl.when(pl.program_id(0) == 0)
    def _():
        gpost_ref[...] = jnp.zeros_like(gpost_ref)

    gpost_ref[...] += gpost


def post(o_all, wo_mine, wo_other, x, gy, gain):
    tp_size, heads, rows, head_dim = o_all.shape
    d_model = x.shape[1]
    block = min(128, rows)
    any_spec = pl.BlockSpec(memory_space=pl.ANY)
    piece = pltpu.VMEM((block, d_model), jnp.bfloat16)
    both = pl.BlockSpec((block, 2 * d_model), lambda i: (i, 0))
    by_head = pl.BlockSpec((tp_size, heads, block, head_dim), lambda i: (0, 0, i, 0))
    return pl.pallas_call(
        post_kernel,
        grid=(rows // block,),
        out_shape=(jax.ShapeDtypeStruct((rows, 2 * d_model), jnp.bfloat16), jax.ShapeDtypeStruct(o_all.shape, jnp.bfloat16), jax.ShapeDtypeStruct((1, d_model), jnp.float32)),
        in_specs=[by_head] + [pl.BlockSpec(wo_mine.shape, lambda i: (0, 0, 0))] * 2 + [any_spec, any_spec, pl.BlockSpec((1, d_model), lambda i: (0, 0))],
        out_specs=(both, by_head, pl.BlockSpec((1, d_model), lambda i: (0, 0))),
        scratch_shapes=[piece, piece, pltpu.SemaphoreType.DMA((2,))],
        compiler_params=pltpu.CompilerParams(vmem_limit_bytes=VMEM_LIMIT),
        cost_estimate=pl.CostEstimate(flops=4 * rows * d_model * d_model, bytes_accessed=4 * d_model * d_model, transcendentals=rows),
        name="post",
    )(o_all, wo_mine, wo_other, x, gy, gain)


def output_weights_kernel(o_ref, gp_ref, out_ref):
    heads, _, head_dim = o_ref.shape
    acc = dot_tn(jnp.concatenate([o_ref[head] for head in range(heads)], axis=1), gp_ref[...])
    for head in range(heads):
        out_ref[head] = acc[head * head_dim:(head + 1) * head_dim, :]


def output_weights(o_heads, both):
    heads, rows, head_dim = o_heads.shape
    d_model = both.shape[1] // 2
    block = min(512, d_model)
    return pl.pallas_call(
        output_weights_kernel,
        grid=(d_model // block,),
        out_shape=jax.ShapeDtypeStruct((heads, head_dim, d_model), jnp.float32),
        in_specs=[pl.BlockSpec(o_heads.shape, lambda i: (0, 0, 0)), pl.BlockSpec((rows, block), lambda i: (0, i))],
        out_specs=pl.BlockSpec((heads, head_dim, block), lambda i: (0, 0, i)),
        compiler_params=pltpu.CompilerParams(vmem_limit_bytes=VMEM_LIMIT),
        cost_estimate=pl.CostEstimate(flops=2 * rows * d_model * heads * head_dim, bytes_accessed=12 * rows * d_model, transcendentals=0),
        name="output_weights",
    )(o_heads, both)


def spread_kernel(in_ref, *out_refs):
    for number, out_ref in enumerate(out_refs):
        for head in range(in_ref.shape[0]):
            out_ref[:, head, :] = in_ref[head, number]


def spread(gathered):
    heads, count, d_model, head_dim = gathered.shape
    block = min(256, d_model)
    return pl.pallas_call(
        spread_kernel,
        grid=(d_model // block,),
        out_shape=tuple([jax.ShapeDtypeStruct((d_model, heads, head_dim), gathered.dtype)] * count),
        in_specs=[pl.BlockSpec((heads, count, block, head_dim), lambda i: (0, 0, i, 0))],
        out_specs=tuple([pl.BlockSpec((block, heads, head_dim), lambda i: (i, 0, 0))] * count),
        compiler_params=pltpu.CompilerParams(vmem_limit_bytes=VMEM_LIMIT),
        cost_estimate=pl.CostEstimate(flops=d_model * heads * head_dim * count, bytes_accessed=8 * d_model * heads * head_dim * count, transcendentals=0),
        name="spread",
    )(gathered)


def chain_kernel(size, n_chunk, lag, tile, dq_ref, dk_ref, dv_ref, wq_ref, wk_ref, wv_ref, gy_ref, out_ref, part_ref, sums_a, sums_b, rs_send, rs_recv, ag_send, ag_recv):
    me = lax.axis_index("tp")
    entry_barrier("tp", size)
    half = part_ref.shape[0] // 2
    rows = half // n_chunk
    last = size - 1

    def parts(side, chunk):
        local = pl.ds(pl.multiple_of(chunk * rows, rows), rows)
        glob = pl.ds(pl.multiple_of(side * half + chunk * rows, rows), rows)
        sums = (sums_a, sums_b)[side]
        return local, glob, sums

    def toward(side):
        return jnp.maximum(me - 1, 0) if side == 0 else jnp.minimum(me + 1, last)

    def away(side):
        return jnp.minimum(me + 1, last) if side == 0 else jnp.maximum(me - 1, 0)

    def rs_copy(side, chunk, first):
        local, glob, sums = parts(side, chunk)
        return pltpu.make_async_remote_copy(
            src_ref=part_ref.at[glob] if first else sums.at[local], dst_ref=sums.at[local],
            send_sem=rs_send.at[side, chunk], recv_sem=rs_recv.at[side, chunk],
            device_id={"tp": toward(side)}, device_id_type=MESH)

    def ag_copy(side, chunk):
        _, glob, _ = parts(side, chunk)
        return pltpu.make_async_remote_copy(
            src_ref=out_ref.at[glob], dst_ref=out_ref.at[glob],
            send_sem=ag_send.at[side, chunk], recv_sem=ag_recv.at[side, chunk],
            device_id={"tp": away(side)}, device_id_type=MESH)

    def place(side):
        return me if side == 0 else last - me

    heads = dq_ref.shape[0]
    d_model = out_ref.shape[1]
    block = min(512, d_model)
    n_tile = 2 * half // tile
    per_tile = tile // rows

    def push(number):
        for side in (0, 1):
            @pl.when((lax.rem(number, 2) == side) & (place(side) == last))
            def _(side=side):
                def one(idx, carry):
                    rs_copy(side, (number // 2) * per_tile + idx, True).start()
                    return carry

                lax.fori_loop(0, per_tile, one, 0)

    def product(number, carry):
        tile_rows = pl.ds(pl.multiple_of(lax.rem(number, 2) * half + (number // 2) * tile, tile), tile)

        def columns(idx, carry):
            cols = pl.ds(pl.multiple_of(idx * block, block), block)
            total = None
            for grad_ref, w_ref in ((dq_ref, wq_ref), (dk_ref, wk_ref), (dv_ref, wv_ref)):
                grad = jnp.concatenate([grad_ref[idx_h, tile_rows, :] for idx_h in range(heads)], axis=1)
                term = dot_nn(grad, w_ref[:, cols])
                total = term if total is None else total + term
            part_ref[tile_rows, cols] = total
            return carry

        lax.fori_loop(0, d_model // block, columns, 0)

        @pl.when(number > 0)
        def _():
            push(number - 1)

        return carry

    lax.fori_loop(0, n_tile, product, 0)
    push(jnp.int32(n_tile - 1))

    def pass_on(side, chunk):
        local, glob, sums = parts(side, chunk)
        rs_copy(side, chunk, False).wait_recv()
        sums[local] = sums[local] + part_ref[glob]
        rs_copy(side, chunk, False).start()

    def finish(side, chunk):
        local, glob, sums = parts(side, chunk)
        rs_copy(side, chunk, False).wait_recv()
        out_ref[glob] = (gy_ref[glob].astype(jnp.float32) + (sums[local] + part_ref[glob])).astype(jnp.bfloat16)
        ag_copy(side, chunk).start()

    def reduce_step(idx, carry):
        for far in range(last - 1, 0, -1):
            chunk = idx - (last - 1 - far) * lag
            for side in (0, 1):
                @pl.when((chunk >= 0) & (chunk < n_chunk) & (place(side) == far))
                def _(side=side, chunk=chunk):
                    pass_on(side, chunk)
        for side in (0, 1):
            @pl.when((idx < n_chunk) & (place(side) == 0))
            def _(side=side):
                finish(side, idx)
        return carry

    lax.fori_loop(0, n_chunk + (last - 2) * lag, reduce_step, 0)

    def return_step(idx, carry):
        for far in range(1, last + 1):
            chunk = idx - (far - 1) * lag
            for side in (0, 1):
                @pl.when((chunk >= 0) & (chunk < n_chunk) & (place(side) == far))
                def _(side=side, chunk=chunk, far=far):
                    ag_copy(side, chunk).wait_recv()
                    if far < last:
                        ag_copy(side, chunk).start()
        return carry

    lax.fori_loop(0, n_chunk + (last - 1) * lag, return_step, 0)

    def drain(idx, carry):
        for side in (0, 1):
            @pl.when(place(side) > 0)
            def _(side=side):
                rs_copy(side, idx, False).wait_send()

            @pl.when(place(side) < last)
            def _(side=side):
                ag_copy(side, idx).wait_send()
        return carry

    lax.fori_loop(0, n_chunk, drain, 0)


def chain_sum(size, collective_id, grads, weights, gy):
    rows, d_model = gy.shape
    n_chunk = 32 if rows >= 512 else 4
    sems = [pltpu.SemaphoreType.DMA((2, n_chunk))] * 4
    return pl.pallas_call(
        functools.partial(chain_kernel, size, n_chunk, 2, min(256, rows // 4)),
        out_shape=jax.ShapeDtypeStruct((rows, d_model), jnp.bfloat16),
        in_specs=[VMEM_SPEC] * 7,
        out_specs=VMEM_SPEC,
        scratch_shapes=[pltpu.VMEM((rows, d_model), jnp.float32), pltpu.VMEM((rows // 2, d_model), jnp.float32), pltpu.VMEM((rows // 2, d_model), jnp.float32)] + sems,
        compiler_params=pltpu.CompilerParams(collective_id=collective_id, has_side_effects=True, vmem_limit_bytes=VMEM_LIMIT),
        cost_estimate=pl.CostEstimate(flops=10 ** 11, bytes_accessed=16 * rows * d_model, transcendentals=0),
        name="chain_sum",
    )(*grads, *weights, gy)


def weights_back_kernel(full_width, sub, x_ref, far0_ref, far1_ref, wq_ref, wk_ref, dq_ref, dk_ref, dv_ref, cos_ref, sin_ref, qg_ref, kg_ref, post_ref,
                        dw_ref, exq_ref, exk_ref, exv_ref, gains_ref, post_out,
                        x_buf, wqk_ref, lin_ref, q16_ref, k16_ref, own, slots_tp, mid, slots_cp, done, total, gq_ref, gk_ref, my_gains,
                        x_sem, w_sem, pair_send, pair_recv, tp_send, tp_recv, cp_send, cp_recv, back_send, back_recv, ex_send, ex_recv):
    me = lax.axis_index("cp")
    my_tp = lax.axis_index("tp")
    rows, head_dim = dq_ref.shape[1:]
    loads = []
    step = far0_ref.shape[0]
    fars = ((far0_ref, pl.ds(0, step)), (far1_ref, pl.ds(step, rows - step)))
    pieces = ((x_ref, 0, pl.ds(0, rows)),) + tuple((ref, 2, part) for ref, part in fars)
    for idx, (src, dist, part) in enumerate(pieces):
        load = pltpu.make_async_copy(src, x_buf.at[dist, part], x_sem.at[idx])
        load.start()
        loads.append(load)
    own_rows = pl.ds(pl.multiple_of(me * head_dim, head_dim), head_dim)
    w_loads = [pltpu.make_async_copy(src.at[own_rows], wqk_ref.at[pl.ds(idx * head_dim, head_dim)], w_sem.at[idx]) for idx, src in enumerate((wq_ref, wk_ref))]
    for load in w_loads:
        load.start()
    peers_barrier()
    for idx, (src, dist, part) in enumerate(pieces):
        load = pltpu.make_async_remote_copy(
            src_ref=src, dst_ref=x_buf.at[dist + 1, part], send_sem=pair_send.at[idx], recv_sem=pair_recv.at[idx],
            device_id={"cp": flip(me, 1)}, device_id_type=MESH)
        load.start()
        loads.append(load)
    own[4:5, :] = jnp.zeros_like(own[4:5, :])
    own[4:5, 0:post_ref.shape[1]] = post_ref[...]

    def ex_copy(idx, src, dst, dist):
        peer = flip(me, dist)
        return pltpu.make_async_remote_copy(
            src_ref=src.at[peer], dst_ref=dst.at[me], send_sem=ex_send.at[idx, dist - 1], recv_sem=ex_recv.at[idx, dist - 1],
            device_id={"cp": peer}, device_id_type=MESH)

    copies = [ex_copy(2, dv_ref, exv_ref, dist) for dist in (2, 3, 1)]
    for copy in copies:
        copy.start()

    def grad_of(ref, blk, part, table):
        g = ref[blk, part, :]
        return g * cos_ref[table, :] - turn(g) * sin_ref[table, :]

    w_loads[0].wait()
    w_loads[1].wait()
    sides = ((dq_ref, qg_ref, 0), (dk_ref, kg_ref, 1))
    for order, dist in enumerate((0, 2, 1, 3)):
        blk = flip(me, dist)
        for load in (loads[0:1], loads[1:3], loads[3:4], loads[4:6])[order]:
            if order < 2:
                load.wait()
            else:
                load.wait_recv()

        def first(idx, carry, dist=dist, blk=blk):
            part = pl.ds(pl.multiple_of(idx * sub, sub), sub)
            table = pl.ds(pl.multiple_of(blk * rows + idx * sub, sub), sub)
            lin = dot_nt(x_buf[dist, part, :], wqk_ref[...])
            lin_ref[dist, part, :] = lin
            for ref, gain_ref, number in sides:
                mine = lin[:, number * head_dim:(number + 1) * head_dim]
                grad = grad_of(ref, blk, part, table) * gain_ref[...]
                own[2 * number:2 * number + 1, table] = jnp.sum((mine * mine).T, axis=0, keepdims=True)
                own[2 * number + 1:2 * number + 2, table] = jnp.sum((grad * mine).T, axis=0, keepdims=True)
            return carry

        lax.fori_loop(0, rows // sub, first, 0)

    quarter = own.shape[1] // 4

    def quarter_of(which):
        return pl.ds(pl.multiple_of(which * quarter, quarter), quarter)

    moves = []
    for shift in (2, 1, 3):
        peer = lax.rem(my_tp + shift, 4)
        move = pltpu.make_async_remote_copy(
            src_ref=own.at[:, quarter_of(peer)], dst_ref=slots_tp.at[my_tp], send_sem=tp_send.at[shift - 1], recv_sem=tp_recv.at[shift - 1],
            device_id={"tp": peer}, device_id_type=MESH)
        move.start()
        moves.append(move)
    slots_tp[my_tp] = own[:, quarter_of(my_tp)]
    for move in moves:
        move.wait()
    mid[...] = slots_tp[0] + slots_tp[1] + slots_tp[2] + slots_tp[3]
    moves = []
    for dist in (2, 3, 1):
        move = pltpu.make_async_remote_copy(
            src_ref=mid, dst_ref=slots_cp.at[me], send_sem=cp_send.at[dist - 1], recv_sem=cp_recv.at[dist - 1],
            device_id={"cp": flip(me, dist)}, device_id_type=MESH)
        move.start()
        moves.append(move)
    slots_cp[me] = mid[...]
    for move in moves:
        move.wait()
    done[...] = slots_cp[0] + slots_cp[1] + slots_cp[2] + slots_cp[3]
    moves = []
    for shift in (2, 1, 3):
        move = pltpu.make_async_remote_copy(
            src_ref=done, dst_ref=total.at[:, quarter_of(my_tp)], send_sem=back_send.at[shift - 1], recv_sem=back_recv.at[shift - 1],
            device_id={"tp": lax.rem(my_tp + shift, 4)}, device_id_type=MESH)
        move.start()
        moves.append(move)
    total[:, quarter_of(my_tp)] = done[...]
    for move in moves:
        move.wait()

    post_out[...] = total[4:5, 0:post_ref.shape[1]]
    gq_ref[...] = jnp.zeros_like(gq_ref)
    gk_ref[...] = jnp.zeros_like(gk_ref)
    outs = ((q16_ref, exq_ref, gq_ref), (k16_ref, exk_ref, gk_ref))
    for dist in (2, 3, 1, 0):
        blk = flip(me, dist)

        def second(idx, carry, dist=dist, blk=blk):
            part = pl.ds(pl.multiple_of(idx * sub, sub), sub)
            table = pl.ds(pl.multiple_of(blk * rows + idx * sub, sub), sub)
            lin = lin_ref[dist, part, :]
            for (ref, gain_ref, number), (d16_ref, _, gain_out) in zip(sides, outs):
                mine = lin[:, number * head_dim:(number + 1) * head_dim]
                inv = lax.rsqrt(total[2 * number:2 * number + 1, table] / full_width + NORM_EPS)
                dot = inv * total[2 * number + 1:2 * number + 2, table] / full_width
                inv = jnp.broadcast_to(inv, (head_dim, sub)).T
                dot = jnp.broadcast_to(dot, (head_dim, sub)).T
                raw = grad_of(ref, blk, part, table)
                hat = mine * inv
                d16_ref[blk, part, :] = (inv * (raw * gain_ref[...] - hat * dot)).astype(jnp.bfloat16)
                gain_out[...] += jnp.sum(raw * hat, axis=0, keepdims=True)
            return carry

        lax.fori_loop(0, rows // sub, second, 0)
        if dist:
            for idx, (d16_ref, ex_ref, _) in enumerate(outs):
                copy = ex_copy(idx, d16_ref, ex_ref, dist)
                copy.start()
                copies.append(copy)
    my_gains[0:1, :] = gq_ref[...]
    my_gains[1:2, :] = gk_ref[...]
    for src, dst in ((q16_ref, exq_ref), (k16_ref, exk_ref), (dv_ref, exv_ref)):
        dst[me] = src[me]
    gains_ref[me] = my_gains[...]
    for dist in (1, 2, 3):
        copy = pltpu.make_async_remote_copy(
            src_ref=my_gains, dst_ref=gains_ref.at[me], send_sem=ex_send.at[3, dist - 1], recv_sem=ex_recv.at[3, dist - 1],
            device_id={"cp": flip(me, dist)}, device_id_type=MESH)
        copy.start()
        copies.append(copy)

    block = min(512, x_buf.shape[2])

    def weight_step(idx, carry):
        cols = pl.ds(pl.multiple_of(idx * block, block), block)
        acc = None
        for dist in range(4):
            blk = flip(me, dist)
            grads = jnp.concatenate([q16_ref[blk], k16_ref[blk], dv_ref[blk]], axis=1)
            term = dot_tn(grads, x_buf[dist, :, cols])
            acc = term if acc is None else acc + term
        acc = acc.T
        for number in range(3):
            dw_ref[number, cols, :] = acc[:, number * head_dim:(number + 1) * head_dim]
        return carry

    lax.fori_loop(0, x_buf.shape[2] // block, weight_step, 0)
    for copy in copies:
        copy.wait()
    for load in loads[3:]:
        load.wait_send()


def weights_back(collective_id, full_width, x, x_far, wq, wk, dq, dk, dv, cos_tab, sin_tab, q_gain, k_gain, grad_post):
    _, rows, head_dim = dq.shape
    d_model = x.shape[1]
    any_spec = pl.BlockSpec(memory_space=pl.ANY)
    dma = pltpu.SemaphoreType.DMA
    span = max(4 * rows, d_model)
    stat = pltpu.VMEM((5, span), jnp.float32)
    slots = pltpu.VMEM((4, 5, span // 4), jnp.float32)
    small = pltpu.VMEM((5, span // 4), jnp.float32)
    ex = jax.ShapeDtypeStruct(dq.shape, jnp.bfloat16)
    return pl.pallas_call(
        functools.partial(weights_back_kernel, full_width, min(512, rows)),
        out_shape=(jax.ShapeDtypeStruct((3, d_model, head_dim), jnp.float32), ex, ex, ex,
                   jax.ShapeDtypeStruct((4, 2, head_dim), jnp.float32), jax.ShapeDtypeStruct((1, d_model), jnp.float32)),
        in_specs=[any_spec] * 5 + [VMEM_SPEC] * 8,
        out_specs=tuple([VMEM_SPEC] * 6),
        scratch_shapes=[pltpu.VMEM((4, rows, d_model), jnp.bfloat16), pltpu.VMEM((2 * head_dim, d_model), jnp.bfloat16), pltpu.VMEM((4, rows, 2 * head_dim), jnp.float32),
                        pltpu.VMEM(dq.shape, jnp.bfloat16), pltpu.VMEM(dq.shape, jnp.bfloat16),
                        stat, slots, small, slots, small, stat,
                        pltpu.VMEM((1, head_dim), jnp.float32), pltpu.VMEM((1, head_dim), jnp.float32), pltpu.VMEM((2, head_dim), jnp.float32),
                        dma((3,)), dma((2,)), dma((3,)), dma((3,)), dma((3,)), dma((3,)), dma((3,)), dma((3,)), dma((3,)), dma((3,)), dma((4, 3)), dma((4, 3))],
        compiler_params=pltpu.CompilerParams(collective_id=collective_id, has_side_effects=True, vmem_limit_bytes=VMEM_LIMIT),
        name="weights_back",
    )(x, *x_far, wq, wk, dq, dk, dv, cos_tab, sin_tab, q_gain, k_gain, grad_post)


def solution(mesh):
    tp_size = mesh.shape["tp"]
    cp_size = mesh.shape["cp"]
    act_spec = P("dp", "cp", None)
    col_spec = P(None, "tp", None)
    part_col = P("dp", "tp", None)
    in_specs = (act_spec, col_spec, col_spec, col_spec, P("tp", None, None), P("tp", None), P("tp", None), P(None), act_spec)
    out_specs = (act_spec, act_spec, part_col, part_col, part_col, P(("dp", "tp"), None, None), P(("dp", "tp"), None), P(("dp", "tp"), None), P("dp"))
    swap_core = [(dev, dev ^ 1) for dev in range(cp_size)]

    def local_run(x_in, w_q, w_k, w_v, w_o, q_norm_w, k_norm_w, post_norm_w, grad_y):
        rows, d_model = x_in.shape[1:]
        heads, head_dim = w_q.shape[1:]
        width = heads * head_dim
        full_width = width * tp_size
        x = x_in[0]
        gy = grad_y[0]
        cp_index = lax.axis_index("cp")

        def wide_tables(cos_tab, sin_tab):
            return jnp.concatenate([cos_tab, cos_tab], axis=1), jnp.concatenate([-sin_tab, sin_tab], axis=1)

        cos_tab, sin_tab = wide_tables(*rope_tables((cp_index * rows + jnp.arange(rows)).astype(jnp.float32), head_dim))
        turned = tuple(w.reshape(d_model, width).T for w in (w_q, w_k, w_v))

        core = cp_index % 2
        own_half = lax.dynamic_slice_in_dim(w_o, core * (heads // 2), heads // 2, axis=0)
        wo_mine = lax.all_gather(own_half, "tp").reshape(tp_size, width // 2, d_model)
        q_seq, k_seq, v_seq = front(1, full_width, x, turned, cos_tab, sin_tab, q_norm_w, k_norm_w)
        seq_shape = (cp_size * rows, head_dim)
        block_shape = (cp_size, rows, head_dim)
        piece = rows // 4

        def fetch(start, size):
            return lax.ppermute(x_free[start:start + size], "cp", [(dev, dev ^ 2) for dev in range(cp_size)])

        q_seq, x_free = lax.optimization_barrier((q_seq, x))
        far0 = fetch(0, piece)
        q_seq, k_seq, v_seq = (t.reshape(seq_shape) for t in (q_seq, k_seq, v_seq))
        o_seq, lse = attend(q_seq, k_seq, v_seq)
        o_seq, wo_mine = lax.optimization_barrier((o_seq, wo_mine))
        wo_other = lax.ppermute(wo_mine, "cp", swap_core)
        o_heads, o_tokens = heads_to_tokens(2, o_seq.reshape(block_shape))
        both, do_tokens, grad_post = post(o_tokens, wo_mine, wo_other, x, gy, post_norm_w[None, :])
        do_seq = tokens_to_heads(3, do_tokens)
        both, do_seq, x_free = lax.optimization_barrier((both, do_seq, x))
        both = lax.all_gather(both, "tp", tiled=True)
        far1 = fetch(piece, rows - piece)

        coarse_cos, coarse_sin = rope_tables(jnp.arange(0, cp_size * rows, 64, dtype=jnp.float32), head_dim)
        fine_cos, fine_sin = (jnp.concatenate([t, t], axis=1)[None] for t in rope_tables(jnp.arange(64, dtype=jnp.float32), head_dim))
        wide_cos, wide_sin, sign_cos, sign_sin = lax.optimization_barrier(tuple(
            jnp.concatenate([sign * t, t], axis=1)[:, None, :] for sign in (1.0, -1.0) for t in (coarse_cos, coarse_sin)))
        fine_cos, fine_sin = lax.optimization_barrier((fine_cos, fine_sin))
        seq_cos = (wide_cos * fine_cos - wide_sin * fine_sin).reshape(cp_size * rows, head_dim)
        seq_sin = (sign_sin * fine_cos + sign_cos * fine_sin).reshape(cp_size * rows, head_dim)
        gains_head = tuple(lax.dynamic_slice_in_dim(w, cp_index, 1, axis=0) for w in (q_norm_w, k_norm_w))
        dq_seq, dk_seq, dv_seq = attend_back(q_seq, k_seq, v_seq, o_seq, do_seq.reshape(seq_shape), lse)
        dw, dq16, dk16, dv16, gains, grad_post = weights_back(
            4, full_width, x, (far0, far1), turned[0], turned[1],
            dq_seq.reshape(block_shape), dk_seq.reshape(block_shape), dv_seq.reshape(block_shape), seq_cos, seq_sin, *gains_head, grad_post)
        o_heads, dw = lax.optimization_barrier((o_heads, dw))
        grad_w_o = lax.psum(output_weights(o_heads, both), "cp")
        y_out = both[:, d_model:]
        dw = spread(lax.all_gather(dw, "cp"))
        grad_x = chain_sum(tp_size, 6, (dq16, dk16, dv16), turned, gy)
        return (y_out[None], grad_x[None]) + tuple(dw) + (grad_w_o, gains[:, 0], gains[:, 1], grad_post[0])

    return jax.shard_map(local_run, mesh=mesh, in_specs=in_specs, out_specs=out_specs, check_vma=False)
```
